32 devices in a mesh: pop: 8 (over z, y), mp: 4 (over x, core).
Axes of the slice: x: 2, y: 2, z: 4, core: 2. Of those that a mesh axis runs over, the one named last changes fastest.
Arguments:
- token_ids: int32 [96, 4, 16], P('pop'), may hold values from 0 to 255
- fitness_ranks: int32 [96], P('pop'), may hold values from 0 to 143, as said below
- embedding: bfloat16 [256, 4096], P(None, 'mp'), may hold values from -6 to 6
- mix_weights: bfloat16 [2, 4096, 4096], P(None, 'mp'), may hold values from -0.09375 to 0.09375
- factors_in: bfloat16 [2, 96, 4, 4096], P(None, 'pop', None, 'mp'), may hold values from -6 to 6
- factors_out: bfloat16 [2, 96, 4, 4096], P(None, 'pop'), may hold values from -6 to 6
- decay_rates: float32 [2, 4096], P(None, 'mp'), may hold values from 0.2 to 0.98
- norm_gain: float32 [2, 4096], P(None, 'mp'), may hold values from 0.1 to 1.9
- reward_dir: float32 [4096], P('mp'), may hold values from -6 to 6
Outputs:
- final_features: bfloat16 [96, 4, 4096], P('pop', None, 'mp')
- scores: float32 [96, 4], P('pop')
- weight_step: float32 [2, 4096, 4096], P(None, 'mp', 'pop')
The draws below stay inside these ranges and needn't reach their ends.
Inputs may be any that keep to these rules, and one draw needn't show every extreme that they name: `fitness_ranks`: ranks may repeat.
All inputs are finite; a program needn't handle non-finite values.
Results may differ from the reference program's by a relative error of at most 0.023.
Values may be sent and summed in bfloat16 or wider, within the bound.
A program may use at most 128 MiB of HBM per device.

```python
import jax
import jax.numpy as jnp
from jax import lax

D = 4096
VOCAB = 256
RANK = 4
LAYERS = 2
STEPS = 16
SEQS = 4
MEMBERS = 96
N_MP = 4


def draw_fitness_ranks(key, part):
    member_idx = jnp.arange(MEMBERS, dtype=jnp.int32)
    upper = MEMBERS // 2 + member_idx + 1
    drawn = jax.random.randint(jax.random.fold_in(key, 11), (MEMBERS,), 0, upper, dtype=jnp.int32)
    drawn = drawn.at[MEMBERS - 1].set(MEMBERS + MEMBERS // 2 - 1)
    drawn = drawn.at[0].set(0)
    return drawn


def place_ends(array, rng, smallest, high):
    dims = array.shape
    index_at = [jax.random.randint(jax.random.fold_in(rng, axis), (), 0, dims[axis]) for axis in range(len(dims))]
    array = array.at[tuple(index_at)].set(smallest)
    longest = dims.index(max(dims))
    index_at[longest] = (index_at[longest] + 1) % dims[longest]
    return array.at[tuple(index_at)].set(high)


def block_levels(stream_key, dims, pieces, smallest, top_value):
    gain, own = 1.0, jax.random.fold_in(stream_key, 6)
    for axis_at, blocks in pieces:
        heights = jnp.exp(jax.random.uniform(jax.random.fold_in(own, axis_at), (blocks,), jnp.float32, smallest / len(pieces), top_value / len(pieces)))
        gain = gain * jnp.repeat(heights, dims[axis_at] // blocks).reshape([-1 if axis == axis_at else 1 for axis in range(len(dims))])
    return gain


def centred(own_key, extent, spread, reach, shards=(), kind=jnp.bfloat16):
    level = block_levels(own_key, extent, shards, -0.22, 0.18) if shards else 1.0
    entries = jax.random.normal(own_key, extent, jnp.float32) * spread * level
    return jnp.minimum(jnp.maximum(entries, -reach), reach).astype(kind)


def setup_inputs(seed: int = 0) -> dict:
    seeds = jax.random.split(jax.random.key(seed), 10)
    token_ids = place_ends(jax.random.randint(seeds[0], (MEMBERS, SEQS, STEPS), 0, VOCAB), jax.random.fold_in(seeds[0], 1), 0, VOCAB - 1).astype(jnp.int32)
    fitness_ranks = draw_fitness_ranks(jax.random.fold_in(seeds[9], 71), 0)
    embedding = centred(seeds[2], (VOCAB, D), 1.0, 6.0, ((1, 4),))
    mix_weights = centred(seeds[3], (LAYERS, D, D), D ** -0.5, 0.09375, ((1, 4),))
    factors_in = centred(seeds[4], (LAYERS, MEMBERS, RANK, D), 1.0, 6.0, ((1, 8), (3, 4)))
    factors_out = centred(seeds[5], (LAYERS, MEMBERS, RANK, D), 1.0, 6.0, ((1, 8),))
    decay_rates = jnp.clip(0.2 + 0.78000002 * jax.random.uniform(seeds[6], (LAYERS, D), jnp.float32) ** block_levels(seeds[6], (LAYERS, D), ((1, 4),), -0.2, 0.2), 0.2, 0.98)
    norm_gain = jnp.clip(1.0 + 0.18 * jax.random.normal(seeds[7], (LAYERS, D), jnp.float32), 0.1, 1.9)
    reward_dir = centred(seeds[8], (D,), 1.0, 6.0, ((0, 4),), jnp.float32)
    return dict(token_ids=token_ids, fitness_ranks=fitness_ranks, embedding=embedding, mix_weights=mix_weights, factors_in=factors_in, factors_out=factors_out, decay_rates=decay_rates, norm_gain=norm_gain, reward_dir=reward_dir)


noise_scale = 0.25
norm_eps = 1e-06
spread_eps = 1e-05

def recurrence(inputs, decay):
    time_major = jnp.moveaxis(inputs, 2, 0)

    def advance(carried, column):
        carried = decay * carried + (1.0 - decay) * column
        return (carried, carried)
    initial = jnp.zeros(time_major.shape[1:], jnp.float32)
    _, states = lax.scan(advance, initial, time_major)
    return jnp.moveaxis(states, 0, 2)

def reference(token_ids, fitness_ranks, embedding, mix_weights, factors_in, factors_out, decay_rates, norm_gain, reward_dir):
    block_width = D // N_MP
    coef = noise_scale * (D * RANK) ** (-0.5)
    hidden = jnp.take(embedding, token_ids, axis=0)
    shape_full = hidden.shape
    for layer_idx in range(LAYERS):
        base_mix = jnp.zeros((MEMBERS * SEQS * STEPS, D), jnp.float32)
        for shard_idx in range(N_MP):
            portion = hidden[..., shard_idx * block_width:(shard_idx + 1) * block_width].reshape(-1, block_width)
            rows_w = mix_weights[layer_idx, shard_idx * block_width:(shard_idx + 1) * block_width, :]
            partial_value = jnp.dot(portion, rows_w, preferred_element_type=jnp.float32).astype(jnp.bfloat16)
            partial_value = lax.optimization_barrier(partial_value)
            base_mix = base_mix + partial_value.astype(jnp.float32)
        base_mix = base_mix.reshape(shape_full)
        low_rank = jnp.einsum('mstd,mrd->mstr', hidden.astype(jnp.float32), factors_in[layer_idx].astype(jnp.float32))
        correction = jnp.einsum('mstr,mrd->mstd', low_rank, factors_out[layer_idx].astype(jnp.float32), precision=lax.Precision.HIGHEST)
        mixed = base_mix + coef * correction
        states = recurrence(mixed, decay_rates[layer_idx])
        mean_sq = lax.optimization_barrier(jnp.mean(states * states, axis=3, keepdims=True))
        norm_scale = lax.rsqrt(mean_sq + norm_eps)
        hidden = (hidden.astype(jnp.float32) + states * norm_scale * norm_gain[layer_idx]).astype(jnp.bfloat16)
    final_features = hidden[:, :, STEPS - 1, :]
    dots = jnp.einsum('mstd,d->mst', hidden.astype(jnp.float32), reward_dir, precision=lax.Precision.HIGHEST)
    scores = lax.optimization_barrier(jnp.mean(dots, axis=2)) * D ** (-0.5)
    shares = fitness_ranks.astype(jnp.float32) / MEMBERS
    rank_mean = jnp.mean(shares)
    rank_spread = jnp.mean((shares - rank_mean) * (shares - rank_mean)) + spread_eps
    shaped = (shares - rank_mean) * lax.rsqrt(rank_spread)
    deltas = []
    for layer_idx in range(LAYERS):
        weighted = (factors_in[layer_idx].astype(jnp.float32) * shaped[:, None, None]).astype(jnp.bfloat16)
        outer = factors_out[layer_idx]
        delta = jnp.dot(weighted.reshape(-1, D).T, outer.reshape(-1, D), preferred_element_type=jnp.float32)
        deltas.append(delta * (MEMBERS * RANK) ** (-0.5))
    weight_step = jnp.stack(deltas, axis=0)
    return (final_features, scores, weight_step)
```

```python
import functools

import jax
import jax.numpy as jnp
from jax import lax
from jax.experimental import pallas as pl
from jax.experimental.pallas import tpu as pltpu
from jax.sharding import PartitionSpec as P

noise_scale = 0.25
norm_eps = 1e-06
spread_eps = 1e-05
lanes = 128
f32, bf16 = jnp.float32, jnp.bfloat16


def policy_kernel(
    dims,
    ids_hbm,
    embed_hbm,
    mix_ref,
    fin_hbm,
    fout_hbm,
    ranks_smem,
    decay_hbm,
    gain_hbm,
    reward_hbm,
    final_ref,
    score_ref,
    step_ref,
    ids_ref,
    embed_ref,
    fin_raw,
    fout_raw,
    decay_ref,
    gain_ref,
    reward_ref,
    weights,
    rows_embed,
    own_part,
    got_part,
    own_over,
    got_over,
    mine_part,
    table,
    own_pair,
    got_pair,
    own_cross,
    got_cross,
    states,
    hidden,
    onehot_ref,
    fin_ref,
    fout_ref,
    scaled,
    gin_ref,
    gout_ref,
    granks_ref,
    lows,
    squares,
    leans,
    lasts,
    heads,
    alphas,
    small,
    weight_sem,
    load_sem,
    part_send,
    part_recv,
    over_send,
    over_recv,
    hand_send,
    hand_recv,
    pair_send,
    pair_recv,
    cross_send,
    cross_recv,
    small_send,
    small_recv,
    relay_send,
    relay_recv,
    plane_send,
    plane_recv,
    in_send,
    in_recv,
    pass_send,
    pass_recv,
    out_send,
    out_recv,
    half_send,
    half_recv,
    self_sem,
):
    pop, chunks, group, steps, member_rows, seqs, rank, width, full, coef, share = dims
    parts = pair_send.shape[2]
    piece = width // parts
    halves = [slice(p * piece, (p + 1) * piece) for p in range(parts)]
    rows = group * steps
    vocab = embed_ref.shape[0]
    members = ids_ref.shape[0]
    members_all = members * pop
    layers, local = fin_ref.shape[0], fin_ref.shape[1]
    columns = gout_ref.shape[2]
    mine = lax.axis_index("pop")
    me = lax.axis_index("mp")
    side, core = me // 2, me % 2
    mate = side * 2 + (1 - core)
    cross = (1 - side) * 2 + core
    diagonal = (1 - side) * 2 + (1 - core)
    others = (mate, cross, diagonal)
    blocks = (diagonal, cross, mate, me)
    outer = pop // 2
    line, twin = mine // 2, mine % 2
    buddy = line * 2 + (1 - twin)

    def at_line(place):
        return place * 2 + twin

    def peer(q, j):
        return {"pop": q, "mp": j}

    def remote(src, dst, send, recv, q, j):
        return pltpu.make_async_remote_copy(
            src_ref=src,
            dst_ref=dst,
            send_sem=send,
            recv_sem=recv,
            device_id=peer(q, j),
            device_id_type=pl.DeviceIdType.MESH,
        )

    def weight_copy(layer, slot):
        start = pl.multiple_of(blocks[slot] * width, lanes)
        return pltpu.make_async_copy(
            mix_ref.at[layer, :, pl.ds(start, width)],
            weights.at[slot],
            weight_sem.at[layer, slot],
        )

    loads = [
        pltpu.make_async_copy(src, dst, load_sem.at[i])
        for i, (src, dst) in enumerate(
            (
                (ids_hbm, ids_ref),
                (embed_hbm, embed_ref),
                (fin_hbm, fin_raw),
                (decay_hbm, decay_ref),
                (gain_hbm, gain_ref),
                (reward_hbm, reward_ref),
                (fout_hbm, fout_raw),
            )
        )
    ]
    for copy in loads[:3]:
        copy.start()
    for slot in range(4):
        weight_copy(0, slot).start()
    for copy in loads[3:]:
        copy.start()

    barrier = pltpu.get_barrier_semaphore()

    def greet(q, j):
        pl.semaphore_signal(
            barrier, inc=1, device_id=peer(q, j), device_id_type=pl.DeviceIdType.MESH
        )

    for other in others:
        greet(mine, other)
    greet(buddy, me)

    @pl.when(line < outer - 1)
    def _():
        greet(at_line(line + 1), me)

    @pl.when(line > 0)
    def _():
        greet(at_line(line - 1), me)

    def rank_block(shape, axis, repeats):
        index = lax.broadcasted_iota(jnp.int32, shape, axis)
        block = jnp.zeros(shape, jnp.int32)
        for m in range(members):
            block = jnp.where(index // repeats == m, ranks_smem[m], block)
        return block

    granks_ref[twin, line] = rank_block((8, lanes), 1, 1)

    def unpack(raw, ref):
        def one(g, carry):
            at = pl.ds(
                pl.multiple_of(g * member_rows * rank, member_rows * rank), member_rows * rank
            )
            for layer in range(layers):
                ref[layer, at, :] = jnp.concatenate(
                    [raw[layer, g * member_rows + m].astype(f32) for m in range(member_rows)],
                    axis=0,
                ).astype(bf16)
            return carry

        lax.fori_loop(0, chunks, one, 0)

    factor_rows = member_rows * rank
    mask = (lax.broadcasted_iota(jnp.int32, (factor_rows, rows), 0) // rank) == (
        (lax.broadcasted_iota(jnp.int32, (factor_rows, rows), 1) % group) // seqs
    )

    def factor_slice(ref, layer, g, start, size):
        at = pl.multiple_of(g * factor_rows, factor_rows)
        return ref[layer, pl.ds(at, factor_rows), pl.ds(start, size)]

    def small_copy(kind, g, r):
        return remote(
            small.at[kind, g, 0],
            small.at[kind, g, r + 1],
            small_send.at[kind, g, r],
            small_recv.at[kind, g, r],
            mine,
            others[r],
        )

    def small_start(kind, g):
        for r in range(3):
            small_copy(kind, g, r).start()

    def small_sum(kind, g):
        for r in range(3):
            small_copy(kind, g, r).wait_recv()
        return (small[kind, g, 0] + small[kind, g, 1]) + (small[kind, g, 2] + small[kind, g, 3])

    def against(left, features):
        return lax.dot_general(
            left, features, (((1,), (1,)), ((), ())), preferred_element_type=f32
        )

    def low_put(layer, g, local_low):
        local_low = jnp.where(mask, local_low, 0.0)
        packed = local_low[:rank]
        for at in range(rank, factor_rows, rank):
            packed = packed + local_low[at : at + rank]
        small[layer, g, 0] = packed

    def low_ready(layer, g):
        packed = small_sum(layer, g)
        low = jnp.concatenate([packed] * member_rows, axis=0)
        low = jnp.where(mask, low, 0.0) * coef
        top = low.astype(bf16).astype(f32)
        blank = jnp.zeros((lanes - 2 * factor_rows, rows), f32)
        lows[g] = jnp.concatenate([top, low - top, blank], axis=0).T.astype(bf16)

    def correction(layer, g, p):
        start = pl.multiple_of(me * width + p * piece, lanes)
        factor = factor_slice(fout_ref, layer, g, start, piece)
        right = jnp.concatenate(
            [factor, factor, jnp.zeros((lanes - 2 * factor_rows, piece), bf16)], axis=0
        )
        return jnp.dot(lows[g], right, preferred_element_type=f32)

    loads[0].wait()
    loads[1].wait()
    rows_embed[:share] = embed_ref[pl.ds(pl.multiple_of(twin * share, share), share), :]
    rows_embed[share:] = embed_ref[2 * share :]
    loads[2].wait()
    unpack(fin_raw, fin_ref)

    def begin(g, carry):
        tokens = jnp.concatenate(
            [ids_ref[g * member_rows + m] for m in range(member_rows)], axis=0
        )
        entries = lax.broadcasted_iota(jnp.int32, (group, vocab), 1)
        for t in range(steps):
            onehot_ref[g, t * group : (t + 1) * group, :] = jnp.where(
                tokens[:, t : t + 1] == entries, 1.0, 0.0
            ).astype(bf16)
        features = jnp.dot(onehot_ref[g], embed_ref[...], preferred_element_type=f32).astype(bf16)
        hidden[g] = features
        low_put(0, g, against(factor_slice(fin_ref, 0, g, 0, width), features))
        return carry

    with jax.named_scope("begin"):
        lax.fori_loop(0, chunks, begin, 0)

    def relay_copy(way, hop, source):
        return remote(
            granks_ref.at[twin, source],
            granks_ref.at[twin, source],
            relay_send.at[way, hop],
            relay_recv.at[way, hop],
            at_line(line + 1) if way == 0 else at_line(line - 1),
            me,
        )

    def relay_each(hop, act, sending):
        shift = hop - 1 if sending else hop
        right = (line >= shift) & (line < outer - 1) if sending else line >= shift
        left = (line + shift < outer) & (line > 0) if sending else line + shift < outer

        @pl.when(right)
        def _():
            act(relay_copy(0, hop, line - shift))

        @pl.when(left)
        def _():
            act(relay_copy(1, hop, line + shift))

    def relay_start(hop):
        relay_each(hop, lambda copy: copy.start(), True)

    def relay_next(hop):
        relay_each(hop, lambda copy: copy.wait_recv(), False)
        if hop + 1 < outer:
            relay_start(hop + 1)

    plane = remote(granks_ref.at[twin], granks_ref.at[twin], plane_send, plane_recv, buddy, me)
    plane_in = remote(
        granks_ref.at[1 - twin], granks_ref.at[1 - twin], plane_send, plane_recv, buddy, me
    )

    def part_copy(slot, p):
        return remote(
            own_part.at[slot, p],
            got_part.at[slot, p],
            part_send.at[slot, p],
            part_recv.at[slot, p],
            mine,
            mate,
        )

    spans = (pl.ds(0, share), pl.ds(share, vocab - 2 * share))

    def over_copy(h, p):
        return remote(
            own_over.at[p, spans[h]],
            got_over.at[p, spans[h]],
            over_send.at[h, p],
            over_recv.at[h, p],
            mine,
            cross,
        )

    def hand_copy(p, half):
        at = pl.ds(pl.multiple_of(half * share, share), share)
        return remote(
            table.at[p, at],
            table.at[p, at],
            hand_send.at[p],
            hand_recv.at[p],
            buddy,
            me,
        )

    def entry(slot, p):
        return jnp.dot(
            rows_embed[...], weights[slot, :, halves[p]], preferred_element_type=f32
        ).astype(bf16)

    def part_put(p):
        own_part[0, p] = entry(0, p)

    def part_sum(p):
        value = entry(1, p).astype(f32)
        part_copy(0, p).wait_recv()
        own_over[p] = (value + got_part[0, p].astype(f32)).astype(bf16)
        over_copy(0, p).start()

    early = 2
    with jax.named_scope("tab0"):
        weight_copy(0, 0).wait()
        for p in range(early):
            part_put(p)
    with jax.named_scope("bar"):
        pl.semaphore_wait(
            barrier,
            4 + jnp.where(line < outer - 1, 1, 0) + jnp.where(line > 0, 1, 0),
        )

    relay_start(1)
    for g in range(chunks):
        small_start(0, g)
    with jax.named_scope("tab1"):
        for p in range(early):
            part_copy(0, p).start()
        weight_copy(0, 1).wait()
        for p in range(parts):
            part_sum(p)
            if p + early < parts:
                part_put(p + early)
                part_copy(0, p + early).start()
        for p in range(parts):
            over_copy(1, p).start()
        weight_copy(1, 0).start()
        weight_copy(1, 1).start()
    with jax.named_scope("tab2"):
        weight_copy(0, 2).wait()
        for p in range(parts):
            own_part[1, p] = entry(2, p)
            part_copy(1, p).start()
        weight_copy(1, 2).start()
        weight_copy(0, 3).wait()
        for p in range(parts):
            mine_part[p] = entry(3, p)
        weight_copy(1, 3).start()

    with jax.named_scope("prep"):
        for copy in loads[3:]:
            copy.wait()
        unpack(fout_raw, fout_ref)
        reward = reward_ref[...]
        high = reward.astype(bf16).astype(f32)
        middle = (reward - high).astype(bf16).astype(f32)
        rest = reward - high - middle
        index = lax.broadcasted_iota(jnp.int32, (16, width), 0)
        heads[...] = jnp.where(
            index == 0,
            high,
            jnp.where(index == 1, middle, jnp.where(index == 2, rest, 0.0)),
        ).astype(bf16)
    with jax.named_scope("lowready"):
        for g in range(chunks):
            low_ready(0, g)
    with jax.named_scope("relay1"):
        relay_next(1)

    def both(h, p):
        at = spans[h]
        return (
            mine_part[p, at].astype(f32) + got_part[1, p, at].astype(f32)
        ) + got_over[p, at].astype(f32)

    with jax.named_scope("tabA"):
        for p in range(parts):
            over_copy(0, p).wait_recv()
            part_copy(1, p).wait_recv()
            table[p, pl.ds(pl.multiple_of(twin * share, share), share)] = both(0, p).astype(bf16)
            hand_copy(p, twin).start()
    with jax.named_scope("relay2"):
        if outer > 2:
            relay_next(2)

    def recur(layer, g, p, inputs):
        decay = decay_ref[layer : layer + 1, halves[p]]
        kept = 1.0 - decay
        carried = jnp.zeros((group, piece), f32)
        if layer:
            lean = gain_ref[layer : layer + 1, halves[p]] * reward_ref[:, halves[p]]
        for t in range(steps):
            at = slice(t * group, (t + 1) * group)
            carried = decay * carried + kept * inputs[at]
            if not layer:
                states[g, at, halves[p]] = carried
            elif t == steps - 1:
                lasts[g, :, halves[p]] = carried
            powers = carried * carried
            total = powers[:, :lanes]
            for c in range(lanes, piece, lanes):
                total = total + powers[:, c : c + lanes]
            if p:
                total = total + squares[g, at, :]
            squares[g, at, :] = total
            if layer:
                leaning = carried * lean
                total = leaning[:, :lanes]
                for c in range(lanes, piece, lanes):
                    total = total + leaning[:, c : c + lanes]
                if p:
                    total = total + leans[g, at, :]
                leans[g, at, :] = total

    def across(value):
        return jnp.sum(value.T, axis=0, keepdims=True)

    def squares_start(g):
        small[2, g, 0] = jnp.broadcast_to(across(squares[g]), (4, rows))
        small_start(2, g)

    for p in range(parts):
        with jax.named_scope("tabB%d" % p):
            over_copy(1, p).wait_recv()
            table[p, 2 * share :] = both(1, p).astype(bf16)
        with jax.named_scope("hand%d" % p):
            hand_copy(p, 1 - twin).wait_recv()
        if p == parts - 1:
            with jax.named_scope("relay3"):
                for hop in range(3, outer):
                    relay_next(hop)
                plane.start()
        with jax.named_scope("lz%d" % p):
            for g in range(chunks):
                inputs = jnp.dot(
                    onehot_ref[g], table[p], preferred_element_type=f32
                ) + correction(0, g, p)
                recur(0, g, p, inputs)
                if p == parts - 1:
                    squares_start(g)
    for slot in range(4):
        weight_copy(1, slot).wait()

    def pair_copy(g, slot, p):
        return remote(
            own_pair.at[g, slot, p],
            got_pair.at[g, slot, p],
            pair_send.at[g, slot, p],
            pair_recv.at[g, slot, p],
            mine,
            mate,
        )

    def cross_copy(g, p):
        return remote(
            own_cross.at[g, p],
            got_cross.at[g, p],
            cross_send.at[g, p],
            cross_recv.at[g, p],
            mine,
            cross,
        )

    def own_rows(q):
        return pl.ds(pl.multiple_of(q * local, local), local)

    def in_copy(hop, source):
        return remote(
            scaled,
            gin_ref.at[:, own_rows(at_line(source)), :],
            in_send.at[hop],
            in_recv.at[hop],
            at_line(lax.rem(line + hop, outer)),
            me,
        )

    def in_buddy(source):
        return remote(
            scaled,
            gin_ref.at[:, own_rows(source), :],
            in_send.at[0],
            in_recv.at[0],
            buddy,
            me,
        )

    def pass_copy(hop, side_of):
        at = own_rows(lax.rem(line + outer - hop, outer) * 2 + side_of)
        return remote(
            gin_ref.at[:, at, :],
            gin_ref.at[:, at, :],
            pass_send.at[hop],
            pass_recv.at[hop],
            buddy,
            me,
        )

    def out_copy(hop, source):
        target = lax.rem(mine + hop, pop)
        cols = pl.multiple_of(target * columns, lanes)
        return remote(
            fout_ref.at[core, :, pl.ds(cols, columns)],
            gout_ref.at[core, own_rows(source), :],
            out_send.at[hop],
            out_recv.at[hop],
            target,
            me,
        )

    def half_copy(which):
        return remote(
            gout_ref.at[which],
            gout_ref.at[which],
            half_send,
            half_recv,
            mine,
            mate,
        )

    def self_copies():
        cols = pl.multiple_of(mine * columns, lanes)
        return (
            pltpu.make_async_copy(scaled, gin_ref.at[:, own_rows(mine), :], self_sem.at[0]),
            pltpu.make_async_copy(
                fout_ref.at[core, :, pl.ds(cols, columns)],
                gout_ref.at[core, own_rows(mine), :],
                self_sem.at[1],
            ),
        )

    def shape_ranks():
        full_block = (2, outer, 8, lanes)
        kept = (lax.broadcasted_iota(jnp.int32, full_block, 2) == 0) & (
            lax.broadcasted_iota(jnp.int32, full_block, 3) < members
        )
        shares = jnp.where(kept, granks_ref[...].astype(f32) / members_all, 0.0)

        def mean_of(value):
            value = jnp.sum(value, axis=0)
            value = jnp.sum(value, axis=0)
            value = jnp.sum(value, axis=0, keepdims=True)
            return jnp.sum(value, axis=1, keepdims=True) / members_all

        rank_mean = mean_of(shares)
        apart = jnp.where(kept, shares - rank_mean[None, None], 0.0)
        spread = mean_of(apart * apart) + spread_eps
        own = rank_block((local, lanes), 0, rank).astype(f32) / members_all
        shaped = (own - rank_mean) * lax.rsqrt(spread)
        shaped = jnp.concatenate([shaped] * (width // lanes), axis=1)
        for layer in range(layers):
            scaled[layer] = (fin_ref[layer].astype(f32) * shaped).astype(bf16)

    def gather_start():
        with jax.named_scope("ranks"):
            plane_in.wait_recv()
            shape_ranks()
            in_buddy(mine).start()
            for hop in range(1, outer):
                in_copy(hop, line).start()
            for hop in range(1, pop):
                out_copy(hop, mine).start()
            for copy in self_copies():
                copy.start()

    def gather_pass(first, last):
        with jax.named_scope("pass"):
            for hop in range(first, min(last, outer)):
                in_copy(hop, lax.rem(line + outer - hop, outer)).wait_recv()
                pass_copy(hop, twin).start()

    def gather_half():
        with jax.named_scope("half"):
            for hop in range(1, pop):
                out_copy(hop, lax.rem(mine + pop - hop, pop)).wait_recv()
            for copy in self_copies():
                copy.wait()
            half_copy(core).start()

    def step_make():
        tile = 256
        with jax.named_scope("arrive"):
            in_buddy(buddy).wait_recv()
            for hop in range(1, outer):
                pass_copy(hop, 1 - twin).wait_recv()
            half_copy(1 - core).wait_recv()
        with jax.named_scope("step"):
            for layer in range(layers):
                for at in range(0, width, tile):
                    value = lax.dot_general(
                        gin_ref[layer, :, at : at + tile],
                        gout_ref[layer],
                        (((0,), (0,)), ((), ())),
                        preferred_element_type=f32,
                    )
                    step_ref[layer, at : at + tile] = value * (members_all * rank) ** (-0.5)

    def between(g):
        with jax.named_scope("normed%d" % g):
            total = small_sum(2, g)[:1]
            scale = lax.rsqrt(total / full + norm_eps)
            scale = jnp.broadcast_to(scale, (lanes, rows)).T
            scale = jnp.concatenate([scale] * (width // lanes), axis=1)
            gain = gain_ref[0:1, :]
            hidden[g] = (hidden[g].astype(f32) + states[g] * scale * gain).astype(bf16)

        def product(slot, p):
            return jnp.dot(
                hidden[g], weights[slot, :, halves[p]], preferred_element_type=f32
            ).astype(bf16)

        with jax.named_scope("exch%d" % g):
            def summed(p):
                value = product(1, p).astype(f32)
                pair_copy(g, 0, p).wait_recv()
                own_cross[g, p] = (value + got_pair[g, 0, p].astype(f32)).astype(bf16)
                cross_copy(g, p).start()

            for p in range(parts):
                own_pair[g, 0, p] = product(0, p)
                pair_copy(g, 0, p).start()
                if p:
                    summed(p - 1)
            left = jnp.concatenate([factor_slice(fin_ref, 1, g, 0, width), heads[...]], axis=0)
            local_low = against(left, hidden[g])
            low_put(1, g, local_low[:factor_rows])
            small_start(1, g)
            aligned = local_low[factor_rows : factor_rows + 8]
            alphas[g] = jnp.broadcast_to(jnp.sum(aligned, axis=0, keepdims=True), (8, rows))
            summed(parts - 1)
            if g == 0:
                gather_start()
            for p in range(parts):
                own_pair[g, 1, p] = product(2, p)
                pair_copy(g, 1, p).start()
            for p in range(parts):
                states[g, :, halves[p]] = product(3, p).astype(f32)

    def layer_one(g):
        with jax.named_scope("lowone%d" % g):
            low_ready(1, g)
        for p in range(parts):
            with jax.named_scope("l1_%d_%d" % (g, p)):
                pair_copy(g, 1, p).wait_recv()
                fixed = (
                    states[g, :, halves[p]] + got_pair[g, 1, p].astype(f32)
                ) + correction(1, g, p)
                cross_copy(g, p).wait_recv()
                recur(1, g, p, fixed + got_cross[g, p].astype(f32))
        with jax.named_scope("end%d" % g):
            small[3, g, 0] = jnp.concatenate(
                [across(squares[g]), across(leans[g]), alphas[g][:2]], axis=0
            )
            small_start(3, g)

    for g in range(chunks):
        between(g)
        if g:
            gather_pass(g, g + 1)
    for g in range(chunks):
        if g == chunks - 1:
            gather_pass(chunks, outer)
            gather_half()
            if g:
                layer_one(g - 1)
            step_make()
            layer_one(g)
        elif g < chunks - 2:
            layer_one(g)

    lane = lax.broadcasted_iota(jnp.int32, (seqs, lanes), 1)
    scores = jnp.zeros((seqs, lanes), f32)
    with jax.named_scope("final"):
        for g in range(chunks):
            sums = small_sum(3, g)
            scale = lax.rsqrt(sums[0:1] / full + norm_eps)
            value = sums[2:3] + scale * sums[1:2]
            total = value[:, :lanes]
            for c in range(lanes, rows, lanes):
                total = total + value[:, c : c + lanes]
            total = jnp.broadcast_to(total, (8, lanes))
            shift = lanes // 2
            while shift >= group:
                total = total + pltpu.roll(total, shift, 1)
                shift //= 2
            total = total * (full ** (-0.5) / steps)
            total = jnp.broadcast_to(total[:1], (lanes, lanes)).T
            for m in range(member_rows):
                scores = jnp.where(
                    lane == g * member_rows + m, total[m * seqs : (m + 1) * seqs], scores
                )
            ending = jnp.broadcast_to(scale[:, rows - lanes :], (lanes, lanes)).T[lanes - group :]
            ending = jnp.concatenate([ending] * (width // lanes), axis=1)
            gain = gain_ref[1:2, :]
            ending = (
                hidden[g, rows - group :].astype(f32) + lasts[g] * ending * gain
            ).astype(bf16).astype(f32)
            for m in range(member_rows):
                final_ref[g * member_rows + m] = ending[m * seqs : (m + 1) * seqs].astype(bf16)
        score_ref[...] = scores

    with jax.named_scope("drain"):
        for hop in range(1, outer):
            relay_each(hop, lambda copy: copy.wait_send(), True)
        plane.wait_send()
        for p in range(parts):
            for slot in range(2):
                part_copy(slot, p).wait_send()
                over_copy(slot, p).wait_send()
            hand_copy(p, twin).wait_send()
        for g in range(chunks):
            for p in range(parts):
                pair_copy(g, 0, p).wait_send()
                pair_copy(g, 1, p).wait_send()
                cross_copy(g, p).wait_send()
            for kind in range(4):
                for r in range(3):
                    small_copy(kind, g, r).wait_send()
        in_buddy(mine).wait_send()
        for hop in range(1, outer):
            in_copy(hop, line).wait_send()
            pass_copy(hop, twin).wait_send()
        for hop in range(1, pop):
            out_copy(hop, mine).wait_send()
        half_copy(core).wait_send()


cuts = 4


def publish(final_ref, marks_ref, step_ref, final_out, score_out, step_out, sems):
    copies = [pltpu.make_async_copy(final_ref, final_out, sems.at[2, 0])]
    layers, width, _ = step_ref.shape
    cut = width // cuts
    for layer in range(layers):
        for c in range(cuts):
            at = pl.ds(c * cut, cut)
            copies.append(
                pltpu.make_async_copy(
                    step_ref.at[layer, at], step_out.at[layer, at], sems.at[layer, c]
                )
            )
    for copy in copies:
        copy.start()
    score_out[...] = marks_ref[:, : score_out.shape[1]]
    for copy in copies:
        copy.wait()


def shards(
    token_ids,
    fitness_ranks,
    embedding,
    mix_weights,
    factors_in,
    factors_out,
    decay_rates,
    norm_gain,
    reward_dir,
):
    members, seqs, steps = token_ids.shape
    vocab, width = embedding.shape
    layers, _, full = mix_weights.shape
    rank = factors_in.shape[2]
    pop = lax.axis_size("pop")
    outer = pop // 2
    coef = noise_scale * (full * rank) ** (-0.5)
    columns = full // pop
    member_rows = 16 // seqs
    chunks = members // member_rows
    group = member_rows * seqs
    rows = group * steps
    local = members * rank
    share = vocab * 3 // 8
    dims = (pop, chunks, group, steps, member_rows, seqs, rank, width, full, coef, share)
    vmem = pl.BlockSpec(memory_space=pltpu.VMEM)
    smem = pl.BlockSpec(memory_space=pltpu.SMEM)
    hbm = pl.BlockSpec(memory_space=pltpu.HBM)
    parts = 4
    piece = width // parts
    entries = vocab - share
    dma = pltpu.SemaphoreType.DMA
    final_features, marks, step = pl.pallas_call(
        functools.partial(policy_kernel, dims),
        out_shape=(
            pltpu.VMEM((members, seqs, width), bf16),
            pltpu.VMEM((seqs, lanes), f32),
            pltpu.VMEM((layers, width, columns), f32),
        ),
        in_specs=[hbm, hbm, hbm, hbm, hbm, smem, hbm, hbm, hbm],
        out_specs=(vmem, vmem, vmem),
        scratch_shapes=[
            pltpu.VMEM((members, seqs, steps), jnp.int32),
            pltpu.VMEM((vocab, width), bf16),
            pltpu.VMEM((layers, members, rank, width), bf16),
            pltpu.VMEM((layers, members, rank, full), bf16),
            pltpu.VMEM((layers, width), f32),
            pltpu.VMEM((layers, width), f32),
            pltpu.VMEM((1, width), f32),
            pltpu.VMEM((4, width, width), bf16),
            pltpu.VMEM((entries, width), bf16),
            pltpu.VMEM((2, parts, entries, piece), bf16),
            pltpu.VMEM((2, parts, entries, piece), bf16),
            pltpu.VMEM((parts, entries, piece), bf16),
            pltpu.VMEM((parts, entries, piece), bf16),
            pltpu.VMEM((parts, entries, piece), bf16),
            pltpu.VMEM((parts, vocab, piece), bf16),
            pltpu.VMEM((chunks, 2, parts, rows, piece), bf16),
            pltpu.VMEM((chunks, 2, parts, rows, piece), bf16),
            pltpu.VMEM((chunks, parts, rows, piece), bf16),
            pltpu.VMEM((chunks, parts, rows, piece), bf16),
            pltpu.VMEM((chunks, rows, width), f32),
            pltpu.VMEM((chunks, rows, width), bf16),
            pltpu.VMEM((chunks, rows, vocab), bf16),
            pltpu.VMEM((layers, local, width), bf16),
            pltpu.VMEM((layers, local, full), bf16),
            pltpu.VMEM((layers, local, width), bf16),
            pltpu.VMEM((layers, pop * local, width), bf16),
            pltpu.VMEM((layers, pop * local, columns), bf16),
            pltpu.VMEM((2, outer, 8, lanes), jnp.int32),
            pltpu.VMEM((chunks, rows, lanes), bf16),
            pltpu.VMEM((chunks, rows, lanes), f32),
            pltpu.VMEM((chunks, rows, lanes), f32),
            pltpu.VMEM((chunks, group, width), f32),
            pltpu.VMEM((16, width), bf16),
            pltpu.VMEM((chunks, 8, rows), f32),
            pltpu.VMEM((4, chunks, 4, 4, rows), f32),
            dma((layers, 4)),
            dma((7,)),
            dma((2, parts)),
            dma((2, parts)),
            dma((2, parts)),
            dma((2, parts)),
            dma((parts,)),
            dma((parts,)),
            dma((chunks, 2, parts)),
            dma((chunks, 2, parts)),
            dma((chunks, parts)),
            dma((chunks, parts)),
            dma((4, chunks, 3)),
            dma((4, chunks, 3)),
            dma((2, outer)),
            dma((2, outer)),
            dma,
            dma,
            dma((outer,)),
            dma((outer,)),
            dma((outer,)),
            dma((outer,)),
            dma((pop,)),
            dma((pop,)),
            dma,
            dma,
            dma((2,)),
        ],
        compiler_params=pltpu.CompilerParams(
            collective_id=0, has_side_effects=True, vmem_limit_bytes=52 * 1024 * 1024
        ),
    )(
        *(
            pltpu.with_memory_space_constraint(value, pltpu.HBM)
            for value in (
                token_ids,
                embedding,
                mix_weights,
                factors_in,
                factors_out,
                fitness_ranks,
                decay_rates,
                norm_gain,
                reward_dir.reshape(1, width),
            )
        )
    )
    final_features, scores, weight_step = pl.pallas_call(
        publish,
        out_shape=(
            jax.ShapeDtypeStruct((members, seqs, width), bf16),
            jax.ShapeDtypeStruct((seqs, members), f32),
            jax.ShapeDtypeStruct((layers, width, columns), f32),
        ),
        in_specs=[vmem, vmem, vmem],
        out_specs=(hbm, vmem, hbm),
        scratch_shapes=[dma((3, cuts))],
        compiler_params=pltpu.CompilerParams(vmem_limit_bytes=1024 * 1024),
    )(final_features, marks, step)
    return (final_features, scores.T, weight_step)


def solution(mesh):
    return jax.shard_map(
        shards,
        mesh=mesh,
        in_specs=(
            P("pop", None, None),
            P("pop"),
            P(None, "mp"),
            P(None, "mp", None),
            P(None, "pop", None, "mp"),
            P(None, "pop", None, None),
            P(None, "mp"),
            P(None, "mp"),
            P("mp"),
        ),
        out_specs=(P("pop", None, "mp"), P("pop", None), P(None, "mp", "pop")),
        check_vma=False,
    )
```

```python
import functools

import jax
import jax.numpy as jnp
from jax import lax
from jax.experimental import pallas as pl
from jax.experimental.pallas import tpu as pltpu
from jax.sharding import PartitionSpec as P

noise_scale = 0.25
norm_eps = 1e-06
spread_eps = 1e-05
lanes = 128
f32, bf16 = jnp.float32, jnp.bfloat16


def policy_kernel(
    dims,
    ids_hbm,
    embed_hbm,
    mix_ref,
    fin_hbm,
    fout_hbm,
    ranks_smem,
    decay_hbm,
    gain_hbm,
    reward_hbm,
    final_ref,
    score_ref,
    step_ref,
    ids_ref,
    embed_ref,
    fin_raw,
    fout_raw,
    decay_ref,
    gain_ref,
    reward_ref,
    weights,
    rows_embed,
    own_part,
    got_part,
    own_over,
    got_over,
    mine_part,
    table,
    own_pair,
    got_pair,
    own_cross,
    got_cross,
    own_lead,
    got_lead,
    own_ahead,
    got_ahead,
    lifted,
    lead_scale,
    states,
    hidden,
    onehot_ref,
    fin_ref,
    fout_ref,
    scaled,
    gin_ref,
    gout_ref,
    granks_ref,
    lows,
    squares,
    leans,
    lasts,
    heads,
    alphas,
    small,
    weight_sem,
    column_sem,
    load_sem,
    part_send,
    part_recv,
    over_send,
    over_recv,
    hand_send,
    hand_recv,
    pair_send,
    pair_recv,
    cross_send,
    cross_recv,
    lead_send,
    lead_recv,
    ahead_send,
    ahead_recv,
    small_send,
    small_recv,
    relay_send,
    relay_recv,
    plane_send,
    plane_recv,
    in_send,
    in_recv,
    pass_send,
    pass_recv,
    out_send,
    out_recv,
    half_send,
    half_recv,
    self_sem,
):
    pop, chunks, group, steps, member_rows, seqs, rank, width, full, coef, share = dims
    parts = cross_recv.shape[1]
    piece = width // parts
    halves = [slice(p * piece, (p + 1) * piece) for p in range(parts)]
    rows = group * steps
    vocab = embed_ref.shape[0]
    members = ids_ref.shape[0]
    members_all = members * pop
    layers, local = fin_ref.shape[0], fin_ref.shape[1]
    columns = gout_ref.shape[2]
    mine = lax.axis_index("pop")
    me = lax.axis_index("mp")
    side, core = me // 2, me % 2
    mate = side * 2 + (1 - core)
    cross = (1 - side) * 2 + core
    diagonal = (1 - side) * 2 + (1 - core)
    others = (mate, cross, diagonal)
    blocks = (diagonal, cross, mate, me)
    outer = pop // 2
    line, twin = mine // 2, mine % 2
    buddy = line * 2 + (1 - twin)

    def at_line(place):
        return place * 2 + twin

    def peer(q, j):
        return {"pop": q, "mp": j}

    def remote(src, dst, send, recv, q, j):
        return pltpu.make_async_remote_copy(
            src_ref=src,
            dst_ref=dst,
            send_sem=send,
            recv_sem=recv,
            device_id=peer(q, j),
            device_id_type=pl.DeviceIdType.MESH,
        )

    barrier = pltpu.get_barrier_semaphore()

    def greet(q, j):
        pl.semaphore_signal(
            barrier, inc=1, device_id=peer(q, j), device_id_type=pl.DeviceIdType.MESH
        )

    for other in others:
        greet(mine, other)
    greet(buddy, me)

    @pl.when(line < outer - 1)
    def _():
        greet(at_line(line + 1), me)

    @pl.when(line > 0)
    def _():
        greet(at_line(line - 1), me)

    def weight_copy(layer, slot):
        start = pl.multiple_of(blocks[slot] * width, lanes)
        return pltpu.make_async_copy(
            mix_ref.at[layer, :, pl.ds(start, width)],
            weights.at[slot],
            weight_sem.at[2 if layer else slot - 2],
        )

    def column_copy(slot, p):
        start = pl.multiple_of(blocks[slot] * width + p * piece, lanes)
        return pltpu.make_async_copy(
            mix_ref.at[0, :, pl.ds(start, piece)],
            weights.at[slot, :, halves[p]],
            column_sem.at[slot, p],
        )

    loads = [
        pltpu.make_async_copy(src, dst, load_sem.at[i])
        for i, (src, dst) in enumerate(
            (
                (embed_hbm, embed_ref),
                (ids_hbm, ids_ref),
                (fin_hbm, fin_raw),
                (decay_hbm, decay_ref),
                (gain_hbm, gain_ref),
                (reward_hbm, reward_ref),
                (fout_hbm, fout_raw),
            )
        )
    ]
    loads[0].start()
    for slot in range(2):
        for p in range(parts):
            column_copy(slot, p).start()
    for copy in loads[1:3]:
        copy.start()
    weight_copy(0, 2).start()
    weight_copy(0, 3).start()
    for copy in loads[3:]:
        copy.start()

    def rank_block(shape, axis, repeats):
        index = lax.broadcasted_iota(jnp.int32, shape, axis)
        block = jnp.zeros(shape, jnp.int32)
        for m in range(members):
            block = jnp.where(index // repeats == m, ranks_smem[m], block)
        return block

    granks_ref[twin, line] = rank_block((8, lanes), 1, 1)

    def unpack(raw, ref):
        def one(g, carry):
            at = pl.ds(
                pl.multiple_of(g * member_rows * rank, member_rows * rank), member_rows * rank
            )
            for layer in range(layers):
                ref[layer, at, :] = jnp.concatenate(
                    [raw[layer, g * member_rows + m].astype(f32) for m in range(member_rows)],
                    axis=0,
                ).astype(bf16)
            return carry

        lax.fori_loop(0, chunks, one, 0)

    factor_rows = member_rows * rank
    mask = (lax.broadcasted_iota(jnp.int32, (factor_rows, rows), 0) // rank) == (
        (lax.broadcasted_iota(jnp.int32, (factor_rows, rows), 1) % group) // seqs
    )

    def factor_slice(ref, layer, g, start, size):
        at = pl.multiple_of(g * factor_rows, factor_rows)
        return ref[layer, pl.ds(at, factor_rows), pl.ds(start, size)]

    def small_copy(kind, g, r):
        return remote(
            small.at[kind, g, 0],
            small.at[kind, g, r + 1],
            small_send,
            small_recv.at[kind, g],
            mine,
            others[r],
        )

    def small_start(kind, g):
        for r in range(3):
            small_copy(kind, g, r).start()

    def small_sum(kind, g):
        arrived = small.at[kind, g, pl.ds(1, 3)]
        remote(arrived, arrived, small_send, small_recv.at[kind, g], mine, mate).wait_recv()
        return (small[kind, g, 0] + small[kind, g, 1]) + (small[kind, g, 2] + small[kind, g, 3])

    def against(left, features):
        return lax.dot_general(
            left, features, (((1,), (1,)), ((), ())), preferred_element_type=f32
        )

    def low_put(layer, g, local_low):
        local_low = jnp.where(mask, local_low, 0.0)
        packed = local_low[:rank]
        for at in range(rank, factor_rows, rank):
            packed = packed + local_low[at : at + rank]
        small[layer, g, 0] = packed

    def low_ready(layer, g):
        packed = small_sum(layer, g)
        low = jnp.concatenate([packed] * member_rows, axis=0)
        low = jnp.where(mask, low, 0.0) * coef
        top = low.astype(bf16).astype(f32)
        blank = jnp.zeros((lanes - 2 * factor_rows, rows), f32)
        lows[g] = jnp.concatenate([top, low - top, blank], axis=0).T.astype(bf16)

    def correction(layer, g, p):
        start = pl.multiple_of(me * width + p * piece, lanes)
        factor = factor_slice(fout_ref, layer, g, start, piece)
        right = jnp.concatenate(
            [factor, factor, jnp.zeros((lanes - 2 * factor_rows, piece), bf16)], axis=0
        )
        return jnp.dot(lows[g], right, preferred_element_type=f32)

    loads[0].wait()
    rows_embed[:share] = embed_ref[pl.ds(pl.multiple_of(twin * share, share), share), :]
    rows_embed[share:] = embed_ref[2 * share :]
    def relay_copy(way, hop, source):
        return remote(
            granks_ref.at[twin, source],
            granks_ref.at[twin, source],
            relay_send.at[way, hop - 1],
            relay_recv.at[way, hop - 1],
            at_line(line + 1) if way == 0 else at_line(line - 1),
            me,
        )

    def relay_each(hop, act, sending):
        shift = hop - 1 if sending else hop
        right = (line >= shift) & (line < outer - 1) if sending else line >= shift
        left = (line + shift < outer) & (line > 0) if sending else line + shift < outer

        @pl.when(right)
        def _():
            act(relay_copy(0, hop, line - shift))

        @pl.when(left)
        def _():
            act(relay_copy(1, hop, line + shift))

    def relay_start(hop):
        relay_each(hop, lambda copy: copy.start(), True)

    def relay_next(hop):
        relay_each(hop, lambda copy: copy.wait_recv(), False)
        if hop + 1 < outer:
            relay_start(hop + 1)

    plane = remote(granks_ref.at[twin], granks_ref.at[twin], plane_send, plane_recv, buddy, me)
    plane_in = remote(
        granks_ref.at[1 - twin], granks_ref.at[1 - twin], plane_send, plane_recv, buddy, me
    )

    def part_copy(slot, p):
        return remote(
            own_part.at[slot, p],
            got_part.at[slot, p],
            part_send,
            part_recv.at[parts if slot else p],
            mine,
            mate,
        )

    def whole_part(slot):
        return remote(
            own_part.at[slot], got_part.at[slot], part_send, part_recv.at[parts], mine, mate
        )

    spans = (pl.ds(0, share), pl.ds(share, vocab - 2 * share))

    def over_copy(h, p):
        return remote(
            own_over.at[p, spans[h]],
            got_over.at[p, spans[h]],
            over_send,
            over_recv.at[h, p],
            mine,
            cross,
        )

    def hand_copy(p, half):
        at = pl.ds(pl.multiple_of(half * share, share), share)
        return remote(
            table.at[p, at],
            table.at[p, at],
            hand_send,
            hand_recv.at[p],
            buddy,
            me,
        )

    def entry(slot, p):
        return jnp.dot(
            rows_embed[...], weights[slot, :, halves[p]], preferred_element_type=f32
        ).astype(bf16)

    def part_put(p):
        column_copy(0, p).wait()
        own_part[0, p] = entry(0, p)

    def part_sum(p):
        column_copy(1, p).wait()
        value = entry(1, p).astype(f32)
        part_copy(0, p).wait_recv()
        own_over[p] = (value + got_part[0, p].astype(f32)).astype(bf16)
        over_copy(0, p).start()

    early = 2
    with jax.named_scope("tab0"):
        for p in range(early):
            part_put(p)
    with jax.named_scope("bar"):
        pl.semaphore_wait(
            barrier,
            4 + jnp.where(line < outer - 1, 1, 0) + jnp.where(line > 0, 1, 0),
        )

    relay_start(1)
    with jax.named_scope("tab1"):
        for p in range(early):
            part_copy(0, p).start()
        for p in range(early, parts):
            part_put(p)
            part_copy(0, p).start()
        for p in range(parts):
            part_sum(p)
        weight_copy(1, 0).start()
        weight_copy(1, 1).start()
    loads[1].wait()
    loads[2].wait()
    unpack(fin_raw, fin_ref)

    def begin(g, carry):
        tokens = jnp.concatenate(
            [ids_ref[g * member_rows + m] for m in range(member_rows)], axis=0
        )
        entries = lax.broadcasted_iota(jnp.int32, (group, vocab), 1)
        for t in range(steps):
            onehot_ref[g, t * group : (t + 1) * group, :] = jnp.where(
                tokens[:, t : t + 1] == entries, 1.0, 0.0
            ).astype(bf16)
        features = jnp.dot(onehot_ref[g], embed_ref[...], preferred_element_type=f32).astype(bf16)
        hidden[g] = features
        low_put(0, g, against(factor_slice(fin_ref, 0, g, 0, width), features))
        return carry

    with jax.named_scope("begin"):
        lax.fori_loop(0, chunks, begin, 0)

    for g in range(chunks):
        small_start(0, g)
    for p in range(parts):
        over_copy(1, p).start()
    with jax.named_scope("relay1"):
        relay_next(1)
    with jax.named_scope("tab2"):
        weight_copy(0, 2).wait()
        for p in range(parts):
            own_part[1, p] = entry(2, p)
            part_copy(1, p).start()
        weight_copy(1, 2).start()
        weight_copy(0, 3).wait()
        for p in range(parts):
            mine_part[p] = entry(3, p)
        weight_copy(1, 3).start()

    with jax.named_scope("prep"):
        for copy in loads[3:]:
            copy.wait()
        unpack(fout_raw, fout_ref)
        reward = reward_ref[...]
        high = reward.astype(bf16).astype(f32)
        middle = (reward - high).astype(bf16).astype(f32)
        rest = reward - high - middle
        index = lax.broadcasted_iota(jnp.int32, (16, width), 0)
        heads[...] = jnp.where(
            index == 0,
            high,
            jnp.where(index == 1, middle, jnp.where(index == 2, rest, 0.0)),
        ).astype(bf16)

    def both(h, p):
        at = spans[h]
        return (
            mine_part[p, at].astype(f32) + got_part[1, p, at].astype(f32)
        ) + got_over[p, at].astype(f32)

    lead = lifted.shape[0]

    def lead_pair(k, p):
        return remote(
            own_lead.at[k, p],
            got_lead.at[k, p],
            lead_send,
            lead_recv.at[1 + p if k else 0],
            mine,
            mate,
        )

    def whole_lead():
        return remote(own_lead.at[0], got_lead.at[0], lead_send, lead_recv.at[0], mine, mate)

    def lead_cross(k, p):
        return remote(
            own_ahead.at[k, p], got_ahead.at[k, p], ahead_send, ahead_recv, mine, cross
        )

    def lead_rows(k):
        return lifted[...] if k else hidden[0, :lead]

    def lead_put(k, p):
        if k == 0 and p == 0:
            wait_weights()
        own_lead[k, p] = jnp.dot(
            lead_rows(k), weights[0, :, halves[p]], preferred_element_type=f32
        ).astype(bf16)
        lead_pair(k, p).start()

    def lead_sum(k, p):
        value = (
            jnp.dot(lead_rows(k), weights[1, :, halves[p]], preferred_element_type=f32)
            .astype(bf16)
            .astype(f32)
        )
        if k:
            lead_pair(k, p).wait_recv()
        own_ahead[k, p] = (value + got_lead[k, p].astype(f32)).astype(bf16)
        lead_cross(k, p).start()

    def wait_weights():
        pltpu.make_async_copy(weights, weights, weight_sem.at[2]).wait()

    with jax.named_scope("tabA"):
        for p in range(parts):
            over_copy(0, p).wait_recv()
            if p == 0:
                whole_part(1).wait_recv()
            table[p, pl.ds(pl.multiple_of(twin * share, share), share)] = both(0, p).astype(bf16)
            hand_copy(p, twin).start()
            lead_put(0, p)
            if p == 1 and outer > 2:
                relay_next(2)
    with jax.named_scope("lowready"):
        for g in range(chunks):
            low_ready(0, g)

    def recur(layer, g, p, inputs):
        decay = decay_ref[layer : layer + 1, halves[p]]
        kept = 1.0 - decay
        carried = jnp.zeros((group, piece), f32)
        if layer:
            lean = gain_ref[layer : layer + 1, halves[p]] * reward_ref[:, halves[p]]
        for t in range(steps):
            at = slice(t * group, (t + 1) * group)
            carried = decay * carried + kept * inputs[at]
            if not layer:
                states[g, at, halves[p]] = carried
            elif t == steps - 1:
                lasts[g, :, halves[p]] = carried
            powers = carried * carried
            total = powers[:, :lanes]
            for c in range(lanes, piece, lanes):
                total = total + powers[:, c : c + lanes]
            if p:
                total = total + squares[g, at, :]
            squares[g, at, :] = total
            if layer:
                leaning = carried * lean
                total = leaning[:, :lanes]
                for c in range(lanes, piece, lanes):
                    total = total + leaning[:, c : c + lanes]
                if p:
                    total = total + leans[g, at, :]
                leans[g, at, :] = total

    def across(value):
        return jnp.sum(value.T, axis=0, keepdims=True)

    def squares_start(g):
        small[2, g, 0] = jnp.broadcast_to(across(squares[g]), (4, rows))
        small_start(2, g)

    for p in range(parts):
        with jax.named_scope("tabB%d" % p):
            over_copy(1, p).wait_recv()
            table[p, 2 * share :] = both(1, p).astype(bf16)
        with jax.named_scope("lead%d" % p):
            if p == 0:
                whole_lead().wait_recv()
            lead_sum(0, p)
        with jax.named_scope("hand%d" % p):
            hand_copy(p, 1 - twin).wait_recv()
        if p == 0:
            with jax.named_scope("relay3"):
                for hop in range(3, outer):
                    relay_next(hop)
                plane.start()
        with jax.named_scope("lz%d" % p):
            for g in range(chunks):
                inputs = jnp.dot(
                    onehot_ref[g], table[p], preferred_element_type=f32
                ) + correction(0, g, p)
                recur(0, g, p, inputs)
                if p == parts - 1:
                    squares_start(g)
                    if g == 0:
                        with jax.named_scope("leadv"):
                            lift = states[0, :lead] * gain_ref[0:1, :]
                            lifted[...] = lift.astype(bf16)
                            for q in range(parts):
                                lead_put(1, q)
                            for q in range(parts):
                                lead_sum(1, q)
    def pair_copy(g, slot, p):
        return remote(
            own_pair.at[g, slot, p],
            got_pair.at[g, slot, p],
            pair_send,
            pair_recv.at[g, parts if slot else p],
            mine,
            mate,
        )

    def whole_pair(g):
        return remote(
            own_pair.at[g, 1], got_pair.at[g, 1], pair_send, pair_recv.at[g, parts], mine, mate
        )

    def cross_copy(g, p):
        at = pl.ds(0 if g else lead, rows if g else rows - lead)
        return remote(
            own_cross.at[g, p, at],
            got_cross.at[g, p, at],
            cross_send.at[1 if g else 0],
            cross_recv.at[g, p],
            mine,
            cross,
        )

    def own_rows(q):
        return pl.ds(pl.multiple_of(q * local, local), local)

    def in_copy(hop, source):
        return remote(
            scaled,
            gin_ref.at[:, own_rows(at_line(source)), :],
            in_send,
            in_recv.at[hop],
            at_line(lax.rem(line + hop, outer)),
            me,
        )

    def in_buddy(source):
        return remote(
            scaled,
            gin_ref.at[:, own_rows(source), :],
            in_send,
            in_recv.at[0],
            buddy,
            me,
        )

    def pass_copy(hop, side_of):
        at = own_rows(lax.rem(line + outer - hop, outer) * 2 + side_of)
        return remote(
            gin_ref.at[:, at, :],
            gin_ref.at[:, at, :],
            pass_send,
            pass_recv,
            buddy,
            me,
        )

    def out_copy(hop, source):
        target = lax.rem(mine + hop, pop)
        cols = pl.multiple_of(target * columns, lanes)
        return remote(
            fout_ref.at[core, :, pl.ds(cols, columns)],
            gout_ref.at[core, own_rows(source), :],
            out_send,
            out_recv,
            target,
            me,
        )

    def stretch(ref, count):
        return ref.at[pl.ds(0, count * local), :]

    def whole_out():
        spot = stretch(gout_ref.at[core], pop - 1)
        return remote(spot, spot, out_send, out_recv, buddy, me)

    def whole_pass():
        spot = gin_ref.at[:, pl.ds(0, (outer - 1) * local), :]
        return remote(spot, spot, pass_send, pass_recv, buddy, me)

    def whole_in():
        spot = gin_ref.at[:, pl.ds(0, outer * local), :]
        return remote(spot, spot, in_send, in_recv.at[0], buddy, me)

    def half_copy(which):
        return remote(
            gout_ref.at[which],
            gout_ref.at[which],
            half_send,
            half_recv,
            mine,
            mate,
        )

    def self_copies():
        cols = pl.multiple_of(mine * columns, lanes)
        return (
            pltpu.make_async_copy(scaled, gin_ref.at[:, own_rows(mine), :], self_sem.at[0]),
            pltpu.make_async_copy(
                fout_ref.at[core, :, pl.ds(cols, columns)],
                gout_ref.at[core, own_rows(mine), :],
                self_sem.at[1],
            ),
        )

    def shape_ranks():
        full_block = (2, outer, 8, lanes)
        kept = (lax.broadcasted_iota(jnp.int32, full_block, 2) == 0) & (
            lax.broadcasted_iota(jnp.int32, full_block, 3) < members
        )
        shares = jnp.where(kept, granks_ref[...].astype(f32) / members_all, 0.0)

        def mean_of(value):
            value = jnp.sum(value, axis=0)
            value = jnp.sum(value, axis=0)
            value = jnp.sum(value, axis=0, keepdims=True)
            return jnp.sum(value, axis=1, keepdims=True) / members_all

        rank_mean = mean_of(shares)
        apart = jnp.where(kept, shares - rank_mean[None, None], 0.0)
        spread = mean_of(apart * apart) + spread_eps
        own = rank_block((local, lanes), 0, rank).astype(f32) / members_all
        shaped = (own - rank_mean) * lax.rsqrt(spread)
        shaped = jnp.concatenate([shaped] * (width // lanes), axis=1)
        for layer in range(layers):
            scaled[layer] = (fin_ref[layer].astype(f32) * shaped).astype(bf16)

    def gather_start():
        with jax.named_scope("ranks"):
            plane_in.wait_recv()
            shape_ranks()
            in_buddy(mine).start()
            for hop in range(1, outer):
                in_copy(hop, line).start()
            for hop in range(1, pop):
                out_copy(hop, mine).start()
            for copy in self_copies():
                copy.start()

    def gather_pass(first, last):
        with jax.named_scope("pass"):
            for hop in range(first, min(last, outer)):
                in_copy(hop, lax.rem(line + outer - hop, outer)).wait_recv()
                pass_copy(hop, twin).start()

    def gather_half():
        with jax.named_scope("half"):
            whole_out().wait_recv()
            for copy in self_copies():
                copy.wait()
            half_copy(core).start()

    def step_make():
        tile = 256
        with jax.named_scope("arrive"):
            in_buddy(buddy).wait_recv()
        with jax.named_scope("arrive_pass"):
            whole_pass().wait_recv()
        with jax.named_scope("arrive_half"):
            half_copy(1 - core).wait_recv()
        with jax.named_scope("step"):
            for layer in range(layers):
                for at in range(0, width, tile):
                    value = lax.dot_general(
                        gin_ref[layer, :, at : at + tile],
                        gout_ref[layer],
                        (((0,), (0,)), ((), ())),
                        preferred_element_type=f32,
                    )
                    step_ref[layer, at : at + tile] = value * (members_all * rank) ** (-0.5)

    def between(g):
        with jax.named_scope("normed%d" % g):
            total = small_sum(2, g)[:1]
            scale = lax.rsqrt(total / full + norm_eps)
            scale = jnp.broadcast_to(scale, (lanes, rows)).T
            if g == 0:
                lead_scale[...] = scale[:lead]
            scale = jnp.concatenate([scale] * (width // lanes), axis=1)
            gain = gain_ref[0:1, :]
            hidden[g] = (hidden[g].astype(f32) + states[g] * scale * gain).astype(bf16)

        def product(slot, p):
            return jnp.dot(
                hidden[g], weights[slot, :, halves[p]], preferred_element_type=f32
            ).astype(bf16)

        with jax.named_scope("exch%d" % g):
            def summed(p):
                value = product(1, p).astype(f32)
                pair_copy(g, 0, p).wait_recv()
                total = (value + got_pair[g, 0, p].astype(f32)).astype(bf16)
                if g:
                    own_cross[g, p] = total
                else:
                    own_cross[g, p, lead:] = total[lead:]
                cross_copy(g, p).start()

            for p in range(parts):
                own_pair[g, 0, p] = product(0, p)
                pair_copy(g, 0, p).start()
                if p:
                    summed(p - 1)
            left = jnp.concatenate([factor_slice(fin_ref, 1, g, 0, width), heads[...]], axis=0)
            local_low = against(left, hidden[g])
            low_put(1, g, local_low[:factor_rows])
            small_start(1, g)
            aligned = local_low[factor_rows : factor_rows + 8]
            alphas[g] = jnp.broadcast_to(jnp.sum(aligned, axis=0, keepdims=True), (8, rows))
            summed(parts - 1)
            for p in range(parts):
                own_pair[g, 1, p] = product(2, p)
                pair_copy(g, 1, p).start()
            for p in range(parts):
                states[g, :, halves[p]] = product(3, p).astype(f32)

    def layer_one(g):
        with jax.named_scope("lowone%d" % g):
            low_ready(1, g)
        for p in range(parts):
            with jax.named_scope("l1_%d_%d" % (g, p)):
                if p == 0:
                    whole_pair(g).wait_recv()
                fixed = (
                    states[g, :, halves[p]] + got_pair[g, 1, p].astype(f32)
                ) + correction(1, g, p)
                cross_copy(g, p).wait_recv()
                if g:
                    other = got_cross[g, p].astype(f32)
                else:
                    if p == 0:
                        remote(
                            own_ahead, got_ahead, ahead_send, ahead_recv, mine, cross
                        ).wait_recv()
                    scale = jnp.concatenate([lead_scale[...]] * (piece // lanes), axis=1)
                    other = got_ahead[0, p].astype(f32) + scale * got_ahead[1, p].astype(f32)
                    other = jnp.concatenate([other, got_cross[0, p, lead:].astype(f32)], axis=0)
                recur(1, g, p, fixed + other)
        with jax.named_scope("end%d" % g):
            small[3, g, 0] = jnp.concatenate(
                [across(squares[g]), across(leans[g]), alphas[g][:2]], axis=0
            )
            small_start(3, g)

    gather_start()
    for g in range(chunks):
        between(g)
        if g:
            gather_pass(g, g + 1)
    for g in range(chunks):
        if g == chunks - 1:
            gather_pass(chunks, outer)
            gather_half()
            if g:
                layer_one(g - 1)
            step_make()
            layer_one(g)
        elif g < chunks - 2:
            layer_one(g)

    lane = lax.broadcasted_iota(jnp.int32, (seqs, lanes), 1)
    scores = jnp.zeros((seqs, lanes), f32)
    with jax.named_scope("final"):
        for g in range(chunks):
            sums = small_sum(3, g)
            scale = lax.rsqrt(sums[0:1] / full + norm_eps)
            value = sums[2:3] + scale * sums[1:2]
            total = value[:, :lanes]
            for c in range(lanes, rows, lanes):
                total = total + value[:, c : c + lanes]
            total = jnp.broadcast_to(total, (8, lanes))
            shift = lanes // 2
            while shift >= group:
                total = total + pltpu.roll(total, shift, 1)
                shift //= 2
            total = total * (full ** (-0.5) / steps)
            total = jnp.broadcast_to(total[:1], (lanes, lanes)).T
            for m in range(member_rows):
                scores = jnp.where(
                    lane == g * member_rows + m, total[m * seqs : (m + 1) * seqs], scores
                )
            ending = jnp.broadcast_to(scale[:, rows - lanes :], (lanes, lanes)).T[lanes - group :]
            ending = jnp.concatenate([ending] * (width // lanes), axis=1)
            gain = gain_ref[1:2, :]
            ending = (
                hidden[g, rows - group :].astype(f32) + lasts[g] * ending * gain
            ).astype(bf16).astype(f32)
            for m in range(member_rows):
                final_ref[g * member_rows + m] = ending[m * seqs : (m + 1) * seqs].astype(bf16)
        score_ref[...] = scores[:, :members]

    with jax.named_scope("drain"):
        for hop in range(1, outer):
            relay_each(hop, lambda copy: copy.wait_send(), True)
        plane.wait_send()
        remote(own_part, got_part, part_send, part_recv.at[0], mine, mate).wait_send()
        remote(own_over, got_over, over_send, over_recv.at[0, 0], mine, cross).wait_send()
        spot = table.at[:, pl.ds(0, share)]
        remote(spot, spot, hand_send, hand_recv.at[0], buddy, me).wait_send()
        remote(own_pair, got_pair, pair_send, pair_recv.at[0, 0], mine, mate).wait_send()
        spot = own_cross.at[0, :, pl.ds(lead, rows - lead)]
        remote(spot, spot, cross_send.at[0], cross_recv.at[0, 0], mine, cross).wait_send()
        if chunks > 1:
            spot = own_cross.at[pl.ds(1, chunks - 1)]
            remote(spot, spot, cross_send.at[1], cross_recv.at[0, 0], mine, cross).wait_send()
        remote(own_lead, got_lead, lead_send, lead_recv.at[0], mine, mate).wait_send()
        remote(own_ahead, got_ahead, ahead_send, ahead_recv, mine, cross).wait_send()
        spot = small.at[:, :, pl.ds(1, 3)]
        remote(spot, spot, small_send, small_recv.at[0, 0], mine, mate).wait_send()
        whole_in().wait_send()
        whole_pass().wait_send()
        whole_out().wait_send()
        half_copy(core).wait_send()


cuts = 4


def publish(final_ref, score_ref, step_ref, final_out, score_out, step_out, sems):
    copies = []
    layers, width, _ = step_ref.shape
    cut = width // cuts
    for layer in range(layers):
        for c in range(cuts):
            at = pl.ds(c * cut, cut)
            copies.append(
                pltpu.make_async_copy(
                    step_ref.at[layer, at], step_out.at[layer, at], sems.at[layer, c]
                )
            )
    copies.append(pltpu.make_async_copy(final_ref, final_out, sems.at[layers, 0]))
    copies.append(pltpu.make_async_copy(score_ref, score_out, sems.at[layers, 1]))
    for copy in copies:
        copy.start()
    for copy in copies:
        copy.wait()


def shards(
    token_ids,
    fitness_ranks,
    embedding,
    mix_weights,
    factors_in,
    factors_out,
    decay_rates,
    norm_gain,
    reward_dir,
):
    members, seqs, steps = token_ids.shape
    vocab, width = embedding.shape
    layers, _, full = mix_weights.shape
    rank = factors_in.shape[2]
    pop = lax.axis_size("pop")
    outer = pop // 2
    coef = noise_scale * (full * rank) ** (-0.5)
    columns = full // pop
    member_rows = 16 // seqs
    chunks = members // member_rows
    group = member_rows * seqs
    rows = group * steps
    local = members * rank
    share = vocab * 3 // 8
    lead = rows * 3 // 8
    dims = (pop, chunks, group, steps, member_rows, seqs, rank, width, full, coef, share)
    vmem = pl.BlockSpec(memory_space=pltpu.VMEM)
    smem = pl.BlockSpec(memory_space=pltpu.SMEM)
    hbm = pl.BlockSpec(memory_space=pltpu.HBM)
    parts = 4
    piece = width // parts
    entries = vocab - share
    dma = pltpu.SemaphoreType.DMA
    final_features, scores, step = pl.pallas_call(
        functools.partial(policy_kernel, dims),
        out_shape=(
            pltpu.VMEM((members, seqs, width), bf16),
            pltpu.VMEM((seqs, members), f32),
            pltpu.VMEM((layers, width, columns), f32),
        ),
        in_specs=[hbm, hbm, hbm, hbm, hbm, smem, hbm, hbm, hbm],
        out_specs=(vmem, vmem, vmem),
        scratch_shapes=[
            pltpu.VMEM((members, seqs, steps), jnp.int32),
            pltpu.VMEM((vocab, width), bf16),
            pltpu.VMEM((layers, members, rank, width), bf16),
            pltpu.VMEM((layers, members, rank, full), bf16),
            pltpu.VMEM((layers, width), f32),
            pltpu.VMEM((layers, width), f32),
            pltpu.VMEM((1, width), f32),
            pltpu.VMEM((4, width, width), bf16),
            pltpu.VMEM((entries, width), bf16),
            pltpu.VMEM((2, parts, entries, piece), bf16),
            pltpu.VMEM((2, parts, entries, piece), bf16),
            pltpu.VMEM((parts, entries, piece), bf16),
            pltpu.VMEM((parts, entries, piece), bf16),
            pltpu.VMEM((parts, entries, piece), bf16),
            pltpu.VMEM((parts, vocab, piece), bf16),
            pltpu.VMEM((chunks, 2, parts, rows, piece), bf16),
            pltpu.VMEM((chunks, 2, parts, rows, piece), bf16),
            pltpu.VMEM((chunks, parts, rows, piece), bf16),
            pltpu.VMEM((chunks, parts, rows, piece), bf16),
            pltpu.VMEM((2, parts, lead, piece), bf16),
            pltpu.VMEM((2, parts, lead, piece), bf16),
            pltpu.VMEM((2, parts, lead, piece), bf16),
            pltpu.VMEM((2, parts, lead, piece), bf16),
            pltpu.VMEM((lead, width), bf16),
            pltpu.VMEM((lead, lanes), f32),
            pltpu.VMEM((chunks, rows, width), f32),
            pltpu.VMEM((chunks, rows, width), bf16),
            pltpu.VMEM((chunks, rows, vocab), bf16),
            pltpu.VMEM((layers, local, width), bf16),
            pltpu.VMEM((layers, local, full), bf16),
            pltpu.VMEM((layers, local, width), bf16),
            pltpu.VMEM((layers, pop * local, width), bf16),
            pltpu.VMEM((layers, pop * local, columns), bf16),
            pltpu.VMEM((2, outer, 8, lanes), jnp.int32),
            pltpu.VMEM((chunks, rows, lanes), bf16),
            pltpu.VMEM((chunks, rows, lanes), f32),
            pltpu.VMEM((chunks, rows, lanes), f32),
            pltpu.VMEM((chunks, group, width), f32),
            pltpu.VMEM((16, width), bf16),
            pltpu.VMEM((chunks, 8, rows), f32),
            pltpu.VMEM((4, chunks, 4, 4, rows), f32),
            dma((3,)),
            dma((2, parts)),
            dma((7,)),
            dma,
            dma((parts + 1,)),
            dma,
            dma((2, parts)),
            dma,
            dma((parts,)),
            dma,
            dma((chunks, parts + 1)),
            dma((2,)),
            dma((chunks, parts)),
            dma,
            dma((parts + 1,)),
            dma,
            dma,
            dma,
            dma((4, chunks)),
            dma((2, outer - 1)),
            dma((2, outer - 1)),
            dma,
            dma,
            dma,
            dma((outer,)),
            dma,
            dma,
            dma,
            dma,
            dma,
            dma,
            dma((2,)),
        ],
        compiler_params=pltpu.CompilerParams(
            collective_id=0, has_side_effects=True, vmem_limit_bytes=52 * 1024 * 1024
        ),
    )(
        *(
            pltpu.with_memory_space_constraint(value, pltpu.HBM)
            for value in (
                token_ids,
                embedding,
                mix_weights,
                factors_in,
                factors_out,
                fitness_ranks,
                decay_rates,
                norm_gain,
                reward_dir.reshape(1, width),
            )
        )
    )
    final_features, scores, weight_step = pl.pallas_call(
        publish,
        out_shape=(
            jax.ShapeDtypeStruct((members, seqs, width), bf16),
            jax.ShapeDtypeStruct((seqs, members), f32),
            jax.ShapeDtypeStruct((layers, width, columns), f32),
        ),
        in_specs=[vmem, vmem, vmem],
        out_specs=(hbm, hbm, hbm),
        scratch_shapes=[dma((layers + 1, cuts))],
        compiler_params=pltpu.CompilerParams(vmem_limit_bytes=1024 * 1024),
    )(final_features, scores, step)
    return (final_features, scores.T, weight_step)


def solution(mesh):
    return jax.shard_map(
        shards,
        mesh=mesh,
        in_specs=(
            P("pop", None, None),
            P("pop"),
            P(None, "mp"),
            P(None, "mp", None),
            P(None, "pop", None, "mp"),
            P(None, "pop", None, None),
            P(None, "mp"),
            P(None, "mp"),
            P("mp"),
        ),
        out_specs=(P("pop", None, "mp"), P("pop", None), P(None, "mp", "pop")),
        check_vma=False,
    )
```

```python
import functools

import jax
import jax.numpy as jnp
from jax import lax
from jax.experimental import pallas as pl
from jax.experimental.pallas import tpu as pltpu
from jax.sharding import PartitionSpec as P

noise_scale = 0.25
norm_eps = 1e-06
spread_eps = 1e-05
lanes = 128
f32, bf16 = jnp.float32, jnp.bfloat16


def policy_kernel(
    dims,
    ids_hbm,
    embed_hbm,
    mix_ref,
    fin_hbm,
    fout_hbm,
    ranks_smem,
    decay_hbm,
    gain_hbm,
    reward_hbm,
    final_ref,
    score_ref,
    step_ref,
    ids_ref,
    embed_ref,
    fin_raw,
    fout_raw,
    decay_ref,
    gain_ref,
    reward_ref,
    weights,
    rows_embed,
    own_part,
    got_part,
    own_over,
    got_over,
    mine_part,
    table,
    own_pair,
    got_pair,
    own_cross,
    got_cross,
    own_lead,
    got_lead,
    own_ahead,
    got_ahead,
    lifted,
    lead_scale,
    states,
    hidden,
    onehot_ref,
    fin_ref,
    fout_ref,
    shaped_ref,
    gin_ref,
    gout_ref,
    granks_ref,
    lows,
    squares,
    leans,
    lasts,
    heads,
    alphas,
    small,
    weight_sem,
    load_sem,
    part_send,
    part_recv,
    over_send,
    over_recv,
    hand_send,
    hand_recv,
    pair_send,
    pair_recv,
    lone_recv,
    cross_send,
    cross_recv,
    lead_send,
    lead_recv,
    ahead_send,
    ahead_recv,
    small_send,
    small_recv,
    relay_send,
    relay_recv,
    plane_send,
    plane_recv,
    in_send,
    in_recv,
    buddy_recv,
    pass_send,
    pass_recv,
    out_send,
    out_recv,
    half_send,
    half_recv,
    self_sem,
):
    pop, chunks, group, steps, member_rows, seqs, rank, width, full, coef, share = dims
    parts = hand_recv.shape[0]
    piece = width // parts
    halves = [slice(p * piece, (p + 1) * piece) for p in range(parts)]
    rows = group * steps
    vocab = embed_ref.shape[0]
    members = ids_ref.shape[0]
    members_all = members * pop
    layers, local = fin_ref.shape[0], fin_ref.shape[1]
    columns = gout_ref.shape[2]
    mine = lax.axis_index("pop")
    me = lax.axis_index("mp")
    side, core = me // 2, me % 2
    mate = side * 2 + (1 - core)
    cross = (1 - side) * 2 + core
    diagonal = (1 - side) * 2 + (1 - core)
    others = (mate, cross, diagonal)
    blocks = (diagonal, cross, mate, me)
    outer = pop // 2
    line, twin = mine // 2, mine % 2
    buddy = line * 2 + (1 - twin)

    def at_line(place):
        return place * 2 + twin

    def peer(q, j):
        return {"pop": q, "mp": j}

    def remote(src, dst, send, recv, q, j):
        return pltpu.make_async_remote_copy(
            src_ref=src,
            dst_ref=dst,
            send_sem=send,
            recv_sem=recv,
            device_id=peer(q, j),
            device_id_type=pl.DeviceIdType.MESH,
        )

    barrier = pltpu.get_barrier_semaphore()

    def greet(q, j):
        pl.semaphore_signal(
            barrier, inc=1, device_id=peer(q, j), device_id_type=pl.DeviceIdType.MESH
        )

    for other in others:
        greet(mine, other)
    greet(buddy, me)

    @pl.when(line < outer - 1)
    def _():
        greet(at_line(line + 1), me)

    @pl.when(line > 0)
    def _():
        greet(at_line(line - 1), me)

    def weight_copy(layer, slot):
        start = pl.multiple_of(blocks[slot] * width, lanes)
        return pltpu.make_async_copy(
            mix_ref.at[layer, :, pl.ds(start, width)],
            weights.at[slot],
            weight_sem.at[4 + slot // 2 if layer else slot],
        )

    loads = [
        pltpu.make_async_copy(src, dst, load_sem.at[i])
        for i, (src, dst) in enumerate(
            (
                (embed_hbm, embed_ref),
                (ids_hbm, ids_ref),
                (fin_hbm, fin_raw),
                (decay_hbm, decay_ref),
                (gain_hbm, gain_ref),
                (reward_hbm, reward_ref),
                (fout_hbm, fout_raw),
            )
        )
    ]
    loads[0].start()
    for slot in range(2):
        weight_copy(0, slot).start()
    for copy in loads[1:3]:
        copy.start()
    weight_copy(0, 2).start()
    weight_copy(0, 3).start()
    for copy in loads[3:]:
        copy.start()

    def rank_block(shape, axis, repeats):
        index = lax.broadcasted_iota(jnp.int32, shape, axis)
        block = jnp.zeros(shape, jnp.int32)
        for m in range(members):
            block = jnp.where(index // repeats == m, ranks_smem[m], block)
        return block

    granks_ref[twin, line] = rank_block((8, lanes), 1, 1)

    def unpack(raw, ref):
        def one(g, carry):
            at = pl.ds(
                pl.multiple_of(g * member_rows * rank, member_rows * rank), member_rows * rank
            )
            for layer in range(layers):
                ref[layer, at, :] = jnp.concatenate(
                    [raw[layer, g * member_rows + m].astype(f32) for m in range(member_rows)],
                    axis=0,
                ).astype(bf16)
            return carry

        lax.fori_loop(0, chunks, one, 0)

    factor_rows = member_rows * rank
    mask = (lax.broadcasted_iota(jnp.int32, (factor_rows, rows), 0) // rank) == (
        (lax.broadcasted_iota(jnp.int32, (factor_rows, rows), 1) % group) // seqs
    )

    def factor_slice(ref, layer, g, start, size):
        at = pl.multiple_of(g * factor_rows, factor_rows)
        return ref[layer, pl.ds(at, factor_rows), pl.ds(start, size)]

    def small_copy(kind, g, r):
        return remote(
            small.at[kind, g, 0],
            small.at[kind, g, r + 1],
            small_send,
            small_recv.at[kind, g],
            mine,
            others[r],
        )

    def small_start(kind, g):
        for r in range(3):
            small_copy(kind, g, r).start()

    def small_sum(kind, g):
        arrived = small.at[kind, g, pl.ds(1, 3)]
        remote(arrived, arrived, small_send, small_recv.at[kind, g], mine, mate).wait_recv()
        return (small[kind, g, 0] + small[kind, g, 1]) + (small[kind, g, 2] + small[kind, g, 3])

    def against(left, features):
        return lax.dot_general(
            left, features, (((1,), (1,)), ((), ())), preferred_element_type=f32
        )

    def low_put(layer, g, local_low):
        local_low = jnp.where(mask, local_low, 0.0)
        packed = local_low[:rank]
        for at in range(rank, factor_rows, rank):
            packed = packed + local_low[at : at + rank]
        small[layer, g, 0] = packed

    def low_ready(layer, g):
        packed = small_sum(layer, g)
        low = jnp.concatenate([packed] * member_rows, axis=0)
        low = jnp.where(mask, low, 0.0) * coef
        top = low.astype(bf16).astype(f32)
        blank = jnp.zeros((lanes - 2 * factor_rows, rows), f32)
        lows[g] = jnp.concatenate([top, low - top, blank], axis=0).T.astype(bf16)

    def correction(layer, g, p):
        start = pl.multiple_of(me * width + p * piece, lanes)
        factor = factor_slice(fout_ref, layer, g, start, piece)
        right = jnp.concatenate(
            [factor, factor, jnp.zeros((lanes - 2 * factor_rows, piece), bf16)], axis=0
        )
        return jnp.dot(lows[g], right, preferred_element_type=f32)

    loads[0].wait()
    rows_embed[:share] = embed_ref[pl.ds(pl.multiple_of(twin * share, share), share), :]
    rows_embed[share:] = embed_ref[2 * share :]
    def relay_copy(way, hop, source):
        return remote(
            granks_ref.at[twin, source],
            granks_ref.at[twin, source],
            relay_send.at[way, hop - 1],
            relay_recv.at[way, hop - 1],
            at_line(line + 1) if way == 0 else at_line(line - 1),
            me,
        )

    def relay_each(hop, act, sending):
        shift = hop - 1 if sending else hop
        right = (line >= shift) & (line < outer - 1) if sending else line >= shift
        left = (line + shift < outer) & (line > 0) if sending else line + shift < outer

        @pl.when(right)
        def _():
            act(relay_copy(0, hop, line - shift))

        @pl.when(left)
        def _():
            act(relay_copy(1, hop, line + shift))

    def relay_start(hop):
        relay_each(hop, lambda copy: copy.start(), True)

    def relay_next(hop):
        relay_each(hop, lambda copy: copy.wait_recv(), False)
        if hop + 1 < outer:
            relay_start(hop + 1)

    plane = remote(granks_ref.at[twin], granks_ref.at[twin], plane_send, plane_recv, buddy, me)
    plane_in = remote(
        granks_ref.at[1 - twin], granks_ref.at[1 - twin], plane_send, plane_recv, buddy, me
    )

    def part_copy(slot, p):
        return remote(
            own_part.at[slot, p],
            got_part.at[slot, p],
            part_send,
            part_recv.at[slot, p],
            mine,
            mate,
        )

    def own_rows(q):
        return pl.ds(pl.multiple_of(q * local, local), local)

    def in_copy(way, hop, source):
        return remote(
            fin_ref,
            gin_ref.at[:, own_rows(at_line(source)), :],
            in_send,
            in_recv.at[way, hop - 1],
            at_line(line + hop) if way == 0 else at_line(line - hop),
            me,
        )

    def in_start(hop):
        @pl.when(line + hop < outer)
        def _():
            in_copy(0, hop, line).start()

        @pl.when(line >= hop)
        def _():
            in_copy(1, hop, line).start()

    def in_pass(hop):
        @pl.when(line >= hop)
        def _():
            in_copy(0, hop, line - hop).wait_recv()
            pass_copy(line - hop, twin).start()

        @pl.when(line + hop < outer)
        def _():
            in_copy(1, hop, line + hop).wait_recv()
            pass_copy(line + hop, twin).start()

    def in_buddy(source):
        return remote(
            fin_ref,
            gin_ref.at[:, own_rows(source), :],
            in_send,
            buddy_recv,
            buddy,
            me,
        )

    def pass_copy(place, side_of):
        at = own_rows(place * 2 + side_of)
        return remote(
            gin_ref.at[:, at, :],
            gin_ref.at[:, at, :],
            pass_send,
            pass_recv,
            buddy,
            me,
        )

    def out_copy(hop, source):
        target = lax.rem(mine + hop, pop)
        cols = pl.multiple_of(target * columns, lanes)
        return remote(
            fout_ref.at[core, :, pl.ds(cols, columns)],
            gout_ref.at[core, own_rows(source), :],
            out_send,
            out_recv,
            target,
            me,
        )

    def stretch(ref, count):
        return ref.at[pl.ds(0, count * local), :]

    def whole_out():
        spot = stretch(gout_ref.at[core], pop - 1)
        return remote(spot, spot, out_send, out_recv, buddy, me)

    def whole_pass():
        spot = gin_ref.at[:, pl.ds(0, (outer - 1) * local), :]
        return remote(spot, spot, pass_send, pass_recv, buddy, me)

    def whole_in():
        spot = gin_ref.at[:, pl.ds(0, outer * local), :]
        return remote(spot, spot, in_send, buddy_recv, buddy, me)

    def half_copy(which):
        return remote(
            gout_ref.at[which],
            gout_ref.at[which],
            half_send,
            half_recv,
            mine,
            mate,
        )

    def self_copies():
        cols = pl.multiple_of(mine * columns, lanes)
        return (
            pltpu.make_async_copy(fin_ref, gin_ref.at[:, own_rows(mine), :], self_sem.at[0]),
            pltpu.make_async_copy(
                fout_ref.at[core, :, pl.ds(cols, columns)],
                gout_ref.at[core, own_rows(mine), :],
                self_sem.at[1],
            ),
        )

    spans = (pl.ds(0, share), pl.ds(share, vocab - 2 * share))

    def over_copy(h, p):
        return remote(
            own_over.at[p, spans[h]],
            got_over.at[p, spans[h]],
            over_send,
            over_recv.at[h, p],
            mine,
            cross,
        )

    def hand_copy(p, half):
        at = pl.ds(pl.multiple_of(half * share, share), share)
        return remote(
            table.at[p, at],
            table.at[p, at],
            hand_send,
            hand_recv.at[p],
            buddy,
            me,
        )

    def entry(slot, p):
        return jnp.dot(
            rows_embed[...], weights[slot, :, halves[p]], preferred_element_type=f32
        ).astype(bf16)

    def part_put(p):
        if p == 0:
            weight_copy(0, 0).wait()
        own_part[0, p] = entry(0, p)

    def part_sum(p):
        if p == 0:
            weight_copy(0, 1).wait()
        value = entry(1, p).astype(f32)
        part_copy(0, p).wait_recv()
        own_over[p] = (value + got_part[0, p].astype(f32)).astype(bf16)
        over_copy(0, p).start()

    early = 2
    with jax.named_scope("tab0"):
        for p in range(early):
            part_put(p)
    with jax.named_scope("bar"):
        pl.semaphore_wait(
            barrier,
            4 + jnp.where(line < outer - 1, 1, 0) + jnp.where(line > 0, 1, 0),
        )

    relay_start(1)
    with jax.named_scope("tab1"):
        for p in range(early):
            part_copy(0, p).start()
        for p in range(early, parts):
            part_put(p)
            part_copy(0, p).start()
        for p in range(parts):
            part_sum(p)
        weight_copy(1, 0).start()
        weight_copy(1, 1).start()
    loads[1].wait()
    loads[2].wait()
    unpack(fin_raw, fin_ref)

    def begin(g, carry):
        tokens = jnp.concatenate(
            [ids_ref[g * member_rows + m] for m in range(member_rows)], axis=0
        )
        entries = lax.broadcasted_iota(jnp.int32, (group, vocab), 1)
        for t in range(steps):
            onehot_ref[g, t * group : (t + 1) * group, :] = jnp.where(
                tokens[:, t : t + 1] == entries, 1.0, 0.0
            ).astype(bf16)
        features = jnp.dot(onehot_ref[g], embed_ref[...], preferred_element_type=f32).astype(bf16)
        hidden[g] = features
        low_put(0, g, against(factor_slice(fin_ref, 0, g, 0, width), features))
        return carry

    with jax.named_scope("begin"):
        lax.fori_loop(0, chunks, begin, 0)

    for g in range(chunks):
        small_start(0, g)
    for p in range(parts):
        over_copy(1, p).start()
    with jax.named_scope("relay1"):
        relay_next(1)
        in_start(1)
    with jax.named_scope("tab2"):
        weight_copy(0, 2).wait()
        for p in range(parts):
            own_part[1, p] = entry(2, p)
            part_copy(1, p).start()
        weight_copy(1, 2).start()
    def both(h, p):
        at = spans[h]
        return (
            mine_part[p, at].astype(f32) + got_part[1, p, at].astype(f32)
        ) + got_over[p, at].astype(f32)

    lead = lifted.shape[0]

    def lead_pair(k, p):
        return remote(
            own_lead.at[k, p],
            got_lead.at[k, p],
            lead_send,
            lead_recv.at[1 + p if k else 0],
            mine,
            mate,
        )

    def whole_lead():
        return remote(own_lead.at[0], got_lead.at[0], lead_send, lead_recv.at[0], mine, mate)

    def lead_cross(k, p):
        return remote(
            own_ahead.at[k, p], got_ahead.at[k, p], ahead_send, ahead_recv, mine, cross
        )

    def lead_rows(k):
        return lifted[...] if k else hidden[0, :lead]

    def lead_put(k, p):
        if k == 0 and p == 0:
            wait_weights(0)
        own_lead[k, p] = jnp.dot(
            lead_rows(k), weights[0, :, halves[p]], preferred_element_type=f32
        ).astype(bf16)
        lead_pair(k, p).start()

    def lead_sum(k, p):
        value = (
            jnp.dot(lead_rows(k), weights[1, :, halves[p]], preferred_element_type=f32)
            .astype(bf16)
            .astype(f32)
        )
        if k:
            lead_pair(k, p).wait_recv()
        own_ahead[k, p] = (value + got_lead[k, p].astype(f32)).astype(bf16)
        lead_cross(k, p).start()

    def wait_weights(half):
        spot = weights.at[pl.ds(2 * half, 2)]
        pltpu.make_async_copy(spot, spot, weight_sem.at[4 + half]).wait()

    with jax.named_scope("tabA"):
        weight_copy(0, 3).wait()
        for p in range(parts):
            mine_part[p] = entry(3, p)
            part_copy(1, p).wait_recv()
            over_copy(0, p).wait_recv()
            table[p, pl.ds(pl.multiple_of(twin * share, share), share)] = both(0, p).astype(bf16)
            hand_copy(p, twin).start()
        weight_copy(1, 3).start()
        in_buddy(mine).start()
    with jax.named_scope("prep"):
        for copy in loads[3:]:
            copy.wait()
        unpack(fout_raw, fout_ref)
        reward = reward_ref[...]
        high = reward.astype(bf16).astype(f32)
        middle = (reward - high).astype(bf16).astype(f32)
        rest = reward - high - middle
        index = lax.broadcasted_iota(jnp.int32, (16, width), 0)
        heads[...] = jnp.where(
            index == 0,
            high,
            jnp.where(index == 1, middle, jnp.where(index == 2, rest, 0.0)),
        ).astype(bf16)

    with jax.named_scope("leadx"):
        for p in range(parts):
            lead_put(0, p)
    with jax.named_scope("lowready"):
        for g in range(chunks):
            low_ready(0, g)
    with jax.named_scope("leads"):
        whole_lead().wait_recv()
        for p in range(parts):
            lead_sum(0, p)
    with jax.named_scope("relay2"):
        if outer > 2:
            relay_next(2)
            in_start(2)

    def recur(layer, g, p, inputs):
        decay = decay_ref[layer : layer + 1, halves[p]]
        kept = 1.0 - decay
        carried = jnp.zeros((group, piece), f32)
        if layer:
            lean = gain_ref[layer : layer + 1, halves[p]] * reward_ref[:, halves[p]]
        for t in range(steps):
            at = slice(t * group, (t + 1) * group)
            carried = decay * carried + kept * inputs[at]
            if not layer:
                states[g, at, halves[p]] = carried
            elif t == steps - 1:
                lasts[g, :, halves[p]] = carried
            powers = carried * carried
            total = powers[:, :lanes]
            for c in range(lanes, piece, lanes):
                total = total + powers[:, c : c + lanes]
            if p:
                total = total + squares[g, at, :]
            squares[g, at, :] = total
            if layer:
                leaning = carried * lean
                total = leaning[:, :lanes]
                for c in range(lanes, piece, lanes):
                    total = total + leaning[:, c : c + lanes]
                if p:
                    total = total + leans[g, at, :]
                leans[g, at, :] = total

    def across(value):
        return jnp.sum(value.T, axis=0, keepdims=True)

    def squares_start(g):
        small[2, g, 0] = jnp.broadcast_to(across(squares[g]), (4, rows))
        small_start(2, g)

    for p in range(parts):
        with jax.named_scope("tabB%d" % p):
            over_copy(1, p).wait_recv()
            table[p, 2 * share :] = both(1, p).astype(bf16)
        with jax.named_scope("hand%d" % p):
            hand_copy(p, 1 - twin).wait_recv()
        with jax.named_scope("lz%d" % p):
            for g in range(chunks):
                inputs = jnp.dot(
                    onehot_ref[g], table[p], preferred_element_type=f32
                ) + correction(0, g, p)
                recur(0, g, p, inputs)
                if p == parts - 1:
                    squares_start(g)
                    if g == 0:
                        with jax.named_scope("leadv"):
                            lift = states[0, :lead] * gain_ref[0:1, :]
                            lifted[...] = lift.astype(bf16)
                            for q in range(parts):
                                lead_put(1, q)
                            for q in range(parts):
                                lead_sum(1, q)
    def pair_copy(g, slot, p):
        return remote(
            own_pair.at[g, slot, p],
            got_pair.at[g, slot, p],
            pair_send,
            pair_recv.at[g, 1] if slot else lone_recv.at[p] if g == 0 else pair_recv.at[g, 0],
            mine,
            mate,
        )

    def whole_pair(g, slot):
        return remote(
            own_pair.at[g, slot],
            got_pair.at[g, slot],
            pair_send,
            pair_recv.at[g, slot],
            mine,
            mate,
        )

    def cross_copy(g, p):
        at = pl.ds(0 if g else lead, rows if g else rows - lead)
        return remote(
            own_cross.at[g, p, at],
            got_cross.at[g, p, at],
            cross_send.at[1 if g else 0],
            cross_recv.at[parts + g if g < chunks - 1 else p],
            mine,
            cross,
        )

    def whole_cross(g):
        at = pl.ds(0 if g else lead, rows if g else rows - lead)
        return remote(
            own_cross.at[g, :, at],
            got_cross.at[g, :, at],
            cross_send.at[1 if g else 0],
            cross_recv.at[parts + g],
            mine,
            cross,
        )

    def shape_ranks():
        full_block = (2, outer, 8, lanes)
        kept = (lax.broadcasted_iota(jnp.int32, full_block, 2) == 0) & (
            lax.broadcasted_iota(jnp.int32, full_block, 3) < members
        )
        shares = jnp.where(kept, granks_ref[...].astype(f32) / members_all, 0.0)

        def mean_of(value):
            value = jnp.sum(value, axis=0)
            value = jnp.sum(value, axis=0)
            value = jnp.sum(value, axis=0, keepdims=True)
            return jnp.sum(value, axis=1, keepdims=True) / members_all

        rank_mean = mean_of(shares)
        apart = jnp.where(kept, shares - rank_mean[None, None], 0.0)
        spread = mean_of(apart * apart) + spread_eps
        owner = lax.broadcasted_iota(jnp.int32, (local, lanes), 0) // rank
        own = owner == lax.broadcasted_iota(jnp.int32, (local, lanes), 1)
        for place in range(outer):
            for side_of in range(2):
                share_row = granks_ref[side_of, place, 0:1].astype(f32) / members_all
                shaped = (share_row - rank_mean) * lax.rsqrt(spread)
                shaped = jnp.where(own, jnp.broadcast_to(shaped, (local, lanes)), 0.0)
                shaped = jnp.sum(shaped, axis=1, keepdims=True)
                at = (place * 2 + side_of) * local
                shaped_ref[at : at + local] = jnp.broadcast_to(shaped, (local, lanes))

    def out_start():
        with jax.named_scope("outs"):
            plane_in.wait_recv()
            for hop in range(1, pop):
                out_copy(hop, mine).start()
            for copy in self_copies():
                copy.start()

    def gather_half():
        with jax.named_scope("half"):
            whole_out().wait_recv()
            for copy in self_copies():
                copy.wait()
            half_copy(core).start()

    def step_make():
        tile = 256
        with jax.named_scope("arrive"):
            in_buddy(buddy).wait_recv()
        with jax.named_scope("arrive_pass"):
            whole_pass().wait_recv()
        with jax.named_scope("arrive_half"):
            half_copy(1 - core).wait_recv()
        with jax.named_scope("step"):
            shape_ranks()
            shaped = jnp.concatenate([shaped_ref[...]] * (tile // lanes), axis=1)
            for layer in range(layers):
                for at in range(0, width, tile):
                    factor = gin_ref[layer, :, at : at + tile].astype(f32)
                    value = lax.dot_general(
                        (factor * shaped).astype(bf16),
                        gout_ref[layer],
                        (((0,), (0,)), ((), ())),
                        preferred_element_type=f32,
                    )
                    step_ref[layer, at : at + tile] = value * (members_all * rank) ** (-0.5)

    def between(g):
        if g == 0:
            wait_weights(1)
        with jax.named_scope("normed%d" % g):
            total = small_sum(2, g)[:1]
            scale = lax.rsqrt(total / full + norm_eps)
            scale = jnp.broadcast_to(scale, (lanes, rows)).T
            if g == 0:
                lead_scale[...] = scale[:lead]
            scale = jnp.concatenate([scale] * (width // lanes), axis=1)
            gain = gain_ref[0:1, :]
            hidden[g] = (hidden[g].astype(f32) + states[g] * scale * gain).astype(bf16)

        def product(slot, p):
            return jnp.dot(
                hidden[g], weights[slot, :, halves[p]], preferred_element_type=f32
            ).astype(bf16)

        with jax.named_scope("exch%d" % g):
            def summed(p):
                value = product(1, p).astype(f32)
                if g == 0:
                    pair_copy(g, 0, p).wait_recv()
                elif p == 0:
                    whole_pair(g, 0).wait_recv()
                total = (value + got_pair[g, 0, p].astype(f32)).astype(bf16)
                if g:
                    own_cross[g, p] = total
                else:
                    own_cross[g, p, lead:] = total[lead:]
                cross_copy(g, p).start()

            for p in range(parts):
                own_pair[g, 0, p] = product(0, p)
                pair_copy(g, 0, p).start()
                if p and g == 0:
                    summed(p - 1)
            left = jnp.concatenate([factor_slice(fin_ref, 1, g, 0, width), heads[...]], axis=0)
            local_low = against(left, hidden[g])
            low_put(1, g, local_low[:factor_rows])
            small_start(1, g)
            aligned = local_low[factor_rows : factor_rows + 8]
            alphas[g] = jnp.broadcast_to(jnp.sum(aligned, axis=0, keepdims=True), (8, rows))
            for p in range(0 if g else parts - 1, parts):
                summed(p)
            for p in range(parts):
                own_pair[g, 1, p] = product(2, p)
                pair_copy(g, 1, p).start()
            for p in range(parts):
                states[g, :, halves[p]] = product(3, p).astype(f32)

    def layer_one(g):
        with jax.named_scope("lowone%d" % g):
            low_ready(1, g)
        for p in range(parts):
            with jax.named_scope("l1_%d_%d" % (g, p)):
                if p == 0:
                    whole_pair(g, 1).wait_recv()
                fixed = (
                    states[g, :, halves[p]] + got_pair[g, 1, p].astype(f32)
                ) + correction(1, g, p)
                if g == chunks - 1:
                    cross_copy(g, p).wait_recv()
                elif p == 0:
                    whole_cross(g).wait_recv()
                if g:
                    other = got_cross[g, p].astype(f32)
                else:
                    if p == 0:
                        remote(
                            own_ahead, got_ahead, ahead_send, ahead_recv, mine, cross
                        ).wait_recv()
                    scale = jnp.concatenate([lead_scale[...]] * (piece // lanes), axis=1)
                    other = got_ahead[0, p].astype(f32) + scale * got_ahead[1, p].astype(f32)
                    other = jnp.concatenate([other, got_cross[0, p, lead:].astype(f32)], axis=0)
                recur(1, g, p, fixed + other)
        with jax.named_scope("end%d" % g):
            small[3, g, 0] = jnp.concatenate(
                [across(squares[g]), across(leans[g]), alphas[g][:2]], axis=0
            )
            small_start(3, g)

    with jax.named_scope("relay3"):
        for hop in range(3, outer):
            relay_next(hop)
            in_start(hop)
        plane.start()
    with jax.named_scope("pass1"):
        in_pass(1)
    for g in range(chunks):
        between(g)
        if g == 0:
            out_start()
        with jax.named_scope("pass"):
            for hop in range(g + 1, min(g + 2, outer) if g else 0):
                in_pass(hop)
    for g in range(chunks):
        if g == chunks - 1:
            with jax.named_scope("pass"):
                for hop in range(chunks + 1, outer):
                    in_pass(hop)
            gather_half()
            if g:
                layer_one(g - 1)
            step_make()
            layer_one(g)
        elif g < chunks - 2:
            layer_one(g)

    lane = lax.broadcasted_iota(jnp.int32, (seqs, lanes), 1)
    scores = jnp.zeros((seqs, lanes), f32)
    with jax.named_scope("final"):
        for g in range(chunks):
            sums = small_sum(3, g)
            scale = lax.rsqrt(sums[0:1] / full + norm_eps)
            value = sums[2:3] + scale * sums[1:2]
            total = value[:, :lanes]
            for c in range(lanes, rows, lanes):
                total = total + value[:, c : c + lanes]
            total = jnp.broadcast_to(total, (8, lanes))
            shift = lanes // 2
            while shift >= group:
                total = total + pltpu.roll(total, shift, 1)
                shift //= 2
            total = total * (full ** (-0.5) / steps)
            total = jnp.broadcast_to(total[:1], (lanes, lanes)).T
            for m in range(member_rows):
                scores = jnp.where(
                    lane == g * member_rows + m, total[m * seqs : (m + 1) * seqs], scores
                )
            ending = jnp.broadcast_to(scale[:, rows - lanes :], (lanes, lanes)).T[lanes - group :]
            ending = jnp.concatenate([ending] * (width // lanes), axis=1)
            gain = gain_ref[1:2, :]
            ending = (
                hidden[g, rows - group :].astype(f32) + lasts[g] * ending * gain
            ).astype(bf16).astype(f32)
            for m in range(member_rows):
                final_ref[g * member_rows + m] = ending[m * seqs : (m + 1) * seqs].astype(bf16)
        score_ref[...] = scores[:, :members]

    with jax.named_scope("drain"):
        for hop in range(1, outer):
            relay_each(hop, lambda copy: copy.wait_send(), True)
        plane.wait_send()
        remote(own_part, got_part, part_send, part_recv.at[0, 0], mine, mate).wait_send()
        remote(own_over, got_over, over_send, over_recv.at[0, 0], mine, cross).wait_send()
        spot = table.at[:, pl.ds(0, share)]
        remote(spot, spot, hand_send, hand_recv.at[0], buddy, me).wait_send()
        remote(own_pair, got_pair, pair_send, pair_recv.at[0, 0], mine, mate).wait_send()
        spot = own_cross.at[0, :, pl.ds(lead, rows - lead)]
        remote(spot, spot, cross_send.at[0], cross_recv.at[0], mine, cross).wait_send()
        if chunks > 1:
            spot = own_cross.at[pl.ds(1, chunks - 1)]
            remote(spot, spot, cross_send.at[1], cross_recv.at[0], mine, cross).wait_send()
        remote(own_lead, got_lead, lead_send, lead_recv.at[0], mine, mate).wait_send()
        remote(own_ahead, got_ahead, ahead_send, ahead_recv, mine, cross).wait_send()
        spot = small.at[:, :, pl.ds(1, 3)]
        remote(spot, spot, small_send, small_recv.at[0, 0], mine, mate).wait_send()
        whole_in().wait_send()
        whole_pass().wait_send()
        whole_out().wait_send()
        half_copy(core).wait_send()


cuts = 4


def publish(final_ref, score_ref, step_ref, final_out, score_out, step_out, sems):
    copies = []
    layers, width, _ = step_ref.shape
    cut = width // cuts
    for layer in range(layers):
        for c in range(cuts):
            at = pl.ds(c * cut, cut)
            copies.append(
                pltpu.make_async_copy(
                    step_ref.at[layer, at], step_out.at[layer, at], sems.at[layer, c]
                )
            )
    copies.append(pltpu.make_async_copy(final_ref, final_out, sems.at[layers, 0]))
    copies.append(pltpu.make_async_copy(score_ref, score_out, sems.at[layers, 1]))
    for copy in copies:
        copy.start()
    for copy in copies:
        copy.wait()


def shards(
    token_ids,
    fitness_ranks,
    embedding,
    mix_weights,
    factors_in,
    factors_out,
    decay_rates,
    norm_gain,
    reward_dir,
):
    members, seqs, steps = token_ids.shape
    vocab, width = embedding.shape
    layers, _, full = mix_weights.shape
    rank = factors_in.shape[2]
    pop = lax.axis_size("pop")
    outer = pop // 2
    coef = noise_scale * (full * rank) ** (-0.5)
    columns = full // pop
    member_rows = 16 // seqs
    chunks = members // member_rows
    group = member_rows * seqs
    rows = group * steps
    local = members * rank
    share = vocab * 5 // 16
    lead = rows * 5 // 16
    dims = (pop, chunks, group, steps, member_rows, seqs, rank, width, full, coef, share)
    vmem = pl.BlockSpec(memory_space=pltpu.VMEM)
    smem = pl.BlockSpec(memory_space=pltpu.SMEM)
    hbm = pl.BlockSpec(memory_space=pltpu.HBM)
    parts = 4
    piece = width // parts
    entries = vocab - share
    dma = pltpu.SemaphoreType.DMA
    final_features, scores, step = pl.pallas_call(
        functools.partial(policy_kernel, dims),
        out_shape=(
            pltpu.VMEM((members, seqs, width), bf16),
            pltpu.VMEM((seqs, members), f32),
            pltpu.VMEM((layers, width, columns), f32),
        ),
        in_specs=[hbm, hbm, hbm, hbm, hbm, smem, hbm, hbm, hbm],
        out_specs=(vmem, vmem, vmem),
        scratch_shapes=[
            pltpu.VMEM((members, seqs, steps), jnp.int32),
            pltpu.VMEM((vocab, width), bf16),
            pltpu.VMEM((layers, members, rank, width), bf16),
            pltpu.VMEM((layers, members, rank, full), bf16),
            pltpu.VMEM((layers, width), f32),
            pltpu.VMEM((layers, width), f32),
            pltpu.VMEM((1, width), f32),
            pltpu.VMEM((4, width, width), bf16),
            pltpu.VMEM((entries, width), bf16),
            pltpu.VMEM((2, parts, entries, piece), bf16),
            pltpu.VMEM((2, parts, entries, piece), bf16),
            pltpu.VMEM((parts, entries, piece), bf16),
            pltpu.VMEM((parts, entries, piece), bf16),
            pltpu.VMEM((parts, entries, piece), bf16),
            pltpu.VMEM((parts, vocab, piece), bf16),
            pltpu.VMEM((chunks, 2, parts, rows, piece), bf16),
            pltpu.VMEM((chunks, 2, parts, rows, piece), bf16),
            pltpu.VMEM((chunks, parts, rows, piece), bf16),
            pltpu.VMEM((chunks, parts, rows, piece), bf16),
            pltpu.VMEM((2, parts, lead, piece), bf16),
            pltpu.VMEM((2, parts, lead, piece), bf16),
            pltpu.VMEM((2, parts, lead, piece), bf16),
            pltpu.VMEM((2, parts, lead, piece), bf16),
            pltpu.VMEM((lead, width), bf16),
            pltpu.VMEM((lead, lanes), f32),
            pltpu.VMEM((chunks, rows, width), f32),
            pltpu.VMEM((chunks, rows, width), bf16),
            pltpu.VMEM((chunks, rows, vocab), bf16),
            pltpu.VMEM((layers, local, width), bf16),
            pltpu.VMEM((layers, local, full), bf16),
            pltpu.VMEM((pop * local, lanes), f32),
            pltpu.VMEM((layers, pop * local, width), bf16),
            pltpu.VMEM((layers, pop * local, columns), bf16),
            pltpu.VMEM((2, outer, 8, lanes), jnp.int32),
            pltpu.VMEM((chunks, rows, lanes), bf16),
            pltpu.VMEM((chunks, rows, lanes), f32),
            pltpu.VMEM((chunks, rows, lanes), f32),
            pltpu.VMEM((chunks, group, width), f32),
            pltpu.VMEM((16, width), bf16),
            pltpu.VMEM((chunks, 8, rows), f32),
            pltpu.VMEM((4, chunks, 4, 4, rows), f32),
            dma((6,)),
            dma((7,)),
            dma,
            dma((2, parts)),
            dma,
            dma((2, parts)),
            dma,
            dma((parts,)),
            dma,
            dma((chunks, 2)),
            dma((parts,)),
            dma((2,)),
            dma((parts + chunks - 1,)),
            dma,
            dma((parts + 1,)),
            dma,
            dma,
            dma,
            dma((4, chunks)),
            dma((2, outer - 1)),
            dma((2, outer - 1)),
            dma,
            dma,
            dma,
            dma((2, outer - 1)),
            dma,
            dma,
            dma,
            dma,
            dma,
            dma,
            dma,
            dma((2,)),
        ],
        compiler_params=pltpu.CompilerParams(
            collective_id=0, has_side_effects=True, vmem_limit_bytes=52 * 1024 * 1024
        ),
    )(
        *(
            pltpu.with_memory_space_constraint(value, pltpu.HBM)
            for value in (
                token_ids,
                embedding,
                mix_weights,
                factors_in,
                factors_out,
                fitness_ranks,
                decay_rates,
                norm_gain,
                reward_dir.reshape(1, width),
            )
        )
    )
    final_features, scores, weight_step = pl.pallas_call(
        publish,
        out_shape=(
            jax.ShapeDtypeStruct((members, seqs, width), bf16),
            jax.ShapeDtypeStruct((seqs, members), f32),
            jax.ShapeDtypeStruct((layers, width, columns), f32),
        ),
        in_specs=[vmem, vmem, vmem],
        out_specs=(hbm, hbm, hbm),
        scratch_shapes=[dma((layers + 1, cuts))],
        compiler_params=pltpu.CompilerParams(vmem_limit_bytes=1024 * 1024),
    )(final_features, scores, step)
    return (final_features, scores.T, weight_step)


def solution(mesh):
    return jax.shard_map(
        shards,
        mesh=mesh,
        in_specs=(
            P("pop", None, None),
            P("pop"),
            P(None, "mp"),
            P(None, "mp", None),
            P(None, "pop", None, "mp"),
            P(None, "pop", None, None),
            P(None, "mp"),
            P(None, "mp"),
            P("mp"),
        ),
        out_specs=(P("pop", None, "mp"), P("pop", None), P(None, "mp", "pop")),
        check_vma=False,
    )
```

```python
import functools

import jax
import jax.numpy as jnp
from jax import lax
from jax.experimental import pallas as pl
from jax.experimental.pallas import tpu as pltpu
from jax.sharding import PartitionSpec as P

noise_scale = 0.25
norm_eps = 1e-06
spread_eps = 1e-05
lanes = 128
f32, bf16 = jnp.float32, jnp.bfloat16


def policy_kernel(
    dims,
    ids_hbm,
    embed_hbm,
    mix_ref,
    fin_hbm,
    fout_hbm,
    ranks_smem,
    decay_hbm,
    gain_hbm,
    reward_hbm,
    final_ref,
    score_ref,
    step_ref,
    ids_ref,
    embed_ref,
    fin_raw,
    fout_raw,
    decay_ref,
    gain_ref,
    reward_ref,
    weights,
    rows_embed,
    own_part,
    got_part,
    own_over,
    got_over,
    mine_part,
    table,
    own_pair,
    got_pair,
    own_cross,
    got_cross,
    own_lead,
    got_lead,
    own_ahead,
    got_ahead,
    lifted,
    lead_scale,
    states,
    hidden,
    onehot_ref,
    fin_ref,
    fout_ref,
    shaped_ref,
    gin_ref,
    gout_ref,
    granks_ref,
    lows,
    squares,
    leans,
    lasts,
    heads,
    alphas,
    small,
    weight_sem,
    column_sem,
    load_sem,
    part_send,
    part_recv,
    over_send,
    over_recv,
    hand_send,
    hand_recv,
    pair_send,
    pair_recv,
    lone_recv,
    cross_send,
    cross_recv,
    lead_send,
    lead_recv,
    ahead_send,
    ahead_recv,
    small_send,
    small_recv,
    low_send,
    low_recv,
    relay_send,
    relay_recv,
    plane_send,
    plane_recv,
    in_send,
    in_recv,
    buddy_recv,
    pass_send,
    pass_recv,
    out_send,
    out_recv,
    half_send,
    half_recv,
    self_sem,
):
    pop, chunks, group, steps, member_rows, seqs, rank, width, full, coef, share = dims
    parts = hand_recv.shape[0]
    piece = width // parts
    halves = [slice(p * piece, (p + 1) * piece) for p in range(parts)]
    rows = group * steps
    vocab = embed_ref.shape[0]
    members = ids_ref.shape[0]
    members_all = members * pop
    layers, local = fin_ref.shape[0], fin_ref.shape[1]
    columns = gout_ref.shape[2]
    mine = lax.axis_index("pop")
    me = lax.axis_index("mp")
    side, core = me // 2, me % 2
    mate = side * 2 + (1 - core)
    cross = (1 - side) * 2 + core
    diagonal = (1 - side) * 2 + (1 - core)
    others = (mate, cross, diagonal)
    blocks = (diagonal, cross, mate, me)
    outer = pop // 2
    line, twin = mine // 2, mine % 2
    buddy = line * 2 + (1 - twin)

    def at_line(place):
        return place * 2 + twin

    def peer(q, j):
        return {"pop": q, "mp": j}

    def remote(src, dst, send, recv, q, j):
        return pltpu.make_async_remote_copy(
            src_ref=src,
            dst_ref=dst,
            send_sem=send,
            recv_sem=recv,
            device_id=peer(q, j),
            device_id_type=pl.DeviceIdType.MESH,
        )

    barrier = pltpu.get_barrier_semaphore()

    def greet(q, j):
        pl.semaphore_signal(
            barrier, inc=1, device_id=peer(q, j), device_id_type=pl.DeviceIdType.MESH
        )

    for other in others:
        greet(mine, other)
    greet(buddy, me)

    @pl.when(line < outer - 1)
    def _():
        greet(at_line(line + 1), me)

    @pl.when(line > 0)
    def _():
        greet(at_line(line - 1), me)

    def weight_copy(layer, slot):
        start = pl.multiple_of(blocks[slot] * width, lanes)
        return pltpu.make_async_copy(
            mix_ref.at[layer, :, pl.ds(start, width)],
            weights.at[slot],
            weight_sem.at[2 + slot // 2 if layer else slot - 2],
        )

    def column_copy(slot, p):
        start = pl.multiple_of(blocks[slot] * width + p * piece, lanes)
        return pltpu.make_async_copy(
            mix_ref.at[0, :, pl.ds(start, piece)],
            weights.at[slot, :, halves[p]],
            column_sem.at[slot, p],
        )

    loads = [
        pltpu.make_async_copy(src, dst, load_sem.at[i])
        for i, (src, dst) in enumerate(
            (
                (
                    embed_hbm.at[pl.ds(pl.multiple_of(twin * share, share), share)],
                    rows_embed.at[pl.ds(0, share)],
                ),
                (
                    embed_hbm.at[pl.ds(2 * share, embed_ref.shape[0] - 2 * share)],
                    rows_embed.at[pl.ds(share, embed_ref.shape[0] - 2 * share)],
                ),
                (embed_hbm, embed_ref),
                (ids_hbm, ids_ref),
                (fin_hbm, fin_raw),
                (decay_hbm, decay_ref),
                (gain_hbm, gain_ref),
                (reward_hbm, reward_ref),
                (fout_hbm, fout_raw),
            )
        )
    ]
    for copy in loads[:2]:
        copy.start()
    for slot in range(2):
        column_copy(slot, 0).start()

    def rank_block(shape, axis, repeats):
        index = lax.broadcasted_iota(jnp.int32, shape, axis)
        block = jnp.zeros(shape, jnp.int32)
        for m in range(members):
            block = jnp.where(index // repeats == m, ranks_smem[m], block)
        return block

    granks_ref[twin, line] = rank_block((8, lanes), 1, 1)

    def unpack(raw, ref):
        def one(g, carry):
            at = pl.ds(
                pl.multiple_of(g * member_rows * rank, member_rows * rank), member_rows * rank
            )
            for layer in range(layers):
                ref[layer, at, :] = jnp.concatenate(
                    [raw[layer, g * member_rows + m].astype(f32) for m in range(member_rows)],
                    axis=0,
                ).astype(bf16)
            return carry

        lax.fori_loop(0, chunks, one, 0)

    factor_rows = member_rows * rank
    mask = (lax.broadcasted_iota(jnp.int32, (factor_rows, rows), 0) // rank) == (
        (lax.broadcasted_iota(jnp.int32, (factor_rows, rows), 1) % group) // seqs
    )

    def factor_slice(ref, layer, g, start, size):
        at = pl.multiple_of(g * factor_rows, factor_rows)
        return ref[layer, pl.ds(at, factor_rows), pl.ds(start, size)]

    def small_copy(kind, g, r):
        return remote(
            small.at[kind, g, 0],
            small.at[kind, g, r + 1],
            small_send,
            small_recv.at[kind - 2, g],
            mine,
            others[r],
        )

    def small_start(kind, g):
        for r in range(3):
            small_copy(kind, g, r).start()

    def small_sum(kind, g):
        arrived = small.at[kind, g, pl.ds(1, 3)]
        remote(arrived, arrived, small_send, small_recv.at[kind - 2, g], mine, mate).wait_recv()
        return (small[kind, g, 0] + small[kind, g, 1]) + (small[kind, g, 2] + small[kind, g, 3])

    def low_copy(layer, g, stage):
        return remote(
            small.at[layer, g, 2 * stage],
            small.at[layer, g, 2 * stage + 1],
            low_send,
            low_recv.at[layer, stage, g],
            mine,
            mate if stage else cross,
        )

    def low_fold(layer, g):
        low_copy(layer, g, 0).wait_recv()
        small[layer, g, 2] = small[layer, g, 0] + small[layer, g, 1]
        low_copy(layer, g, 1).start()

    def against(left, features):
        return lax.dot_general(
            left, features, (((1,), (1,)), ((), ())), preferred_element_type=f32
        )

    def low_put(layer, g, local_low):
        local_low = jnp.where(mask, local_low, 0.0)
        packed = local_low[:rank]
        for at in range(rank, factor_rows, rank):
            packed = packed + local_low[at : at + rank]
        small[layer, g, 0] = packed

    def low_ready(layer, g):
        low_copy(layer, g, 1).wait_recv()
        packed = small[layer, g, 2] + small[layer, g, 3]
        low = jnp.concatenate([packed] * member_rows, axis=0)
        low = jnp.where(mask, low, 0.0) * coef
        top = low.astype(bf16).astype(f32)
        blank = jnp.zeros((lanes - 2 * factor_rows, rows), f32)
        lows[g] = jnp.concatenate([top, low - top, blank], axis=0).T.astype(bf16)

    def correction(layer, g, p):
        start = pl.multiple_of(me * width + p * piece, lanes)
        factor = factor_slice(fout_ref, layer, g, start, piece)
        right = jnp.concatenate(
            [factor, factor, jnp.zeros((lanes - 2 * factor_rows, piece), bf16)], axis=0
        )
        return jnp.dot(lows[g], right, preferred_element_type=f32)

    for copy in loads[:2]:
        copy.wait()
    for p in range(1, parts):
        for slot in range(2):
            column_copy(slot, p).start()
    def relay_copy(way, hop, source):
        return remote(
            granks_ref.at[twin, source],
            granks_ref.at[twin, source],
            relay_send.at[way, hop - 1],
            relay_recv.at[way, hop - 1],
            at_line(line + 1) if way == 0 else at_line(line - 1),
            me,
        )

    def relay_each(hop, act, sending):
        shift = hop - 1 if sending else hop
        right = (line >= shift) & (line < outer - 1) if sending else line >= shift
        left = (line + shift < outer) & (line > 0) if sending else line + shift < outer

        @pl.when(right)
        def _():
            act(relay_copy(0, hop, line - shift))

        @pl.when(left)
        def _():
            act(relay_copy(1, hop, line + shift))

    def relay_start(hop):
        relay_each(hop, lambda copy: copy.start(), True)

    def relay_next(hop):
        relay_each(hop, lambda copy: copy.wait_recv(), False)
        if hop + 1 < outer:
            relay_start(hop + 1)

    plane = remote(granks_ref.at[twin], granks_ref.at[twin], plane_send, plane_recv, buddy, me)
    plane_in = remote(
        granks_ref.at[1 - twin], granks_ref.at[1 - twin], plane_send, plane_recv, buddy, me
    )

    def part_copy(slot, p):
        return remote(
            own_part.at[slot, p],
            got_part.at[slot, p],
            part_send,
            part_recv.at[slot, p],
            mine,
            mate,
        )

    def own_rows(q):
        return pl.ds(pl.multiple_of(q * local, local), local)

    def in_copy(way, hop, source):
        return remote(
            fin_ref,
            gin_ref.at[:, own_rows(at_line(source)), :],
            in_send,
            in_recv.at[way, hop - 1],
            at_line(line + hop) if way == 0 else at_line(line - hop),
            me,
        )

    def in_start(hop):
        @pl.when(line + hop < outer)
        def _():
            in_copy(0, hop, line).start()

        @pl.when(line >= hop)
        def _():
            in_copy(1, hop, line).start()

    def in_pass(hop):
        @pl.when(line >= hop)
        def _():
            in_copy(0, hop, line - hop).wait_recv()
            pass_copy(line - hop, twin).start()

        @pl.when(line + hop < outer)
        def _():
            in_copy(1, hop, line + hop).wait_recv()
            pass_copy(line + hop, twin).start()

    def in_buddy(source):
        return remote(
            fin_ref,
            gin_ref.at[:, own_rows(source), :],
            in_send,
            buddy_recv,
            buddy,
            me,
        )

    def pass_copy(place, side_of):
        at = own_rows(place * 2 + side_of)
        return remote(
            gin_ref.at[:, at, :],
            gin_ref.at[:, at, :],
            pass_send,
            pass_recv,
            buddy,
            me,
        )

    def out_copy(hop, source):
        target = lax.rem(mine + hop, pop)
        cols = pl.multiple_of(target * columns, lanes)
        return remote(
            fout_ref.at[core, :, pl.ds(cols, columns)],
            gout_ref.at[core, own_rows(source), :],
            out_send,
            out_recv,
            target,
            me,
        )

    def stretch(ref, count):
        return ref.at[pl.ds(0, count * local), :]

    def whole_out():
        spot = stretch(gout_ref.at[core], pop - 1)
        return remote(spot, spot, out_send, out_recv, buddy, me)

    def whole_pass():
        spot = gin_ref.at[:, pl.ds(0, (outer - 1) * local), :]
        return remote(spot, spot, pass_send, pass_recv, buddy, me)

    def whole_in():
        spot = gin_ref.at[:, pl.ds(0, outer * local), :]
        return remote(spot, spot, in_send, buddy_recv, buddy, me)

    def half_copy(which):
        return remote(
            gout_ref.at[which],
            gout_ref.at[which],
            half_send,
            half_recv,
            mine,
            mate,
        )

    def self_copies():
        cols = pl.multiple_of(mine * columns, lanes)
        return (
            pltpu.make_async_copy(fin_ref, gin_ref.at[:, own_rows(mine), :], self_sem.at[0]),
            pltpu.make_async_copy(
                fout_ref.at[core, :, pl.ds(cols, columns)],
                gout_ref.at[core, own_rows(mine), :],
                self_sem.at[1],
            ),
        )

    spans = (pl.ds(0, share), pl.ds(share, vocab - 2 * share))

    def over_copy(h, p):
        return remote(
            own_over.at[p, spans[h]],
            got_over.at[p, spans[h]],
            over_send,
            over_recv.at[h, p],
            mine,
            cross,
        )

    def hand_copy(p, half):
        at = pl.ds(pl.multiple_of(half * share, share), share)
        return remote(
            table.at[p, at],
            table.at[p, at],
            hand_send,
            hand_recv.at[p],
            buddy,
            me,
        )

    def entry(slot, p):
        return jnp.dot(
            rows_embed[...], weights[slot, :, halves[p]], preferred_element_type=f32
        ).astype(bf16)

    def part_put(p):
        column_copy(0, p).wait()
        own_part[0, p] = entry(0, p)

    def part_make(p):
        column_copy(1, p).wait()
        own_over[p] = entry(1, p)

    def part_sum(p):
        part_copy(0, p).wait_recv()
        own_over[p] = (own_over[p].astype(f32) + got_part[0, p].astype(f32)).astype(bf16)
        over_copy(0, p).start()

    with jax.named_scope("tab0"):
        part_put(0)
    with jax.named_scope("bar"):
        pl.semaphore_wait(
            barrier,
            4 + jnp.where(line < outer - 1, 1, 0) + jnp.where(line > 0, 1, 0),
        )

    relay_start(1)
    with jax.named_scope("tab1"):
        part_copy(0, 0).start()
        for copy in loads[2:5]:
            copy.start()
        for slot in range(2, 4):
            weight_copy(0, slot).start()
        for copy in loads[5:]:
            copy.start()
        part_make(0)
        for p in range(1, parts):
            part_put(p)
            part_copy(0, p).start()
            if p > 1:
                part_make(p - 1)
            part_sum(p - 1)
        part_make(parts - 1)
        part_sum(parts - 1)
        weight_copy(1, 0).start()
        weight_copy(1, 1).start()
    over_copy(1, 0).start()
    def begin(g):
        tokens = jnp.concatenate(
            [ids_ref[g * member_rows + m] for m in range(member_rows)], axis=0
        )
        entries = lax.broadcasted_iota(jnp.int32, (group, vocab), 1)
        for t in range(steps):
            onehot_ref[g, t * group : (t + 1) * group, :] = jnp.where(
                tokens[:, t : t + 1] == entries, 1.0, 0.0
            ).astype(bf16)
        features = jnp.dot(onehot_ref[g], embed_ref[...], preferred_element_type=f32).astype(bf16)
        hidden[g] = features
        low_put(0, g, against(factor_slice(fin_ref, 0, g, 0, width), features))

    def both(h, p):
        at = spans[h]
        return (
            mine_part[p, at].astype(f32) + got_part[1, p, at].astype(f32)
        ) + got_over[p, at].astype(f32)

    def lead_pair(k):
        return remote(
            own_lead.at[k], got_lead.at[k], lead_send, lead_recv.at[k], mine, mate
        )

    def lead_cross(k):
        return remote(own_ahead.at[k], got_ahead.at[k], ahead_send, ahead_recv, mine, cross)

    def lead_dot(k, slot):
        left = lifted[...] if k else hidden[0]
        return jnp.dot(
            left, weights[slot, :, halves[0]], preferred_element_type=f32
        ).astype(bf16)

    def lead_put(k):
        own_lead[k] = lead_dot(k, 0)
        lead_pair(k).start()

    def lead_sum(k):
        value = lead_dot(k, 1).astype(f32)
        lead_pair(k).wait_recv()
        own_ahead[k] = (value + got_lead[k].astype(f32)).astype(bf16)
        lead_cross(k).start()

    def wait_weights(half):
        spot = weights.at[pl.ds(2 * half, 2)]
        pltpu.make_async_copy(spot, spot, weight_sem.at[2 + half]).wait()

    with jax.named_scope("tab2"):
        for copy in loads[2:5]:
            copy.wait()
        unpack(fin_raw, fin_ref)
        weight_copy(0, 2).wait()
        for p in range(parts):
            own_part[1, p] = entry(2, p)
            part_copy(1, p).start()
        weight_copy(1, 2).start()
    with jax.named_scope("relay1"):
        relay_next(1)
        in_start(1)
    weight_copy(0, 3).wait()
    issued = 1
    first = min(max(chunks - 1, 1), parts)
    for p in range(parts):
        if p < first:
            with jax.named_scope("begin%d" % p):
                begin(p)
                low_copy(0, p, 0).start()
            if issued < parts:
                over_copy(1, issued).start()
                issued += 1
        with jax.named_scope("tabA%d" % p):
            mine_part[p] = entry(3, p)
            part_copy(1, p).wait_recv()
            over_copy(0, p).wait_recv()
            at = pl.ds(pl.multiple_of(twin * share, share), share)
            table[p, at] = both(0, p).astype(bf16)
            hand_copy(p, twin).start()
    for p in range(issued, parts):
        over_copy(1, p).start()
    weight_copy(1, 3).start()
    in_buddy(mine).start()
    with jax.named_scope("prep"):
        for copy in loads[5:]:
            copy.wait()
        unpack(fout_raw, fout_ref)
        reward = reward_ref[...]
        high = reward.astype(bf16).astype(f32)
        middle = (reward - high).astype(bf16).astype(f32)
        rest = reward - high - middle
        index = lax.broadcasted_iota(jnp.int32, (16, width), 0)
        heads[...] = jnp.where(
            index == 0,
            high,
            jnp.where(index == 1, middle, jnp.where(index == 2, rest, 0.0)),
        ).astype(bf16)

    wait_weights(0)
    with jax.named_scope("leadx"):
        lead_put(0)
        for g in range(first, chunks):
            begin(g)
            low_copy(0, g, 0).start()
        lead_sum(0)
    with jax.named_scope("folds"):
        for g in range(max(chunks - 1, 1)):
            low_fold(0, g)
    with jax.named_scope("relay2"):
        if outer > 2:
            relay_next(2)
            in_start(2)

    def recur(layer, g, p, inputs):
        decay = decay_ref[layer : layer + 1, halves[p]]
        kept = 1.0 - decay
        carried = jnp.zeros((group, piece), f32)
        if layer:
            lean = gain_ref[layer : layer + 1, halves[p]] * reward_ref[:, halves[p]]
        for t in range(steps):
            at = slice(t * group, (t + 1) * group)
            carried = decay * carried + kept * inputs[at]
            if not layer:
                states[g, at, halves[p]] = carried
            elif t == steps - 1:
                lasts[g, :, halves[p]] = carried
            powers = carried * carried
            total = powers[:, :lanes]
            for c in range(lanes, piece, lanes):
                total = total + powers[:, c : c + lanes]
            if p:
                total = total + squares[g, at, :]
            squares[g, at, :] = total
            if layer:
                leaning = carried * lean
                total = leaning[:, :lanes]
                for c in range(lanes, piece, lanes):
                    total = total + leaning[:, c : c + lanes]
                if p:
                    total = total + leans[g, at, :]
                leans[g, at, :] = total

    def across(value):
        return jnp.sum(value.T, axis=0, keepdims=True)

    def squares_start(g):
        small[2, g, 0] = jnp.broadcast_to(across(squares[g]), (4, rows))
        small_start(2, g)

    def complete(p):
        with jax.named_scope("tabB%d" % p):
            over_copy(1, p).wait_recv()
            table[p, 2 * share :] = both(1, p).astype(bf16)
        with jax.named_scope("hand%d" % p):
            hand_copy(p, 1 - twin).wait_recv()

    def layer_zero(g, p):
        with jax.named_scope("lz%d_%d" % (g, p)):
            inputs = jnp.dot(
                onehot_ref[g], table[p], preferred_element_type=f32
            ) + correction(0, g, p)
            recur(0, g, p, inputs)

    late = parts - 1

    low_ready(0, 0)
    for p in range(late):
        complete(p)
        layer_zero(0, p)
    for g in range(1, chunks - 1):
        low_ready(0, g)
        for p in range(min(2, late)):
            layer_zero(g, p)
    if chunks > 1:
        low_fold(0, chunks - 1)
    complete(late)
    layer_zero(0, late)
    squares_start(0)
    with jax.named_scope("leadv"):
        lifted[...] = (states[0] * gain_ref[0:1, :]).astype(bf16)
        lead_put(1)
    for g in range(1, chunks - 1):
        for p in range(min(2, late), late):
            layer_zero(g, p)
    if chunks > 1:
        low_ready(0, chunks - 1)
        for p in range(late):
            layer_zero(chunks - 1, p)
    with jax.named_scope("leadw"):
        lead_sum(1)
    for g in range(1, chunks):
        layer_zero(g, late)
        squares_start(g)

    def pair_copy(g, slot, p):
        return remote(
            own_pair.at[g, slot, p],
            got_pair.at[g, slot, p],
            pair_send.at[2 if g else slot],
            pair_recv.at[g, 1] if slot else lone_recv.at[p] if g == 0 else pair_recv.at[g, 0],
            mine,
            mate,
        )

    def whole_pair(g, slot):
        return remote(
            own_pair.at[g, slot],
            got_pair.at[g, slot],
            pair_send.at[2 if g else slot],
            pair_recv.at[g, slot],
            mine,
            mate,
        )

    def cross_copy(g, p):
        return remote(
            own_cross.at[g, p],
            got_cross.at[g, p],
            cross_send.at[1 if g else 0],
            cross_recv.at[parts + g if g < chunks - 1 else p],
            mine,
            cross,
        )

    def whole_cross(g):
        at = pl.ds(0 if g else 1, parts if g else late)
        return remote(
            own_cross.at[g, at],
            got_cross.at[g, at],
            cross_send.at[1 if g else 0],
            cross_recv.at[parts + g],
            mine,
            cross,
        )

    def shape_ranks():
        full_block = (2, outer, 8, lanes)
        kept = (lax.broadcasted_iota(jnp.int32, full_block, 2) == 0) & (
            lax.broadcasted_iota(jnp.int32, full_block, 3) < members
        )
        shares = jnp.where(kept, granks_ref[...].astype(f32) / members_all, 0.0)

        def mean_of(value):
            value = jnp.sum(value, axis=0)
            value = jnp.sum(value, axis=0)
            value = jnp.sum(value, axis=0, keepdims=True)
            return jnp.sum(value, axis=1, keepdims=True) / members_all

        rank_mean = mean_of(shares)
        apart = jnp.where(kept, shares - rank_mean[None, None], 0.0)
        spread = mean_of(apart * apart) + spread_eps
        owner = lax.broadcasted_iota(jnp.int32, (local, lanes), 0) // rank
        own = owner == lax.broadcasted_iota(jnp.int32, (local, lanes), 1)
        for place in range(outer):
            for side_of in range(2):
                share_row = granks_ref[side_of, place, 0:1].astype(f32) / members_all
                shaped = (share_row - rank_mean) * lax.rsqrt(spread)
                shaped = jnp.where(own, jnp.broadcast_to(shaped, (local, lanes)), 0.0)
                shaped = jnp.sum(shaped, axis=1, keepdims=True)
                at = (place * 2 + side_of) * local
                shaped_ref[at : at + local] = jnp.broadcast_to(shaped, (local, lanes))

    def out_start():
        with jax.named_scope("outs"):
            plane_in.wait_recv()
            for hop in range(1, pop):
                out_copy(hop, mine).start()
            for copy in self_copies():
                copy.start()

    def gather_half():
        with jax.named_scope("half"):
            whole_out().wait_recv()
            for copy in self_copies():
                copy.wait()
            half_copy(core).start()

    def step_make():
        tile = 256
        with jax.named_scope("arrive"):
            in_buddy(buddy).wait_recv()
        with jax.named_scope("arrive_pass"):
            whole_pass().wait_recv()
        with jax.named_scope("arrive_half"):
            half_copy(1 - core).wait_recv()
        with jax.named_scope("step"):
            shape_ranks()
            shaped = jnp.concatenate([shaped_ref[...]] * (tile // lanes), axis=1)
            for layer in range(layers):
                for at in range(0, width, tile):
                    factor = gin_ref[layer, :, at : at + tile].astype(f32)
                    value = lax.dot_general(
                        (factor * shaped).astype(bf16),
                        gout_ref[layer],
                        (((0,), (0,)), ((), ())),
                        preferred_element_type=f32,
                    )
                    step_ref[layer, at : at + tile] = value * (members_all * rank) ** (-0.5)

    def between(g):
        if g == 0:
            wait_weights(1)
        with jax.named_scope("normed%d" % g):
            total = small_sum(2, g)[:1]
            scale = lax.rsqrt(total / full + norm_eps)
            scale = jnp.broadcast_to(scale, (lanes, rows)).T
            if g == 0:
                lead_scale[...] = scale
            scale = jnp.concatenate([scale] * (width // lanes), axis=1)
            gain = gain_ref[0:1, :]
            hidden[g] = (hidden[g].astype(f32) + states[g] * scale * gain).astype(bf16)

        def product(slot, p):
            return jnp.dot(
                hidden[g], weights[slot, :, halves[p]], preferred_element_type=f32
            ).astype(bf16)

        with jax.named_scope("exch%d" % g):
            def summed(p):
                value = product(1, p).astype(f32)
                if g == 0:
                    pair_copy(g, 0, p).wait_recv()
                elif p == 0:
                    whole_pair(g, 0).wait_recv()
                total = (value + got_pair[g, 0, p].astype(f32)).astype(bf16)
                own_cross[g, p] = total
                cross_copy(g, p).start()

            for p in range(0 if g else 1, parts):
                own_pair[g, 0, p] = product(0, p)
                pair_copy(g, 0, p).start()
                if p > 1 and g == 0:
                    summed(p - 1)
            left = jnp.concatenate([factor_slice(fin_ref, 1, g, 0, width), heads[...]], axis=0)
            local_low = against(left, hidden[g])
            low_put(1, g, local_low[:factor_rows])
            low_copy(1, g, 0).start()
            aligned = local_low[factor_rows : factor_rows + 8]
            alphas[g] = jnp.broadcast_to(jnp.sum(aligned, axis=0, keepdims=True), (8, rows))
            for p in range(0 if g else parts - 1, parts):
                summed(p)
            for p in range(parts):
                own_pair[g, 1, p] = product(2, p)
                pair_copy(g, 1, p).start()
            for p in range(parts):
                states[g, :, halves[p]] = product(3, p).astype(f32)

    def layer_one(g):
        with jax.named_scope("lowone%d" % g):
            low_ready(1, g)
        for p in range(parts):
            with jax.named_scope("l1_%d_%d" % (g, p)):
                if p == 0:
                    whole_pair(g, 1).wait_recv()
                fixed = (
                    states[g, :, halves[p]] + got_pair[g, 1, p].astype(f32)
                ) + correction(1, g, p)
                if g == 0 and p == 0:
                    remote(own_ahead, got_ahead, ahead_send, ahead_recv, mine, cross).wait_recv()
                    scale = jnp.concatenate([lead_scale[...]] * (piece // lanes), axis=1)
                    other = got_ahead[0].astype(f32) + scale * got_ahead[1].astype(f32)
                else:
                    if g == chunks - 1:
                        cross_copy(g, p).wait_recv()
                    elif p == (0 if g else 1):
                        whole_cross(g).wait_recv()
                    other = got_cross[g, p].astype(f32)
                recur(1, g, p, fixed + other)
        with jax.named_scope("end%d" % g):
            small[3, g, 0] = jnp.concatenate(
                [across(squares[g]), across(leans[g]), alphas[g][:2]], axis=0
            )
            small_start(3, g)

    with jax.named_scope("relay3"):
        for hop in range(3, outer):
            relay_next(hop)
            in_start(hop)
        plane.start()
    with jax.named_scope("pass1"):
        in_pass(1)
    for g in range(chunks):
        between(g)
        if g == 0:
            out_start()
        with jax.named_scope("pass"):
            for hop in range(g + 1, min(g + 2, outer) if g else 0):
                in_pass(hop)
    for g in range(chunks):
        if g < chunks - 1:
            low_fold(1, g)
        else:
            with jax.named_scope("pass"):
                for hop in range(chunks + 1, outer):
                    in_pass(hop)
            gather_half()
            if g:
                layer_one(g - 1)
            low_fold(1, g)
            step_make()
            layer_one(g)
        if g < chunks - 2:
            layer_one(g)

    lane = lax.broadcasted_iota(jnp.int32, (seqs, lanes), 1)
    scores = jnp.zeros((seqs, lanes), f32)
    with jax.named_scope("final"):
        for g in range(chunks):
            sums = small_sum(3, g)
            scale = lax.rsqrt(sums[0:1] / full + norm_eps)
            value = sums[2:3] + scale * sums[1:2]
            total = value[:, :lanes]
            for c in range(lanes, rows, lanes):
                total = total + value[:, c : c + lanes]
            total = jnp.broadcast_to(total, (8, lanes))
            shift = lanes // 2
            while shift >= group:
                total = total + pltpu.roll(total, shift, 1)
                shift //= 2
            total = total * (full ** (-0.5) / steps)
            total = jnp.broadcast_to(total[:1], (lanes, lanes)).T
            for m in range(member_rows):
                scores = jnp.where(
                    lane == g * member_rows + m, total[m * seqs : (m + 1) * seqs], scores
                )
            ending = jnp.broadcast_to(scale[:, rows - lanes :], (lanes, lanes)).T[lanes - group :]
            ending = jnp.concatenate([ending] * (width // lanes), axis=1)
            gain = gain_ref[1:2, :]
            ending = (
                hidden[g, rows - group :].astype(f32) + lasts[g] * ending * gain
            ).astype(bf16).astype(f32)
            for m in range(member_rows):
                final_ref[g * member_rows + m] = ending[m * seqs : (m + 1) * seqs].astype(bf16)
        score_ref[...] = scores[:, :members]

    with jax.named_scope("drain"):
        for hop in range(1, outer):
            relay_each(hop, lambda copy: copy.wait_send(), True)
        plane.wait_send()
        remote(own_part, got_part, part_send, part_recv.at[0, 0], mine, mate).wait_send()
        remote(own_over, got_over, over_send, over_recv.at[0, 0], mine, cross).wait_send()
        spot = table.at[:, pl.ds(0, share)]
        remote(spot, spot, hand_send, hand_recv.at[0], buddy, me).wait_send()
        spot = own_pair.at[0, 0, pl.ds(1, late)]
        remote(spot, spot, pair_send.at[0], pair_recv.at[0, 0], mine, mate).wait_send()
        spot = own_pair.at[0, 1]
        remote(spot, spot, pair_send.at[1], pair_recv.at[0, 0], mine, mate).wait_send()
        spot = own_cross.at[0, pl.ds(1, late)]
        remote(spot, spot, cross_send.at[0], cross_recv.at[0], mine, cross).wait_send()
        if chunks > 1:
            spot = own_pair.at[pl.ds(1, chunks - 1)]
            remote(spot, spot, pair_send.at[2], pair_recv.at[0, 0], mine, mate).wait_send()
        if chunks > 1:
            spot = own_cross.at[pl.ds(1, chunks - 1)]
            remote(spot, spot, cross_send.at[1], cross_recv.at[0], mine, cross).wait_send()
        remote(own_lead, got_lead, lead_send, lead_recv.at[0], mine, mate).wait_send()
        remote(own_ahead, got_ahead, ahead_send, ahead_recv, mine, cross).wait_send()
        spot = small.at[pl.ds(0, 2), :, pl.ds(0, 2)]
        remote(spot, spot, low_send, low_recv.at[0, 0, 0], mine, mate).wait_send()
        spot = small.at[pl.ds(2, 2), :, pl.ds(1, 3)]
        remote(spot, spot, small_send, small_recv.at[0, 0], mine, mate).wait_send()
        whole_in().wait_send()
        whole_pass().wait_send()
        whole_out().wait_send()
        half_copy(core).wait_send()


cuts = 2


def publish(final_ref, score_ref, step_ref, final_out, score_out, step_out, sems):
    copies = []
    layers, width, _ = step_ref.shape
    cut = width // cuts
    for layer in range(layers):
        for c in range(cuts):
            at = pl.ds(c * cut, cut)
            copies.append(
                pltpu.make_async_copy(
                    step_ref.at[layer, at], step_out.at[layer, at], sems.at[layer, c]
                )
            )
    copies.append(pltpu.make_async_copy(final_ref, final_out, sems.at[layers, 0]))
    copies.append(pltpu.make_async_copy(score_ref, score_out, sems.at[layers, 1]))
    for copy in copies:
        copy.start()
    for copy in copies:
        copy.wait()


def shards(
    token_ids,
    fitness_ranks,
    embedding,
    mix_weights,
    factors_in,
    factors_out,
    decay_rates,
    norm_gain,
    reward_dir,
):
    members, seqs, steps = token_ids.shape
    vocab, width = embedding.shape
    layers, _, full = mix_weights.shape
    rank = factors_in.shape[2]
    pop = lax.axis_size("pop")
    outer = pop // 2
    coef = noise_scale * (full * rank) ** (-0.5)
    columns = full // pop
    member_rows = 16 // seqs
    chunks = members // member_rows
    group = member_rows * seqs
    rows = group * steps
    local = members * rank
    share = vocab * 5 // 16
    dims = (pop, chunks, group, steps, member_rows, seqs, rank, width, full, coef, share)
    vmem = pl.BlockSpec(memory_space=pltpu.VMEM)
    smem = pl.BlockSpec(memory_space=pltpu.SMEM)
    hbm = pl.BlockSpec(memory_space=pltpu.HBM)
    parts = 4
    piece = width // parts
    entries = vocab - share
    dma = pltpu.SemaphoreType.DMA
    final_features, scores, step = pl.pallas_call(
        functools.partial(policy_kernel, dims),
        out_shape=(
            pltpu.VMEM((members, seqs, width), bf16),
            pltpu.VMEM((seqs, members), f32),
            pltpu.VMEM((layers, width, columns), f32),
        ),
        in_specs=[hbm, hbm, hbm, hbm, hbm, smem, hbm, hbm, hbm],
        out_specs=(vmem, vmem, vmem),
        scratch_shapes=[
            pltpu.VMEM((members, seqs, steps), jnp.int32),
            pltpu.VMEM((vocab, width), bf16),
            pltpu.VMEM((layers, members, rank, width), bf16),
            pltpu.VMEM((layers, members, rank, full), bf16),
            pltpu.VMEM((layers, width), f32),
            pltpu.VMEM((layers, width), f32),
            pltpu.VMEM((1, width), f32),
            pltpu.VMEM((4, width, width), bf16),
            pltpu.VMEM((entries, width), bf16),
            pltpu.VMEM((2, parts, entries, piece), bf16),
            pltpu.VMEM((2, parts, entries, piece), bf16),
            pltpu.VMEM((parts, entries, piece), bf16),
            pltpu.VMEM((parts, entries, piece), bf16),
            pltpu.VMEM((parts, entries, piece), bf16),
            pltpu.VMEM((parts, vocab, piece), bf16),
            pltpu.VMEM((chunks, 2, parts, rows, piece), bf16),
            pltpu.VMEM((chunks, 2, parts, rows, piece), bf16),
            pltpu.VMEM((chunks, parts, rows, piece), bf16),
            pltpu.VMEM((chunks, parts, rows, piece), bf16),
            pltpu.VMEM((2, rows, piece), bf16),
            pltpu.VMEM((2, rows, piece), bf16),
            pltpu.VMEM((2, rows, piece), bf16),
            pltpu.VMEM((2, rows, piece), bf16),
            pltpu.VMEM((rows, width), bf16),
            pltpu.VMEM((rows, lanes), f32),
            pltpu.VMEM((chunks, rows, width), f32),
            pltpu.VMEM((chunks, rows, width), bf16),
            pltpu.VMEM((chunks, rows, vocab), bf16),
            pltpu.VMEM((layers, local, width), bf16),
            pltpu.VMEM((layers, local, full), bf16),
            pltpu.VMEM((pop * local, lanes), f32),
            pltpu.VMEM((layers, pop * local, width), bf16),
            pltpu.VMEM((layers, pop * local, columns), bf16),
            pltpu.VMEM((2, outer, 8, lanes), jnp.int32),
            pltpu.VMEM((chunks, rows, lanes), bf16),
            pltpu.VMEM((chunks, rows, lanes), f32),
            pltpu.VMEM((chunks, rows, lanes), f32),
            pltpu.VMEM((chunks, group, width), f32),
            pltpu.VMEM((16, width), bf16),
            pltpu.VMEM((chunks, 8, rows), f32),
            pltpu.VMEM((4, chunks, 4, 4, rows), f32),
            dma((4,)),
            dma((2, parts)),
            dma((9,)),
            dma,
            dma((2, parts)),
            dma,
            dma((2, parts)),
            dma,
            dma((parts,)),
            dma((3,)),
            dma((chunks, 2)),
            dma((parts,)),
            dma((2,)),
            dma((parts + chunks - 1,)),
            dma,
            dma((2,)),
            dma,
            dma,
            dma,
            dma((2, chunks)),
            dma,
            dma((2, 2, chunks)),
            dma((2, outer - 1)),
            dma((2, outer - 1)),
            dma,
            dma,
            dma,
            dma((2, outer - 1)),
            dma,
            dma,
            dma,
            dma,
            dma,
            dma,
            dma,
            dma((2,)),
        ],
        compiler_params=pltpu.CompilerParams(
            collective_id=0, has_side_effects=True, vmem_limit_bytes=52 * 1024 * 1024
        ),
    )(
        *(
            pltpu.with_memory_space_constraint(value, pltpu.HBM)
            for value in (
                token_ids,
                embedding,
                mix_weights,
                factors_in,
                factors_out,
                fitness_ranks,
                decay_rates,
                norm_gain,
                reward_dir.reshape(1, width),
            )
        )
    )
    final_features, scores, weight_step = pl.pallas_call(
        publish,
        out_shape=(
            jax.ShapeDtypeStruct((members, seqs, width), bf16),
            jax.ShapeDtypeStruct((seqs, members), f32),
            jax.ShapeDtypeStruct((layers, width, columns), f32),
        ),
        in_specs=[vmem, vmem, vmem],
        out_specs=(hbm, hbm, hbm),
        scratch_shapes=[dma((layers + 1, cuts))],
        compiler_params=pltpu.CompilerParams(vmem_limit_bytes=1024 * 1024),
    )(final_features, scores, step)
    return (final_features, scores.T, weight_step)


def solution(mesh):
    return jax.shard_map(
        shards,
        mesh=mesh,
        in_specs=(
            P("pop", None, None),
            P("pop"),
            P(None, "mp"),
            P(None, "mp", None),
            P(None, "pop", None, "mp"),
            P(None, "pop", None, None),
            P(None, "mp"),
            P(None, "mp"),
            P("mp"),
        ),
        out_specs=(P("pop", None, "mp"), P("pop", None), P(None, "mp", "pop")),
        check_vma=False,
    )
```

```python
import functools

import jax
import jax.numpy as jnp
from jax import lax
from jax.experimental import pallas as pl
from jax.experimental.pallas import tpu as pltpu
from jax.sharding import PartitionSpec as P

noise_scale = 0.25
norm_eps = 1e-06
spread_eps = 1e-05
lanes = 128
f32, bf16 = jnp.float32, jnp.bfloat16


def policy_kernel(
    dims,
    ids_hbm,
    embed_hbm,
    mix_ref,
    fin_hbm,
    fout_hbm,
    ranks_smem,
    decay_hbm,
    gain_hbm,
    reward_hbm,
    final_ref,
    score_ref,
    step_ref,
    ids_ref,
    embed_ref,
    fin_raw,
    fout_raw,
    decay_ref,
    gain_ref,
    reward_ref,
    weights,
    rows_embed,
    own_part,
    got_part,
    own_over,
    got_over,
    mine_part,
    table,
    own_pair,
    got_pair,
    own_cross,
    got_cross,
    own_lead,
    got_lead,
    own_ahead,
    got_ahead,
    lifted,
    lead_scale,
    states,
    hidden,
    onehot_ref,
    fin_ref,
    fout_ref,
    shaped_ref,
    gin_ref,
    gout_ref,
    granks_ref,
    lows,
    squares,
    leans,
    lasts,
    heads,
    alphas,
    small,
    weight_sem,
    column_sem,
    load_sem,
    part_send,
    part_recv,
    over_send,
    over_recv,
    hand_send,
    hand_recv,
    pair_send,
    pair_recv,
    lone_recv,
    cross_send,
    cross_recv,
    lead_send,
    lead_recv,
    ahead_send,
    ahead_recv,
    small_send,
    small_recv,
    low_send,
    low_recv,
    relay_send,
    relay_recv,
    plane_send,
    plane_recv,
    in_send,
    in_recv,
    buddy_recv,
    pass_send,
    pass_recv,
    out_send,
    out_recv,
    half_send,
    half_recv,
    self_sem,
):
    pop, chunks, group, steps, member_rows, seqs, rank, width, full, coef, share = dims
    parts = hand_recv.shape[0]
    piece = width // parts
    halves = [slice(p * piece, (p + 1) * piece) for p in range(parts)]
    rows = group * steps
    vocab = embed_ref.shape[0]
    members = ids_ref.shape[0]
    members_all = members * pop
    layers, local = fin_ref.shape[0], fin_ref.shape[1]
    columns = gout_ref.shape[2]
    mine = lax.axis_index("pop")
    me = lax.axis_index("mp")
    side, core = me // 2, me % 2
    mate = side * 2 + (1 - core)
    cross = (1 - side) * 2 + core
    diagonal = (1 - side) * 2 + (1 - core)
    others = (mate, cross, diagonal)
    blocks = (diagonal, cross, mate, me)
    outer = pop // 2
    line, twin = mine // 2, mine % 2
    buddy = line * 2 + (1 - twin)

    def at_line(place):
        return place * 2 + twin

    def peer(q, j):
        return {"pop": q, "mp": j}

    def remote(src, dst, send, recv, q, j):
        return pltpu.make_async_remote_copy(
            src_ref=src,
            dst_ref=dst,
            send_sem=send,
            recv_sem=recv,
            device_id=peer(q, j),
            device_id_type=pl.DeviceIdType.MESH,
        )

    barrier = pltpu.get_barrier_semaphore()

    def greet(q, j):
        pl.semaphore_signal(
            barrier, inc=1, device_id=peer(q, j), device_id_type=pl.DeviceIdType.MESH
        )

    for other in others:
        greet(mine, other)
    greet(buddy, me)

    @pl.when(line < outer - 1)
    def _():
        greet(at_line(line + 1), me)

    @pl.when(line > 0)
    def _():
        greet(at_line(line - 1), me)

    def weight_copy(layer, slot):
        start = pl.multiple_of(blocks[slot] * width, lanes)
        return pltpu.make_async_copy(
            mix_ref.at[layer, :, pl.ds(start, width)],
            weights.at[slot],
            weight_sem.at[2 + slot // 2 if layer else slot - 2],
        )

    def column_copy(slot, p):
        start = pl.multiple_of(blocks[slot] * width + p * piece, lanes)
        return pltpu.make_async_copy(
            mix_ref.at[0, :, pl.ds(start, piece)],
            weights.at[slot, :, halves[p]],
            column_sem.at[slot, p],
        )

    loads = [
        pltpu.make_async_copy(src, dst, load_sem.at[i])
        for i, (src, dst) in enumerate(
            (
                (
                    embed_hbm.at[pl.ds(pl.multiple_of(twin * share, share), share)],
                    rows_embed.at[pl.ds(0, share)],
                ),
                (
                    embed_hbm.at[pl.ds(2 * share, embed_ref.shape[0] - 2 * share)],
                    rows_embed.at[pl.ds(share, embed_ref.shape[0] - 2 * share)],
                ),
                (embed_hbm, embed_ref),
                (ids_hbm, ids_ref),
                (fin_hbm, fin_raw),
                (decay_hbm, decay_ref),
                (gain_hbm, gain_ref),
                (reward_hbm, reward_ref),
                (fout_hbm, fout_raw),
            )
        )
    ]
    for copy in loads[:2]:
        copy.start()
    for slot in range(2):
        column_copy(slot, 0).start()

    def rank_block(shape, axis, repeats):
        index = lax.broadcasted_iota(jnp.int32, shape, axis)
        block = jnp.zeros(shape, jnp.int32)
        for m in range(members):
            block = jnp.where(index // repeats == m, ranks_smem[m], block)
        return block

    granks_ref[twin, line] = rank_block((8, lanes), 1, 1)

    def unpack(raw, ref):
        def one(g, carry):
            at = pl.ds(
                pl.multiple_of(g * member_rows * rank, member_rows * rank), member_rows * rank
            )
            for layer in range(layers):
                ref[layer, at, :] = jnp.concatenate(
                    [raw[layer, g * member_rows + m].astype(f32) for m in range(member_rows)],
                    axis=0,
                ).astype(bf16)
            return carry

        lax.fori_loop(0, chunks, one, 0)

    factor_rows = member_rows * rank
    mask = (lax.broadcasted_iota(jnp.int32, (factor_rows, rows), 0) // rank) == (
        (lax.broadcasted_iota(jnp.int32, (factor_rows, rows), 1) % group) // seqs
    )

    def factor_slice(ref, layer, g, start, size):
        at = pl.multiple_of(g * factor_rows, factor_rows)
        return ref[layer, pl.ds(at, factor_rows), pl.ds(start, size)]

    def small_copy(kind, g, r):
        return remote(
            small.at[kind, g, 0],
            small.at[kind, g, r + 1],
            small_send,
            small_recv.at[kind - 2, g],
            mine,
            others[r],
        )

    def small_start(kind, g):
        for r in range(3):
            small_copy(kind, g, r).start()

    def small_sum(kind, g):
        arrived = small.at[kind, g, pl.ds(1, 3)]
        remote(arrived, arrived, small_send, small_recv.at[kind - 2, g], mine, mate).wait_recv()
        return (small[kind, g, 0] + small[kind, g, 1]) + (small[kind, g, 2] + small[kind, g, 3])

    def low_copy(layer, g, stage):
        return remote(
            small.at[layer, g, 2 * stage],
            small.at[layer, g, 2 * stage + 1],
            low_send,
            low_recv.at[layer, stage, g],
            mine,
            mate if stage else cross,
        )

    def low_fold(layer, g):
        low_copy(layer, g, 0).wait_recv()
        small[layer, g, 2] = small[layer, g, 0] + small[layer, g, 1]
        low_copy(layer, g, 1).start()

    def against(left, features):
        return lax.dot_general(
            left, features, (((1,), (1,)), ((), ())), preferred_element_type=f32
        )

    def low_put(layer, g, local_low):
        local_low = jnp.where(mask, local_low, 0.0)
        packed = local_low[:rank]
        for at in range(rank, factor_rows, rank):
            packed = packed + local_low[at : at + rank]
        small[layer, g, 0] = packed

    def low_ready(layer, g):
        low_copy(layer, g, 1).wait_recv()
        packed = small[layer, g, 2] + small[layer, g, 3]
        low = jnp.concatenate([packed] * member_rows, axis=0)
        low = jnp.where(mask, low, 0.0) * coef
        top = low.astype(bf16).astype(f32)
        blank = jnp.zeros((lanes - 2 * factor_rows, rows), f32)
        lows[g] = jnp.concatenate([top, low - top, blank], axis=0).T.astype(bf16)

    def correction(layer, g, p):
        start = pl.multiple_of(me * width + p * piece, lanes)
        factor = factor_slice(fout_ref, layer, g, start, piece)
        right = jnp.concatenate(
            [factor, factor, jnp.zeros((lanes - 2 * factor_rows, piece), bf16)], axis=0
        )
        return jnp.dot(lows[g], right, preferred_element_type=f32)

    for copy in loads[:2]:
        copy.wait()
    for p in range(1, parts):
        for slot in range(2):
            column_copy(slot, p).start()
    def relay_copy(way, hop, source):
        return remote(
            granks_ref.at[twin, source],
            granks_ref.at[twin, source],
            relay_send.at[way, hop - 1],
            relay_recv.at[way, hop - 1],
            at_line(line + 1) if way == 0 else at_line(line - 1),
            me,
        )

    def relay_each(hop, act, sending):
        shift = hop - 1 if sending else hop
        right = (line >= shift) & (line < outer - 1) if sending else line >= shift
        left = (line + shift < outer) & (line > 0) if sending else line + shift < outer

        @pl.when(right)
        def _():
            act(relay_copy(0, hop, line - shift))

        @pl.when(left)
        def _():
            act(relay_copy(1, hop, line + shift))

    def relay_start(hop):
        relay_each(hop, lambda copy: copy.start(), True)

    def relay_next(hop):
        relay_each(hop, lambda copy: copy.wait_recv(), False)
        if hop + 1 < outer:
            relay_start(hop + 1)

    plane = remote(granks_ref.at[twin], granks_ref.at[twin], plane_send, plane_recv, buddy, me)
    plane_in = remote(
        granks_ref.at[1 - twin], granks_ref.at[1 - twin], plane_send, plane_recv, buddy, me
    )

    def part_copy(slot, p):
        return remote(
            own_part.at[slot, p],
            got_part.at[slot, p],
            part_send,
            part_recv.at[slot, p],
            mine,
            mate,
        )

    def own_rows(q):
        return pl.ds(pl.multiple_of(q * local, local), local)

    def in_copy(way, hop, source):
        return remote(
            fin_ref,
            gin_ref.at[:, own_rows(at_line(source)), :],
            in_send,
            in_recv.at[way, hop - 1],
            at_line(line + hop) if way == 0 else at_line(line - hop),
            me,
        )

    def in_start(hop):
        @pl.when(line + hop < outer)
        def _():
            in_copy(0, hop, line).start()

        @pl.when(line >= hop)
        def _():
            in_copy(1, hop, line).start()

    def in_pass(hop):
        @pl.when(line >= hop)
        def _():
            in_copy(0, hop, line - hop).wait_recv()
            pass_copy(line - hop, twin).start()

        @pl.when(line + hop < outer)
        def _():
            in_copy(1, hop, line + hop).wait_recv()
            pass_copy(line + hop, twin).start()

    def in_buddy(source):
        return remote(
            fin_ref,
            gin_ref.at[:, own_rows(source), :],
            in_send,
            buddy_recv,
            buddy,
            me,
        )

    def pass_copy(place, side_of):
        at = own_rows(place * 2 + side_of)
        return remote(
            gin_ref.at[:, at, :],
            gin_ref.at[:, at, :],
            pass_send,
            pass_recv,
            buddy,
            me,
        )

    def out_copy(hop, source):
        target = lax.rem(mine + hop, pop)
        cols = pl.multiple_of(target * columns, lanes)
        return remote(
            fout_ref.at[core, :, pl.ds(cols, columns)],
            gout_ref.at[core, own_rows(source), :],
            out_send,
            out_recv,
            target,
            me,
        )

    def stretch(ref, count):
        return ref.at[pl.ds(0, count * local), :]

    def whole_out():
        spot = stretch(gout_ref.at[core], pop - 1)
        return remote(spot, spot, out_send, out_recv, buddy, me)

    def whole_pass():
        spot = gin_ref.at[:, pl.ds(0, (outer - 1) * local), :]
        return remote(spot, spot, pass_send, pass_recv, buddy, me)

    def whole_in():
        spot = gin_ref.at[:, pl.ds(0, outer * local), :]
        return remote(spot, spot, in_send, buddy_recv, buddy, me)

    def half_copy(which):
        return remote(
            gout_ref.at[which],
            gout_ref.at[which],
            half_send,
            half_recv,
            mine,
            mate,
        )

    def self_copies():
        cols = pl.multiple_of(mine * columns, lanes)
        return (
            pltpu.make_async_copy(fin_ref, gin_ref.at[:, own_rows(mine), :], self_sem.at[0]),
            pltpu.make_async_copy(
                fout_ref.at[core, :, pl.ds(cols, columns)],
                gout_ref.at[core, own_rows(mine), :],
                self_sem.at[1],
            ),
        )

    spans = (pl.ds(0, share), pl.ds(share, vocab - 2 * share))

    def over_copy(h, p):
        return remote(
            own_over.at[p, spans[h]],
            got_over.at[p, spans[h]],
            over_send,
            over_recv.at[h, p],
            mine,
            cross,
        )

    def hand_copy(p, half):
        at = pl.ds(pl.multiple_of(half * share, share), share)
        return remote(
            table.at[p, at],
            table.at[p, at],
            hand_send,
            hand_recv.at[p],
            buddy,
            me,
        )

    def entry(slot, p):
        return jnp.dot(
            rows_embed[...], weights[slot, :, halves[p]], preferred_element_type=f32
        ).astype(bf16)

    def part_put(p):
        column_copy(0, p).wait()
        own_part[0, p] = entry(0, p)

    def part_make(p):
        column_copy(1, p).wait()
        own_over[p] = entry(1, p)

    def part_sum(p):
        part_copy(0, p).wait_recv()
        own_over[p] = (own_over[p].astype(f32) + got_part[0, p].astype(f32)).astype(bf16)
        over_copy(0, p).start()

    with jax.named_scope("tab0"):
        part_put(0)
    with jax.named_scope("bar"):
        pl.semaphore_wait(
            barrier,
            4 + jnp.where(line < outer - 1, 1, 0) + jnp.where(line > 0, 1, 0),
        )

    relay_start(1)
    with jax.named_scope("tab1"):
        part_copy(0, 0).start()
        for copy in loads[2:5]:
            copy.start()
        for slot in range(2, 4):
            weight_copy(0, slot).start()
        for copy in loads[5:]:
            copy.start()
        part_make(0)
        for p in range(1, parts):
            part_put(p)
            part_copy(0, p).start()
            if p > 1:
                part_make(p - 1)
            part_sum(p - 1)
        part_make(parts - 1)
        part_sum(parts - 1)
        weight_copy(1, 0).start()
        weight_copy(1, 1).start()
    over_copy(1, 0).start()
    def begin(g):
        tokens = jnp.concatenate(
            [ids_ref[g * member_rows + m] for m in range(member_rows)], axis=0
        )
        entries = lax.broadcasted_iota(jnp.int32, (group, vocab), 1)
        for t in range(steps):
            onehot_ref[g, t * group : (t + 1) * group, :] = jnp.where(
                tokens[:, t : t + 1] == entries, 1.0, 0.0
            ).astype(bf16)
        features = jnp.dot(onehot_ref[g], embed_ref[...], preferred_element_type=f32).astype(bf16)
        hidden[g] = features
        low_put(0, g, against(factor_slice(fin_ref, 0, g, 0, width), features))

    def both(h, p):
        at = spans[h]
        return (
            mine_part[p, at].astype(f32) + got_part[1, p, at].astype(f32)
        ) + got_over[p, at].astype(f32)

    def lead_pair(k):
        return remote(
            own_lead.at[k], got_lead.at[k], lead_send, lead_recv.at[k], mine, mate
        )

    def lead_cross(k):
        return remote(own_ahead.at[k], got_ahead.at[k], ahead_send, ahead_recv, mine, cross)

    def lead_dot(k, slot):
        left = lifted[...] if k else hidden[0]
        return jnp.dot(
            left, weights[slot, :, halves[0]], preferred_element_type=f32
        ).astype(bf16)

    def lead_put(k):
        own_lead[k] = lead_dot(k, 0)
        lead_pair(k).start()

    def lead_sum(k):
        value = lead_dot(k, 1).astype(f32)
        lead_pair(k).wait_recv()
        own_ahead[k] = (value + got_lead[k].astype(f32)).astype(bf16)
        lead_cross(k).start()

    def wait_weights(half):
        spot = weights.at[pl.ds(2 * half, 2)]
        pltpu.make_async_copy(spot, spot, weight_sem.at[2 + half]).wait()

    with jax.named_scope("tab2"):
        for copy in loads[2:5]:
            copy.wait()
        unpack(fin_raw, fin_ref)
        weight_copy(0, 2).wait()
        for p in range(parts):
            own_part[1, p] = entry(2, p)
            part_copy(1, p).start()
        weight_copy(1, 2).start()
    with jax.named_scope("relay1"):
        relay_next(1)
        in_start(1)
    weight_copy(0, 3).wait()
    issued = 1
    first = min(max(chunks - 1, 1), parts)
    for p in range(parts):
        with jax.named_scope("tabA%d" % p):
            mine_part[p] = entry(3, p)
            part_copy(1, p).wait_recv()
            over_copy(0, p).wait_recv()
            at = pl.ds(pl.multiple_of(twin * share, share), share)
            table[p, at] = both(0, p).astype(bf16)
            hand_copy(p, twin).start()
        if p < first:
            with jax.named_scope("begin%d" % p):
                begin(p)
                low_copy(0, p, 0).start()
            if issued < parts:
                over_copy(1, issued).start()
                issued += 1
    for p in range(issued, parts):
        over_copy(1, p).start()
    weight_copy(1, 3).start()
    in_buddy(mine).start()
    with jax.named_scope("prep"):
        for copy in loads[5:]:
            copy.wait()
        unpack(fout_raw, fout_ref)
        reward = reward_ref[...]
        high = reward.astype(bf16).astype(f32)
        middle = (reward - high).astype(bf16).astype(f32)
        rest = reward - high - middle
        index = lax.broadcasted_iota(jnp.int32, (16, width), 0)
        heads[...] = jnp.where(
            index == 0,
            high,
            jnp.where(index == 1, middle, jnp.where(index == 2, rest, 0.0)),
        ).astype(bf16)

    wait_weights(0)
    with jax.named_scope("leadx"):
        lead_put(0)
        for g in range(first, chunks):
            begin(g)
            low_copy(0, g, 0).start()
        lead_sum(0)
    with jax.named_scope("folds"):
        for g in range(max(chunks - 1, 1)):
            low_fold(0, g)
    with jax.named_scope("relay2"):
        if outer > 2:
            relay_next(2)
            in_start(2)

    def recur(layer, g, p, inputs):
        decay = decay_ref[layer : layer + 1, halves[p]]
        kept = 1.0 - decay
        carried = jnp.zeros((group, piece), f32)
        if layer:
            lean = gain_ref[layer : layer + 1, halves[p]] * reward_ref[:, halves[p]]
        for t in range(steps):
            at = slice(t * group, (t + 1) * group)
            carried = decay * carried + kept * inputs[at]
            if not layer:
                states[g, at, halves[p]] = carried
            elif t == steps - 1:
                lasts[g, :, halves[p]] = carried
            powers = carried * carried
            total = powers[:, :lanes]
            for c in range(lanes, piece, lanes):
                total = total + powers[:, c : c + lanes]
            if p:
                total = total + squares[g, at, :]
            squares[g, at, :] = total
            if layer:
                leaning = carried * lean
                total = leaning[:, :lanes]
                for c in range(lanes, piece, lanes):
                    total = total + leaning[:, c : c + lanes]
                if p:
                    total = total + leans[g, at, :]
                leans[g, at, :] = total

    def across(value):
        return jnp.sum(value.T, axis=0, keepdims=True)

    def squares_start(g):
        small[2, g, 0] = jnp.broadcast_to(across(squares[g]), (4, rows))
        small_start(2, g)

    def complete(p):
        with jax.named_scope("tabB%d" % p):
            over_copy(1, p).wait_recv()
            table[p, 2 * share :] = both(1, p).astype(bf16)
        with jax.named_scope("hand%d" % p):
            hand_copy(p, 1 - twin).wait_recv()

    def layer_zero(g, p):
        with jax.named_scope("lz%d_%d" % (g, p)):
            inputs = jnp.dot(
                onehot_ref[g], table[p], preferred_element_type=f32
            ) + correction(0, g, p)
            recur(0, g, p, inputs)

    late = parts - 1

    low_ready(0, 0)
    for p in range(late):
        complete(p)
        layer_zero(0, p)
    for g in range(1, chunks - 1):
        low_ready(0, g)
        for p in range(min(2, late)):
            layer_zero(g, p)
    if chunks > 1:
        low_fold(0, chunks - 1)
    complete(late)
    layer_zero(0, late)
    squares_start(0)
    with jax.named_scope("leadv"):
        lifted[...] = (states[0] * gain_ref[0:1, :]).astype(bf16)
        lead_put(1)
    for g in range(1, chunks - 1):
        for p in range(min(2, late), late):
            layer_zero(g, p)
    if chunks > 1:
        low_ready(0, chunks - 1)
        for p in range(late):
            layer_zero(chunks - 1, p)
    with jax.named_scope("leadw"):
        lead_sum(1)
    for g in range(1, chunks):
        layer_zero(g, late)
        squares_start(g)

    def pair_copy(g, slot, p):
        return remote(
            own_pair.at[g, slot, p],
            got_pair.at[g, slot, p],
            pair_send.at[2 if g else slot],
            pair_recv.at[g, 1] if slot else lone_recv.at[p] if g == 0 else pair_recv.at[g, 0],
            mine,
            mate,
        )

    def whole_pair(g, slot):
        return remote(
            own_pair.at[g, slot],
            got_pair.at[g, slot],
            pair_send.at[2 if g else slot],
            pair_recv.at[g, slot],
            mine,
            mate,
        )

    def cross_copy(g, p):
        return remote(
            own_cross.at[g, p],
            got_cross.at[g, p],
            cross_send.at[1 if g else 0],
            cross_recv.at[parts + g if g < chunks - 1 else p],
            mine,
            cross,
        )

    def whole_cross(g):
        at = pl.ds(0 if g else 1, parts if g else late)
        return remote(
            own_cross.at[g, at],
            got_cross.at[g, at],
            cross_send.at[1 if g else 0],
            cross_recv.at[parts + g],
            mine,
            cross,
        )

    def shape_ranks():
        full_block = (2, outer, 8, lanes)
        kept = (lax.broadcasted_iota(jnp.int32, full_block, 2) == 0) & (
            lax.broadcasted_iota(jnp.int32, full_block, 3) < members
        )
        shares = jnp.where(kept, granks_ref[...].astype(f32) / members_all, 0.0)

        def mean_of(value):
            value = jnp.sum(value, axis=0)
            value = jnp.sum(value, axis=0)
            value = jnp.sum(value, axis=0, keepdims=True)
            return jnp.sum(value, axis=1, keepdims=True) / members_all

        rank_mean = mean_of(shares)
        apart = jnp.where(kept, shares - rank_mean[None, None], 0.0)
        spread = mean_of(apart * apart) + spread_eps
        owner = lax.broadcasted_iota(jnp.int32, (local, lanes), 0) // rank
        own = owner == lax.broadcasted_iota(jnp.int32, (local, lanes), 1)
        for place in range(outer):
            for side_of in range(2):
                share_row = granks_ref[side_of, place, 0:1].astype(f32) / members_all
                shaped = (share_row - rank_mean) * lax.rsqrt(spread)
                shaped = jnp.where(own, jnp.broadcast_to(shaped, (local, lanes)), 0.0)
                shaped = jnp.sum(shaped, axis=1, keepdims=True)
                at = (place * 2 + side_of) * local
                shaped_ref[at : at + local] = jnp.broadcast_to(shaped, (local, lanes))

    def out_start():
        with jax.named_scope("outs"):
            plane_in.wait_recv()
            for hop in range(1, pop):
                out_copy(hop, mine).start()
            for copy in self_copies():
                copy.start()

    def gather_half():
        with jax.named_scope("half"):
            whole_out().wait_recv()
            for copy in self_copies():
                copy.wait()
            half_copy(core).start()

    def step_make():
        tile = 256
        with jax.named_scope("arrive"):
            in_buddy(buddy).wait_recv()
        with jax.named_scope("arrive_pass"):
            whole_pass().wait_recv()
        with jax.named_scope("arrive_half"):
            half_copy(1 - core).wait_recv()
        with jax.named_scope("step"):
            shape_ranks()
            shaped = jnp.concatenate([shaped_ref[...]] * (tile // lanes), axis=1)
            for layer in range(layers):
                for at in range(0, width, tile):
                    factor = gin_ref[layer, :, at : at + tile].astype(f32)
                    value = lax.dot_general(
                        (factor * shaped).astype(bf16),
                        gout_ref[layer],
                        (((0,), (0,)), ((), ())),
                        preferred_element_type=f32,
                    )
                    step_ref[layer, at : at + tile] = value * (members_all * rank) ** (-0.5)

    def between(g):
        if g == 0:
            wait_weights(1)
        with jax.named_scope("normed%d" % g):
            total = small_sum(2, g)[:1]
            scale = lax.rsqrt(total / full + norm_eps)
            scale = jnp.broadcast_to(scale, (lanes, rows)).T
            if g == 0:
                lead_scale[...] = scale
            scale = jnp.concatenate([scale] * (width // lanes), axis=1)
            gain = gain_ref[0:1, :]
            hidden[g] = (hidden[g].astype(f32) + states[g] * scale * gain).astype(bf16)

        def product(slot, p):
            return jnp.dot(
                hidden[g], weights[slot, :, halves[p]], preferred_element_type=f32
            ).astype(bf16)

        with jax.named_scope("exch%d" % g):
            def summed(p):
                value = product(1, p).astype(f32)
                if g == 0:
                    pair_copy(g, 0, p).wait_recv()
                elif p == 0:
                    whole_pair(g, 0).wait_recv()
                total = (value + got_pair[g, 0, p].astype(f32)).astype(bf16)
                own_cross[g, p] = total
                cross_copy(g, p).start()

            for p in range(0 if g else 1, parts):
                own_pair[g, 0, p] = product(0, p)
                pair_copy(g, 0, p).start()
                if p > 1 and g == 0:
                    summed(p - 1)
            left = jnp.concatenate([factor_slice(fin_ref, 1, g, 0, width), heads[...]], axis=0)
            local_low = against(left, hidden[g])
            low_put(1, g, local_low[:factor_rows])
            low_copy(1, g, 0).start()
            aligned = local_low[factor_rows : factor_rows + 8]
            alphas[g] = jnp.broadcast_to(jnp.sum(aligned, axis=0, keepdims=True), (8, rows))
            for p in range(0 if g else parts - 1, parts):
                summed(p)
            for p in range(parts):
                own_pair[g, 1, p] = product(2, p)
                pair_copy(g, 1, p).start()
            for p in range(parts):
                states[g, :, halves[p]] = product(3, p).astype(f32)

    def layer_one(g):
        with jax.named_scope("lowone%d" % g):
            low_ready(1, g)
        for p in range(parts):
            with jax.named_scope("l1_%d_%d" % (g, p)):
                if p == 0:
                    whole_pair(g, 1).wait_recv()
                fixed = (
                    states[g, :, halves[p]] + got_pair[g, 1, p].astype(f32)
                ) + correction(1, g, p)
                if g == 0 and p == 0:
                    remote(own_ahead, got_ahead, ahead_send, ahead_recv, mine, cross).wait_recv()
                    scale = jnp.concatenate([lead_scale[...]] * (piece // lanes), axis=1)
                    other = got_ahead[0].astype(f32) + scale * got_ahead[1].astype(f32)
                else:
                    if g == chunks - 1:
                        cross_copy(g, p).wait_recv()
                    elif p == (0 if g else 1):
                        whole_cross(g).wait_recv()
                    other = got_cross[g, p].astype(f32)
                recur(1, g, p, fixed + other)
        with jax.named_scope("end%d" % g):
            small[3, g, 0] = jnp.concatenate(
                [across(squares[g]), across(leans[g]), alphas[g][:2]], axis=0
            )
            small_start(3, g)

    with jax.named_scope("relay3"):
        for hop in range(3, outer):
            relay_next(hop)
            in_start(hop)
        plane.start()
    with jax.named_scope("pass1"):
        in_pass(1)
    for g in range(chunks):
        between(g)
        if g == 0:
            out_start()
        with jax.named_scope("pass"):
            for hop in range(g + 1, min(g + 2, outer) if g else 0):
                in_pass(hop)
    for g in range(chunks):
        if g < chunks - 1:
            low_fold(1, g)
        else:
            with jax.named_scope("pass"):
                for hop in range(chunks + 1, outer):
                    in_pass(hop)
            gather_half()
            if g:
                layer_one(g - 1)
            low_fold(1, g)
            step_make()
            layer_one(g)
        if g < chunks - 2:
            layer_one(g)

    lane = lax.broadcasted_iota(jnp.int32, (seqs, lanes), 1)
    scores = jnp.zeros((seqs, lanes), f32)
    with jax.named_scope("final"):
        for g in range(chunks):
            sums = small_sum(3, g)
            scale = lax.rsqrt(sums[0:1] / full + norm_eps)
            value = sums[2:3] + scale * sums[1:2]
            total = value[:, :lanes]
            for c in range(lanes, rows, lanes):
                total = total + value[:, c : c + lanes]
            total = jnp.broadcast_to(total, (8, lanes))
            shift = lanes // 2
            while shift >= group:
                total = total + pltpu.roll(total, shift, 1)
                shift //= 2
            total = total * (full ** (-0.5) / steps)
            total = jnp.broadcast_to(total[:1], (lanes, lanes)).T
            for m in range(member_rows):
                scores = jnp.where(
                    lane == g * member_rows + m, total[m * seqs : (m + 1) * seqs], scores
                )
            ending = jnp.broadcast_to(scale[:, rows - lanes :], (lanes, lanes)).T[lanes - group :]
            ending = jnp.concatenate([ending] * (width // lanes), axis=1)
            gain = gain_ref[1:2, :]
            ending = (
                hidden[g, rows - group :].astype(f32) + lasts[g] * ending * gain
            ).astype(bf16).astype(f32)
            for m in range(member_rows):
                final_ref[g * member_rows + m] = ending[m * seqs : (m + 1) * seqs].astype(bf16)
        score_ref[...] = scores[:, :members]

    with jax.named_scope("drain"):
        for hop in range(1, outer):
            relay_each(hop, lambda copy: copy.wait_send(), True)
        plane.wait_send()
        remote(own_part, got_part, part_send, part_recv.at[0, 0], mine, mate).wait_send()
        remote(own_over, got_over, over_send, over_recv.at[0, 0], mine, cross).wait_send()
        spot = table.at[:, pl.ds(0, share)]
        remote(spot, spot, hand_send, hand_recv.at[0], buddy, me).wait_send()
        spot = own_pair.at[0, 0, pl.ds(1, late)]
        remote(spot, spot, pair_send.at[0], pair_recv.at[0, 0], mine, mate).wait_send()
        spot = own_pair.at[0, 1]
        remote(spot, spot, pair_send.at[1], pair_recv.at[0, 0], mine, mate).wait_send()
        spot = own_cross.at[0, pl.ds(1, late)]
        remote(spot, spot, cross_send.at[0], cross_recv.at[0], mine, cross).wait_send()
        if chunks > 1:
            spot = own_pair.at[pl.ds(1, chunks - 1)]
            remote(spot, spot, pair_send.at[2], pair_recv.at[0, 0], mine, mate).wait_send()
        if chunks > 1:
            spot = own_cross.at[pl.ds(1, chunks - 1)]
            remote(spot, spot, cross_send.at[1], cross_recv.at[0], mine, cross).wait_send()
        remote(own_lead, got_lead, lead_send, lead_recv.at[0], mine, mate).wait_send()
        remote(own_ahead, got_ahead, ahead_send, ahead_recv, mine, cross).wait_send()
        spot = small.at[pl.ds(0, 2), :, pl.ds(0, 2)]
        remote(spot, spot, low_send, low_recv.at[0, 0, 0], mine, mate).wait_send()
        spot = small.at[pl.ds(2, 2), :, pl.ds(1, 3)]
        remote(spot, spot, small_send, small_recv.at[0, 0], mine, mate).wait_send()
        whole_in().wait_send()
        whole_pass().wait_send()
        whole_out().wait_send()
        half_copy(core).wait_send()


cuts = 2


def publish(final_ref, score_ref, step_ref, final_out, score_out, step_out, sems):
    copies = []
    layers, width, _ = step_ref.shape
    cut = width // cuts
    for layer in range(layers):
        for c in range(cuts):
            at = pl.ds(c * cut, cut)
            copies.append(
                pltpu.make_async_copy(
                    step_ref.at[layer, at], step_out.at[layer, at], sems.at[layer, c]
                )
            )
    copies.append(pltpu.make_async_copy(final_ref, final_out, sems.at[layers, 0]))
    copies.append(pltpu.make_async_copy(score_ref, score_out, sems.at[layers, 1]))
    for copy in copies:
        copy.start()
    for copy in copies:
        copy.wait()


def shards(
    token_ids,
    fitness_ranks,
    embedding,
    mix_weights,
    factors_in,
    factors_out,
    decay_rates,
    norm_gain,
    reward_dir,
):
    members, seqs, steps = token_ids.shape
    vocab, width = embedding.shape
    layers, _, full = mix_weights.shape
    rank = factors_in.shape[2]
    pop = lax.axis_size("pop")
    outer = pop // 2
    coef = noise_scale * (full * rank) ** (-0.5)
    columns = full // pop
    member_rows = 16 // seqs
    chunks = members // member_rows
    group = member_rows * seqs
    rows = group * steps
    local = members * rank
    share = vocab * 5 // 16
    dims = (pop, chunks, group, steps, member_rows, seqs, rank, width, full, coef, share)
    vmem = pl.BlockSpec(memory_space=pltpu.VMEM)
    smem = pl.BlockSpec(memory_space=pltpu.SMEM)
    hbm = pl.BlockSpec(memory_space=pltpu.HBM)
    parts = 4
    piece = width // parts
    entries = vocab - share
    dma = pltpu.SemaphoreType.DMA
    final_features, scores, step = pl.pallas_call(
        functools.partial(policy_kernel, dims),
        out_shape=(
            pltpu.VMEM((members, seqs, width), bf16),
            pltpu.VMEM((seqs, members), f32),
            pltpu.VMEM((layers, width, columns), f32),
        ),
        in_specs=[hbm, hbm, hbm, hbm, hbm, smem, hbm, hbm, hbm],
        out_specs=(vmem, vmem, vmem),
        scratch_shapes=[
            pltpu.VMEM((members, seqs, steps), jnp.int32),
            pltpu.VMEM((vocab, width), bf16),
            pltpu.VMEM((layers, members, rank, width), bf16),
            pltpu.VMEM((layers, members, rank, full), bf16),
            pltpu.VMEM((layers, width), f32),
            pltpu.VMEM((layers, width), f32),
            pltpu.VMEM((1, width), f32),
            pltpu.VMEM((4, width, width), bf16),
            pltpu.VMEM((entries, width), bf16),
            pltpu.VMEM((2, parts, entries, piece), bf16),
            pltpu.VMEM((2, parts, entries, piece), bf16),
            pltpu.VMEM((parts, entries, piece), bf16),
            pltpu.VMEM((parts, entries, piece), bf16),
            pltpu.VMEM((parts, entries, piece), bf16),
            pltpu.VMEM((parts, vocab, piece), bf16),
            pltpu.VMEM((chunks, 2, parts, rows, piece), bf16),
            pltpu.VMEM((chunks, 2, parts, rows, piece), bf16),
            pltpu.VMEM((chunks, parts, rows, piece), bf16),
            pltpu.VMEM((chunks, parts, rows, piece), bf16),
            pltpu.VMEM((2, rows, piece), bf16),
            pltpu.VMEM((2, rows, piece), bf16),
            pltpu.VMEM((2, rows, piece), bf16),
            pltpu.VMEM((2, rows, piece), bf16),
            pltpu.VMEM((rows, width), bf16),
            pltpu.VMEM((rows, lanes), f32),
            pltpu.VMEM((chunks, rows, width), f32),
            pltpu.VMEM((chunks, rows, width), bf16),
            pltpu.VMEM((chunks, rows, vocab), bf16),
            pltpu.VMEM((layers, local, width), bf16),
            pltpu.VMEM((layers, local, full), bf16),
            pltpu.VMEM((pop * local, lanes), f32),
            pltpu.VMEM((layers, pop * local, width), bf16),
            pltpu.VMEM((layers, pop * local, columns), bf16),
            pltpu.VMEM((2, outer, 8, lanes), jnp.int32),
            pltpu.VMEM((chunks, rows, lanes), bf16),
            pltpu.VMEM((chunks, rows, lanes), f32),
            pltpu.VMEM((chunks, rows, lanes), f32),
            pltpu.VMEM((chunks, group, width), f32),
            pltpu.VMEM((16, width), bf16),
            pltpu.VMEM((chunks, 8, rows), f32),
            pltpu.VMEM((4, chunks, 4, 4, rows), f32),
            dma((4,)),
            dma((2, parts)),
            dma((9,)),
            dma,
            dma((2, parts)),
            dma,
            dma((2, parts)),
            dma,
            dma((parts,)),
            dma((3,)),
            dma((chunks, 2)),
            dma((parts,)),
            dma((2,)),
            dma((parts + chunks - 1,)),
            dma,
            dma((2,)),
            dma,
            dma,
            dma,
            dma((2, chunks)),
            dma,
            dma((2, 2, chunks)),
            dma((2, outer - 1)),
            dma((2, outer - 1)),
            dma,
            dma,
            dma,
            dma((2, outer - 1)),
            dma,
            dma,
            dma,
            dma,
            dma,
            dma,
            dma,
            dma((2,)),
        ],
        compiler_params=pltpu.CompilerParams(
            collective_id=0, has_side_effects=True, vmem_limit_bytes=52 * 1024 * 1024
        ),
    )(
        *(
            pltpu.with_memory_space_constraint(value, pltpu.HBM)
            for value in (
                token_ids,
                embedding,
                mix_weights,
                factors_in,
                factors_out,
                fitness_ranks,
                decay_rates,
                norm_gain,
                reward_dir.reshape(1, width),
            )
        )
    )
    final_features, scores, weight_step = pl.pallas_call(
        publish,
        out_shape=(
            jax.ShapeDtypeStruct((members, seqs, width), bf16),
            jax.ShapeDtypeStruct((seqs, members), f32),
            jax.ShapeDtypeStruct((layers, width, columns), f32),
        ),
        in_specs=[vmem, vmem, vmem],
        out_specs=(hbm, hbm, hbm),
        scratch_shapes=[dma((layers + 1, cuts))],
        compiler_params=pltpu.CompilerParams(vmem_limit_bytes=1024 * 1024),
    )(final_features, scores, step)
    return (final_features, scores.T, weight_step)


def solution(mesh):
    return jax.shard_map(
        shards,
        mesh=mesh,
        in_specs=(
            P("pop", None, None),
            P("pop"),
            P(None, "mp"),
            P(None, "mp", None),
            P(None, "pop", None, "mp"),
            P(None, "pop", None, None),
            P(None, "mp"),
            P(None, "mp"),
            P("mp"),
        ),
        out_specs=(P("pop", None, "mp"), P("pop", None), P(None, "mp", "pop")),
        check_vma=False,
    )
```

```python
import functools

import jax
import jax.numpy as jnp
from jax import lax
from jax.experimental import pallas as pl
from jax.experimental.pallas import tpu as pltpu
from jax.sharding import PartitionSpec as P

noise_scale = 0.25
norm_eps = 1e-06
spread_eps = 1e-05
lanes = 128
f32, bf16 = jnp.float32, jnp.bfloat16


def policy_kernel(
    dims,
    ids_hbm,
    embed_hbm,
    mix_ref,
    fin_hbm,
    fout_hbm,
    ranks_smem,
    decay_hbm,
    gain_hbm,
    reward_hbm,
    final_ref,
    score_ref,
    step_ref,
    ids_ref,
    embed_ref,
    fin_raw,
    fout_raw,
    decay_ref,
    gain_ref,
    reward_ref,
    weights,
    rows_embed,
    own_part,
    got_part,
    own_over,
    got_over,
    mine_part,
    table,
    own_pair,
    got_pair,
    own_cross,
    got_cross,
    own_lead,
    got_lead,
    own_ahead,
    got_ahead,
    lifted,
    lead_scale,
    states,
    hidden,
    onehot_ref,
    fin_ref,
    fout_ref,
    shaped_ref,
    gin_ref,
    gout_ref,
    granks_ref,
    lows,
    squares,
    leans,
    lasts,
    heads,
    alphas,
    small,
    weight_sem,
    column_sem,
    load_sem,
    part_send,
    part_recv,
    over_send,
    over_recv,
    hand_send,
    hand_recv,
    pair_send,
    pair_recv,
    lone_recv,
    cross_send,
    cross_recv,
    lead_send,
    lead_recv,
    ahead_send,
    ahead_recv,
    small_send,
    small_recv,
    low_send,
    low_recv,
    relay_send,
    relay_recv,
    plane_send,
    plane_recv,
    in_send,
    in_recv,
    buddy_recv,
    pass_send,
    pass_recv,
    out_send,
    out_recv,
    half_send,
    half_recv,
    self_sem,
):
    pop, chunks, group, steps, member_rows, seqs, rank, width, full, coef, share = dims
    parts = hand_recv.shape[0]
    piece = width // parts
    halves = [slice(p * piece, (p + 1) * piece) for p in range(parts)]
    rows = group * steps
    vocab = embed_ref.shape[0]
    members = ids_ref.shape[0]
    members_all = members * pop
    layers, local = fin_ref.shape[0], fin_ref.shape[1]
    columns = gout_ref.shape[2]
    mine = lax.axis_index("pop")
    me = lax.axis_index("mp")
    side, core = me // 2, me % 2
    mate = side * 2 + (1 - core)
    cross = (1 - side) * 2 + core
    diagonal = (1 - side) * 2 + (1 - core)
    others = (mate, cross, diagonal)
    blocks = (diagonal, cross, mate, me)
    outer = pop // 2
    line, twin = mine // 2, mine % 2
    buddy = line * 2 + (1 - twin)

    def at_line(place):
        return place * 2 + twin

    def peer(q, j):
        return {"pop": q, "mp": j}

    def remote(src, dst, send, recv, q, j):
        return pltpu.make_async_remote_copy(
            src_ref=src,
            dst_ref=dst,
            send_sem=send,
            recv_sem=recv,
            device_id=peer(q, j),
            device_id_type=pl.DeviceIdType.MESH,
        )

    barrier = pltpu.get_barrier_semaphore()

    def greet(q, j):
        pl.semaphore_signal(
            barrier, inc=1, device_id=peer(q, j), device_id_type=pl.DeviceIdType.MESH
        )

    for other in others:
        greet(mine, other)
    greet(buddy, me)

    @pl.when(line < outer - 1)
    def _():
        greet(at_line(line + 1), me)

    @pl.when(line > 0)
    def _():
        greet(at_line(line - 1), me)

    def weight_copy(layer, slot):
        start = pl.multiple_of(blocks[slot] * width, lanes)
        return pltpu.make_async_copy(
            mix_ref.at[layer, :, pl.ds(start, width)],
            weights.at[slot],
            weight_sem.at[2 + slot // 2 if layer else slot - 2],
        )

    def column_copy(slot, p):
        start = pl.multiple_of(blocks[slot] * width + p * piece, lanes)
        return pltpu.make_async_copy(
            mix_ref.at[0, :, pl.ds(start, piece)],
            weights.at[slot, :, halves[p]],
            column_sem.at[slot, p],
        )

    loads = [
        pltpu.make_async_copy(src, dst, load_sem.at[i])
        for i, (src, dst) in enumerate(
            (
                (
                    embed_hbm.at[pl.ds(pl.multiple_of(twin * share, share), share)],
                    rows_embed.at[pl.ds(0, share)],
                ),
                (
                    embed_hbm.at[pl.ds(2 * share, embed_ref.shape[0] - 2 * share)],
                    rows_embed.at[pl.ds(share, embed_ref.shape[0] - 2 * share)],
                ),
                (embed_hbm, embed_ref),
                (ids_hbm, ids_ref),
                (fin_hbm, fin_raw),
                (decay_hbm, decay_ref),
                (gain_hbm, gain_ref),
                (reward_hbm, reward_ref),
                (fout_hbm, fout_raw),
            )
        )
    ]
    for copy in loads[:2]:
        copy.start()
    for slot in range(2):
        column_copy(slot, 0).start()

    def rank_block(shape, axis, repeats):
        index = lax.broadcasted_iota(jnp.int32, shape, axis)
        block = jnp.zeros(shape, jnp.int32)
        for m in range(members):
            block = jnp.where(index // repeats == m, ranks_smem[m], block)
        return block

    granks_ref[twin, line] = rank_block((8, lanes), 1, 1)

    def unpack(raw, ref):
        def one(g, carry):
            at = pl.ds(
                pl.multiple_of(g * member_rows * rank, member_rows * rank), member_rows * rank
            )
            for layer in range(layers):
                ref[layer, at, :] = jnp.concatenate(
                    [raw[layer, g * member_rows + m].astype(f32) for m in range(member_rows)],
                    axis=0,
                ).astype(bf16)
            return carry

        lax.fori_loop(0, chunks, one, 0)

    factor_rows = member_rows * rank
    mask = (lax.broadcasted_iota(jnp.int32, (factor_rows, rows), 0) // rank) == (
        (lax.broadcasted_iota(jnp.int32, (factor_rows, rows), 1) % group) // seqs
    )

    def factor_slice(ref, layer, g, start, size):
        at = pl.multiple_of(g * factor_rows, factor_rows)
        return ref[layer, pl.ds(at, factor_rows), pl.ds(start, size)]

    def small_copy(kind, g, r):
        return remote(
            small.at[kind, g, 0],
            small.at[kind, g, r + 1],
            small_send,
            small_recv.at[kind - 2, g],
            mine,
            others[r],
        )

    def small_start(kind, g):
        for r in range(3):
            small_copy(kind, g, r).start()

    def small_sum(kind, g):
        arrived = small.at[kind, g, pl.ds(1, 3)]
        remote(arrived, arrived, small_send, small_recv.at[kind - 2, g], mine, mate).wait_recv()
        return (small[kind, g, 0] + small[kind, g, 1]) + (small[kind, g, 2] + small[kind, g, 3])

    def low_copy(layer, g, stage):
        return remote(
            small.at[layer, g, 2 * stage],
            small.at[layer, g, 2 * stage + 1],
            low_send,
            low_recv.at[layer, stage, g],
            mine,
            mate if stage else cross,
        )

    def low_fold(layer, g):
        low_copy(layer, g, 0).wait_recv()
        small[layer, g, 2] = small[layer, g, 0] + small[layer, g, 1]
        low_copy(layer, g, 1).start()

    def against(left, features):
        return lax.dot_general(
            left, features, (((1,), (1,)), ((), ())), preferred_element_type=f32
        )

    def low_put(layer, g, local_low):
        local_low = jnp.where(mask, local_low, 0.0)
        packed = local_low[:rank]
        for at in range(rank, factor_rows, rank):
            packed = packed + local_low[at : at + rank]
        small[layer, g, 0] = packed

    def low_ready(layer, g):
        low_copy(layer, g, 1).wait_recv()
        packed = small[layer, g, 2] + small[layer, g, 3]
        low = jnp.concatenate([packed] * member_rows, axis=0)
        low = jnp.where(mask, low, 0.0) * coef
        top = low.astype(bf16).astype(f32)
        blank = jnp.zeros((lanes - 2 * factor_rows, rows), f32)
        lows[g] = jnp.concatenate([top, low - top, blank], axis=0).T.astype(bf16)

    def correction(layer, g, p):
        start = pl.multiple_of(me * width + p * piece, lanes)
        factor = factor_slice(fout_ref, layer, g, start, piece)
        right = jnp.concatenate(
            [factor, factor, jnp.zeros((lanes - 2 * factor_rows, piece), bf16)], axis=0
        )
        return jnp.dot(lows[g], right, preferred_element_type=f32)

    for copy in loads[:2]:
        copy.wait()
    for p in range(1, parts):
        for slot in range(2):
            column_copy(slot, p).start()
    def relay_copy(way, hop, source):
        return remote(
            granks_ref.at[twin, source],
            granks_ref.at[twin, source],
            relay_send.at[way, hop - 1],
            relay_recv.at[way, hop - 1],
            at_line(line + 1) if way == 0 else at_line(line - 1),
            me,
        )

    def relay_each(hop, act, sending):
        shift = hop - 1 if sending else hop
        right = (line >= shift) & (line < outer - 1) if sending else line >= shift
        left = (line + shift < outer) & (line > 0) if sending else line + shift < outer

        @pl.when(right)
        def _():
            act(relay_copy(0, hop, line - shift))

        @pl.when(left)
        def _():
            act(relay_copy(1, hop, line + shift))

    def relay_start(hop):
        relay_each(hop, lambda copy: copy.start(), True)

    def relay_next(hop):
        relay_each(hop, lambda copy: copy.wait_recv(), False)
        if hop + 1 < outer:
            relay_start(hop + 1)

    plane = remote(granks_ref.at[twin], granks_ref.at[twin], plane_send, plane_recv, buddy, me)
    plane_in = remote(
        granks_ref.at[1 - twin], granks_ref.at[1 - twin], plane_send, plane_recv, buddy, me
    )

    def part_copy(slot, p):
        return remote(
            own_part.at[slot, p],
            got_part.at[slot, p],
            part_send,
            part_recv.at[slot, p],
            mine,
            mate,
        )

    def own_rows(q):
        return pl.ds(pl.multiple_of(q * local, local), local)

    def in_copy(way, hop, source):
        return remote(
            fin_ref,
            gin_ref.at[:, own_rows(at_line(source)), :],
            in_send,
            in_recv.at[way, hop - 1],
            at_line(line + hop) if way == 0 else at_line(line - hop),
            me,
        )

    def in_start(hop):
        @pl.when(line + hop < outer)
        def _():
            in_copy(0, hop, line).start()

        @pl.when(line >= hop)
        def _():
            in_copy(1, hop, line).start()

    def in_pass(hop):
        @pl.when(line >= hop)
        def _():
            in_copy(0, hop, line - hop).wait_recv()
            pass_copy(line - hop, twin).start()

        @pl.when(line + hop < outer)
        def _():
            in_copy(1, hop, line + hop).wait_recv()
            pass_copy(line + hop, twin).start()

    def in_buddy(source):
        return remote(
            fin_ref,
            gin_ref.at[:, own_rows(source), :],
            in_send,
            buddy_recv,
            buddy,
            me,
        )

    def pass_copy(place, side_of):
        at = own_rows(place * 2 + side_of)
        return remote(
            gin_ref.at[:, at, :],
            gin_ref.at[:, at, :],
            pass_send,
            pass_recv,
            buddy,
            me,
        )

    def out_copy(hop, source):
        target = lax.rem(mine + hop, pop)
        cols = pl.multiple_of(target * columns, lanes)
        return remote(
            fout_ref.at[core, :, pl.ds(cols, columns)],
            gout_ref.at[core, own_rows(source), :],
            out_send,
            out_recv,
            target,
            me,
        )

    def stretch(ref, count):
        return ref.at[pl.ds(0, count * local), :]

    def whole_out():
        spot = stretch(gout_ref.at[core], pop - 1)
        return remote(spot, spot, out_send, out_recv, buddy, me)

    def whole_pass():
        spot = gin_ref.at[:, pl.ds(0, (outer - 1) * local), :]
        return remote(spot, spot, pass_send, pass_recv, buddy, me)

    def whole_in():
        spot = gin_ref.at[:, pl.ds(0, outer * local), :]
        return remote(spot, spot, in_send, buddy_recv, buddy, me)

    def half_copy(which):
        return remote(
            gout_ref.at[which],
            gout_ref.at[which],
            half_send,
            half_recv,
            mine,
            mate,
        )

    def self_copies():
        cols = pl.multiple_of(mine * columns, lanes)
        return (
            pltpu.make_async_copy(fin_ref, gin_ref.at[:, own_rows(mine), :], self_sem.at[0]),
            pltpu.make_async_copy(
                fout_ref.at[core, :, pl.ds(cols, columns)],
                gout_ref.at[core, own_rows(mine), :],
                self_sem.at[1],
            ),
        )

    spans = (pl.ds(0, share), pl.ds(share, vocab - 2 * share))

    def over_copy(h, p):
        return remote(
            own_over.at[p, spans[h]],
            got_over.at[p, spans[h]],
            over_send,
            over_recv.at[h, p],
            mine,
            cross,
        )

    def hand_copy(p, half):
        at = pl.ds(pl.multiple_of(half * share, share), share)
        return remote(
            table.at[p, at],
            table.at[p, at],
            hand_send,
            hand_recv.at[p],
            buddy,
            me,
        )

    def entry(slot, p):
        return jnp.dot(
            rows_embed[...], weights[slot, :, halves[p]], preferred_element_type=f32
        ).astype(bf16)

    def part_put(p):
        column_copy(0, p).wait()
        own_part[0, p] = entry(0, p)

    def part_make(p):
        column_copy(1, p).wait()
        own_over[p] = entry(1, p)

    def part_sum(p):
        part_copy(0, p).wait_recv()
        own_over[p] = (own_over[p].astype(f32) + got_part[0, p].astype(f32)).astype(bf16)
        over_copy(0, p).start()

    with jax.named_scope("tab0"):
        part_put(0)
    with jax.named_scope("bar"):
        pl.semaphore_wait(
            barrier,
            4 + jnp.where(line < outer - 1, 1, 0) + jnp.where(line > 0, 1, 0),
        )

    relay_start(1)
    with jax.named_scope("tab1"):
        part_copy(0, 0).start()
        for copy in loads[2:5]:
            copy.start()
        for slot in range(2, 4):
            weight_copy(0, slot).start()
        for copy in loads[5:]:
            copy.start()
        part_make(0)
        for p in range(1, parts):
            part_put(p)
            part_copy(0, p).start()
            if p > 1:
                part_make(p - 1)
            part_sum(p - 1)
        part_make(parts - 1)
        part_sum(parts - 1)
        weight_copy(1, 0).start()
        weight_copy(1, 1).start()
    over_copy(1, 0).start()
    def begin(g):
        tokens = jnp.concatenate(
            [ids_ref[g * member_rows + m] for m in range(member_rows)], axis=0
        )
        entries = lax.broadcasted_iota(jnp.int32, (group, vocab), 1)
        for t in range(steps):
            onehot_ref[g, t * group : (t + 1) * group, :] = jnp.where(
                tokens[:, t : t + 1] == entries, 1.0, 0.0
            ).astype(bf16)
        features = jnp.dot(onehot_ref[g], embed_ref[...], preferred_element_type=f32).astype(bf16)
        hidden[g] = features
        low_put(0, g, against(factor_slice(fin_ref, 0, g, 0, width), features))

    def both(h, p):
        at = spans[h]
        return (
            mine_part[p, at].astype(f32) + got_part[1, p, at].astype(f32)
        ) + got_over[p, at].astype(f32)

    def lead_pair(k):
        return remote(
            own_lead.at[k], got_lead.at[k], lead_send, lead_recv.at[k], mine, mate
        )

    def lead_cross(k):
        return remote(own_ahead.at[k], got_ahead.at[k], ahead_send, ahead_recv, mine, cross)

    def lead_dot(k, slot):
        left = lifted[...] if k else hidden[0]
        return jnp.dot(
            left, weights[slot, :, halves[0]], preferred_element_type=f32
        ).astype(bf16)

    def lead_put(k):
        own_lead[k] = lead_dot(k, 0)
        lead_pair(k).start()

    def lead_sum(k):
        value = lead_dot(k, 1).astype(f32)
        lead_pair(k).wait_recv()
        own_ahead[k] = (value + got_lead[k].astype(f32)).astype(bf16)
        lead_cross(k).start()

    def wait_weights(half):
        spot = weights.at[pl.ds(2 * half, 2)]
        pltpu.make_async_copy(spot, spot, weight_sem.at[2 + half]).wait()

    with jax.named_scope("tab2"):
        for copy in loads[2:5]:
            copy.wait()
        unpack(fin_raw, fin_ref)
        weight_copy(0, 2).wait()
        for p in range(parts):
            own_part[1, p] = entry(2, p)
            part_copy(1, p).start()
        weight_copy(1, 2).start()
    with jax.named_scope("relay1"):
        relay_next(1)
        in_start(1)
    weight_copy(0, 3).wait()
    issued = 1
    first = min(max(chunks - 1, 1), parts)
    for p in range(parts):
        with jax.named_scope("tabA%d" % p):
            mine_part[p] = entry(3, p)
            part_copy(1, p).wait_recv()
            over_copy(0, p).wait_recv()
            at = pl.ds(pl.multiple_of(twin * share, share), share)
            table[p, at] = both(0, p).astype(bf16)
            hand_copy(p, twin).start()
        if p < first:
            with jax.named_scope("begin%d" % p):
                begin(p)
                low_copy(0, p, 0).start()
            if issued < parts:
                over_copy(1, issued).start()
                issued += 1
    for p in range(issued, parts):
        over_copy(1, p).start()
    weight_copy(1, 3).start()
    in_buddy(mine).start()
    with jax.named_scope("prep"):
        for copy in loads[5:]:
            copy.wait()
        unpack(fout_raw, fout_ref)
        reward = reward_ref[...]
        high = reward.astype(bf16).astype(f32)
        middle = (reward - high).astype(bf16).astype(f32)
        rest = reward - high - middle
        index = lax.broadcasted_iota(jnp.int32, (16, width), 0)
        heads[...] = jnp.where(
            index == 0,
            high,
            jnp.where(index == 1, middle, jnp.where(index == 2, rest, 0.0)),
        ).astype(bf16)

    wait_weights(0)
    with jax.named_scope("leadx"):
        lead_put(0)
        for g in range(first, chunks):
            begin(g)
            low_copy(0, g, 0).start()
        lead_sum(0)
    with jax.named_scope("folds"):
        for g in range(max(chunks - 1, 1)):
            low_fold(0, g)
    with jax.named_scope("relay2"):
        if outer > 2:
            relay_next(2)
            in_start(2)

    def recur(layer, g, p, inputs):
        decay = decay_ref[layer : layer + 1, halves[p]]
        kept = 1.0 - decay
        carried = jnp.zeros((group, piece), f32)
        if layer:
            lean = gain_ref[layer : layer + 1, halves[p]] * reward_ref[:, halves[p]]
        for t in range(steps):
            at = slice(t * group, (t + 1) * group)
            carried = decay * carried + kept * inputs[at]
            if not layer:
                states[g, at, halves[p]] = carried
            elif t == steps - 1:
                lasts[g, :, halves[p]] = carried
            powers = carried * carried
            total = powers[:, :lanes]
            for c in range(lanes, piece, lanes):
                total = total + powers[:, c : c + lanes]
            if p:
                total = total + squares[g, at, :]
            squares[g, at, :] = total
            if layer:
                leaning = carried * lean
                total = leaning[:, :lanes]
                for c in range(lanes, piece, lanes):
                    total = total + leaning[:, c : c + lanes]
                if p:
                    total = total + leans[g, at, :]
                leans[g, at, :] = total

    def across(value):
        return jnp.sum(value.T, axis=0, keepdims=True)

    def squares_start(g):
        small[2, g, 0] = jnp.broadcast_to(across(squares[g]), (4, rows))
        small_start(2, g)

    def complete(p):
        with jax.named_scope("tabB%d" % p):
            over_copy(1, p).wait_recv()
            table[p, 2 * share :] = both(1, p).astype(bf16)
        with jax.named_scope("hand%d" % p):
            hand_copy(p, 1 - twin).wait_recv()

    def layer_zero(g, p):
        with jax.named_scope("lz%d_%d" % (g, p)):
            inputs = jnp.dot(
                onehot_ref[g], table[p], preferred_element_type=f32
            ) + correction(0, g, p)
            recur(0, g, p, inputs)

    late = parts - 1

    low_ready(0, 0)
    for p in range(late):
        complete(p)
        layer_zero(0, p)
    for g in range(1, chunks - 1):
        low_ready(0, g)
        for p in range(min(1, late)):
            layer_zero(g, p)
    if chunks > 1:
        low_fold(0, chunks - 1)
    complete(late)
    layer_zero(0, late)
    squares_start(0)
    with jax.named_scope("leadv"):
        lifted[...] = (states[0] * gain_ref[0:1, :]).astype(bf16)
        lead_put(1)
    for g in range(1, chunks - 1):
        for p in range(min(1, late), late):
            layer_zero(g, p)
    if chunks > 1:
        low_ready(0, chunks - 1)
        for p in range(late):
            layer_zero(chunks - 1, p)
    with jax.named_scope("leadw"):
        lead_sum(1)
    for g in range(1, chunks):
        layer_zero(g, late)
        squares_start(g)

    def pair_copy(g, slot, p):
        return remote(
            own_pair.at[g, slot, p],
            got_pair.at[g, slot, p],
            pair_send.at[2 if g else slot],
            pair_recv.at[g, 1] if slot else lone_recv.at[p] if g == 0 else pair_recv.at[g, 0],
            mine,
            mate,
        )

    def whole_pair(g, slot):
        return remote(
            own_pair.at[g, slot],
            got_pair.at[g, slot],
            pair_send.at[2 if g else slot],
            pair_recv.at[g, slot],
            mine,
            mate,
        )

    def cross_copy(g, p):
        return remote(
            own_cross.at[g, p],
            got_cross.at[g, p],
            cross_send.at[1 if g else 0],
            cross_recv.at[parts + g if g < chunks - 1 else p],
            mine,
            cross,
        )

    def whole_cross(g):
        at = pl.ds(0 if g else 1, parts if g else late)
        return remote(
            own_cross.at[g, at],
            got_cross.at[g, at],
            cross_send.at[1 if g else 0],
            cross_recv.at[parts + g],
            mine,
            cross,
        )

    def shape_ranks():
        full_block = (2, outer, 8, lanes)
        kept = (lax.broadcasted_iota(jnp.int32, full_block, 2) == 0) & (
            lax.broadcasted_iota(jnp.int32, full_block, 3) < members
        )
        shares = jnp.where(kept, granks_ref[...].astype(f32) / members_all, 0.0)

        def mean_of(value):
            value = jnp.sum(value, axis=0)
            value = jnp.sum(value, axis=0)
            value = jnp.sum(value, axis=0, keepdims=True)
            return jnp.sum(value, axis=1, keepdims=True) / members_all

        rank_mean = mean_of(shares)
        apart = jnp.where(kept, shares - rank_mean[None, None], 0.0)
        spread = mean_of(apart * apart) + spread_eps
        owner = lax.broadcasted_iota(jnp.int32, (local, lanes), 0) // rank
        own = owner == lax.broadcasted_iota(jnp.int32, (local, lanes), 1)
        for place in range(outer):
            for side_of in range(2):
                share_row = granks_ref[side_of, place, 0:1].astype(f32) / members_all
                shaped = (share_row - rank_mean) * lax.rsqrt(spread)
                shaped = jnp.where(own, jnp.broadcast_to(shaped, (local, lanes)), 0.0)
                shaped = jnp.sum(shaped, axis=1, keepdims=True)
                at = (place * 2 + side_of) * local
                shaped_ref[at : at + local] = jnp.broadcast_to(shaped, (local, lanes))

    def out_start():
        with jax.named_scope("outs"):
            plane_in.wait_recv()
            for hop in range(1, pop):
                out_copy(hop, mine).start()
            for copy in self_copies():
                copy.start()

    def gather_half():
        with jax.named_scope("half"):
            whole_out().wait_recv()
            for copy in self_copies():
                copy.wait()
            half_copy(core).start()

    def step_make():
        tile = 256
        with jax.named_scope("arrive"):
            in_buddy(buddy).wait_recv()
        with jax.named_scope("arrive_pass"):
            whole_pass().wait_recv()
        with jax.named_scope("arrive_half"):
            half_copy(1 - core).wait_recv()
        with jax.named_scope("step"):
            shape_ranks()
            shaped = jnp.concatenate([shaped_ref[...]] * (tile // lanes), axis=1)
            for layer in range(layers):
                for at in range(0, width, tile):
                    factor = gin_ref[layer, :, at : at + tile].astype(f32)
                    value = lax.dot_general(
                        (factor * shaped).astype(bf16),
                        gout_ref[layer],
                        (((0,), (0,)), ((), ())),
                        preferred_element_type=f32,
                    )
                    step_ref[layer, at : at + tile] = value * (members_all * rank) ** (-0.5)

    def between(g):
        if g == 0:
            wait_weights(1)
        with jax.named_scope("normed%d" % g):
            total = small_sum(2, g)[:1]
            scale = lax.rsqrt(total / full + norm_eps)
            scale = jnp.broadcast_to(scale, (lanes, rows)).T
            if g == 0:
                lead_scale[...] = scale
            scale = jnp.concatenate([scale] * (width // lanes), axis=1)
            gain = gain_ref[0:1, :]
            hidden[g] = (hidden[g].astype(f32) + states[g] * scale * gain).astype(bf16)

        def product(slot, p):
            return jnp.dot(
                hidden[g], weights[slot, :, halves[p]], preferred_element_type=f32
            ).astype(bf16)

        with jax.named_scope("exch%d" % g):
            def summed(p):
                value = product(1, p).astype(f32)
                if g == 0:
                    pair_copy(g, 0, p).wait_recv()
                elif p == 0:
                    whole_pair(g, 0).wait_recv()
                total = (value + got_pair[g, 0, p].astype(f32)).astype(bf16)
                own_cross[g, p] = total
                cross_copy(g, p).start()

            for p in range(0 if g else 1, parts):
                own_pair[g, 0, p] = product(0, p)
                pair_copy(g, 0, p).start()
                if p > 1 and g == 0:
                    summed(p - 1)
            left = jnp.concatenate([factor_slice(fin_ref, 1, g, 0, width), heads[...]], axis=0)
            local_low = against(left, hidden[g])
            low_put(1, g, local_low[:factor_rows])
            low_copy(1, g, 0).start()
            aligned = local_low[factor_rows : factor_rows + 8]
            alphas[g] = jnp.broadcast_to(jnp.sum(aligned, axis=0, keepdims=True), (8, rows))
            for p in range(0 if g else parts - 1, parts):
                summed(p)
            for p in range(parts):
                own_pair[g, 1, p] = product(2, p)
                pair_copy(g, 1, p).start()
            for p in range(parts):
                states[g, :, halves[p]] = product(3, p).astype(f32)

    def layer_one(g):
        with jax.named_scope("lowone%d" % g):
            low_ready(1, g)
        for p in range(parts):
            with jax.named_scope("l1_%d_%d" % (g, p)):
                if p == 0:
                    whole_pair(g, 1).wait_recv()
                fixed = (
                    states[g, :, halves[p]] + got_pair[g, 1, p].astype(f32)
                ) + correction(1, g, p)
                if g == 0 and p == 0:
                    remote(own_ahead, got_ahead, ahead_send, ahead_recv, mine, cross).wait_recv()
                    scale = jnp.concatenate([lead_scale[...]] * (piece // lanes), axis=1)
                    other = got_ahead[0].astype(f32) + scale * got_ahead[1].astype(f32)
                else:
                    if g == chunks - 1:
                        cross_copy(g, p).wait_recv()
                    elif p == (0 if g else 1):
                        whole_cross(g).wait_recv()
                    other = got_cross[g, p].astype(f32)
                recur(1, g, p, fixed + other)
        with jax.named_scope("end%d" % g):
            small[3, g, 0] = jnp.concatenate(
                [across(squares[g]), across(leans[g]), alphas[g][:2]], axis=0
            )
            small_start(3, g)

    with jax.named_scope("relay3"):
        for hop in range(3, outer):
            relay_next(hop)
            in_start(hop)
        plane.start()
    with jax.named_scope("pass1"):
        in_pass(1)
    for g in range(chunks):
        between(g)
        if g == 0:
            out_start()
        with jax.named_scope("pass"):
            for hop in range(g + 1, min(g + 2, outer) if g else 0):
                in_pass(hop)
    for g in range(chunks):
        if g < chunks - 1:
            low_fold(1, g)
        else:
            with jax.named_scope("pass"):
                for hop in range(chunks + 1, outer):
                    in_pass(hop)
            gather_half()
            if g:
                layer_one(g - 1)
            low_fold(1, g)
            step_make()
            layer_one(g)
        if g < chunks - 2:
            layer_one(g)

    lane = lax.broadcasted_iota(jnp.int32, (seqs, lanes), 1)
    scores = jnp.zeros((seqs, lanes), f32)
    with jax.named_scope("final"):
        for g in range(chunks):
            sums = small_sum(3, g)
            scale = lax.rsqrt(sums[0:1] / full + norm_eps)
            value = sums[2:3] + scale * sums[1:2]
            total = value[:, :lanes]
            for c in range(lanes, rows, lanes):
                total = total + value[:, c : c + lanes]
            total = jnp.broadcast_to(total, (8, lanes))
            shift = lanes // 2
            while shift >= group:
                total = total + pltpu.roll(total, shift, 1)
                shift //= 2
            total = total * (full ** (-0.5) / steps)
            total = jnp.broadcast_to(total[:1], (lanes, lanes)).T
            for m in range(member_rows):
                scores = jnp.where(
                    lane == g * member_rows + m, total[m * seqs : (m + 1) * seqs], scores
                )
            ending = jnp.broadcast_to(scale[:, rows - lanes :], (lanes, lanes)).T[lanes - group :]
            ending = jnp.concatenate([ending] * (width // lanes), axis=1)
            gain = gain_ref[1:2, :]
            ending = (
                hidden[g, rows - group :].astype(f32) + lasts[g] * ending * gain
            ).astype(bf16).astype(f32)
            for m in range(member_rows):
                final_ref[g * member_rows + m] = ending[m * seqs : (m + 1) * seqs].astype(bf16)
        score_ref[...] = scores[:, :members]

    with jax.named_scope("drain"):
        for hop in range(1, outer):
            relay_each(hop, lambda copy: copy.wait_send(), True)
        plane.wait_send()
        remote(own_part, got_part, part_send, part_recv.at[0, 0], mine, mate).wait_send()
        remote(own_over, got_over, over_send, over_recv.at[0, 0], mine, cross).wait_send()
        spot = table.at[:, pl.ds(0, share)]
        remote(spot, spot, hand_send, hand_recv.at[0], buddy, me).wait_send()
        spot = own_pair.at[0, 0, pl.ds(1, late)]
        remote(spot, spot, pair_send.at[0], pair_recv.at[0, 0], mine, mate).wait_send()
        spot = own_pair.at[0, 1]
        remote(spot, spot, pair_send.at[1], pair_recv.at[0, 0], mine, mate).wait_send()
        spot = own_cross.at[0, pl.ds(1, late)]
        remote(spot, spot, cross_send.at[0], cross_recv.at[0], mine, cross).wait_send()
        if chunks > 1:
            spot = own_pair.at[pl.ds(1, chunks - 1)]
            remote(spot, spot, pair_send.at[2], pair_recv.at[0, 0], mine, mate).wait_send()
        if chunks > 1:
            spot = own_cross.at[pl.ds(1, chunks - 1)]
            remote(spot, spot, cross_send.at[1], cross_recv.at[0], mine, cross).wait_send()
        remote(own_lead, got_lead, lead_send, lead_recv.at[0], mine, mate).wait_send()
        remote(own_ahead, got_ahead, ahead_send, ahead_recv, mine, cross).wait_send()
        spot = small.at[pl.ds(0, 2), :, pl.ds(0, 2)]
        remote(spot, spot, low_send, low_recv.at[0, 0, 0], mine, mate).wait_send()
        spot = small.at[pl.ds(2, 2), :, pl.ds(1, 3)]
        remote(spot, spot, small_send, small_recv.at[0, 0], mine, mate).wait_send()
        whole_in().wait_send()
        whole_pass().wait_send()
        whole_out().wait_send()
        half_copy(core).wait_send()


cuts = 2


def publish(final_ref, score_ref, step_ref, final_out, score_out, step_out, sems):
    copies = []
    layers, width, _ = step_ref.shape
    cut = width // cuts
    for layer in range(layers):
        for c in range(cuts):
            at = pl.ds(c * cut, cut)
            copies.append(
                pltpu.make_async_copy(
                    step_ref.at[layer, at], step_out.at[layer, at], sems.at[layer, c]
                )
            )
    copies.append(pltpu.make_async_copy(final_ref, final_out, sems.at[layers, 0]))
    copies.append(pltpu.make_async_copy(score_ref, score_out, sems.at[layers, 1]))
    for copy in copies:
        copy.start()
    for copy in copies:
        copy.wait()


def shards(
    token_ids,
    fitness_ranks,
    embedding,
    mix_weights,
    factors_in,
    factors_out,
    decay_rates,
    norm_gain,
    reward_dir,
):
    members, seqs, steps = token_ids.shape
    vocab, width = embedding.shape
    layers, _, full = mix_weights.shape
    rank = factors_in.shape[2]
    pop = lax.axis_size("pop")
    outer = pop // 2
    coef = noise_scale * (full * rank) ** (-0.5)
    columns = full // pop
    member_rows = 16 // seqs
    chunks = members // member_rows
    group = member_rows * seqs
    rows = group * steps
    local = members * rank
    share = vocab * 5 // 16
    dims = (pop, chunks, group, steps, member_rows, seqs, rank, width, full, coef, share)
    vmem = pl.BlockSpec(memory_space=pltpu.VMEM)
    smem = pl.BlockSpec(memory_space=pltpu.SMEM)
    hbm = pl.BlockSpec(memory_space=pltpu.HBM)
    parts = 4
    piece = width // parts
    entries = vocab - share
    dma = pltpu.SemaphoreType.DMA
    final_features, scores, step = pl.pallas_call(
        functools.partial(policy_kernel, dims),
        out_shape=(
            pltpu.VMEM((members, seqs, width), bf16),
            pltpu.VMEM((seqs, members), f32),
            pltpu.VMEM((layers, width, columns), f32),
        ),
        in_specs=[hbm, hbm, hbm, hbm, hbm, smem, hbm, hbm, hbm],
        out_specs=(vmem, vmem, vmem),
        scratch_shapes=[
            pltpu.VMEM((members, seqs, steps), jnp.int32),
            pltpu.VMEM((vocab, width), bf16),
            pltpu.VMEM((layers, members, rank, width), bf16),
            pltpu.VMEM((layers, members, rank, full), bf16),
            pltpu.VMEM((layers, width), f32),
            pltpu.VMEM((layers, width), f32),
            pltpu.VMEM((1, width), f32),
            pltpu.VMEM((4, width, width), bf16),
            pltpu.VMEM((entries, width), bf16),
            pltpu.VMEM((2, parts, entries, piece), bf16),
            pltpu.VMEM((2, parts, entries, piece), bf16),
            pltpu.VMEM((parts, entries, piece), bf16),
            pltpu.VMEM((parts, entries, piece), bf16),
            pltpu.VMEM((parts, entries, piece), bf16),
            pltpu.VMEM((parts, vocab, piece), bf16),
            pltpu.VMEM((chunks, 2, parts, rows, piece), bf16),
            pltpu.VMEM((chunks, 2, parts, rows, piece), bf16),
            pltpu.VMEM((chunks, parts, rows, piece), bf16),
            pltpu.VMEM((chunks, parts, rows, piece), bf16),
            pltpu.VMEM((2, rows, piece), bf16),
            pltpu.VMEM((2, rows, piece), bf16),
            pltpu.VMEM((2, rows, piece), bf16),
            pltpu.VMEM((2, rows, piece), bf16),
            pltpu.VMEM((rows, width), bf16),
            pltpu.VMEM((rows, lanes), f32),
            pltpu.VMEM((chunks, rows, width), f32),
            pltpu.VMEM((chunks, rows, width), bf16),
            pltpu.VMEM((chunks, rows, vocab), bf16),
            pltpu.VMEM((layers, local, width), bf16),
            pltpu.VMEM((layers, local, full), bf16),
            pltpu.VMEM((pop * local, lanes), f32),
            pltpu.VMEM((layers, pop * local, width), bf16),
            pltpu.VMEM((layers, pop * local, columns), bf16),
            pltpu.VMEM((2, outer, 8, lanes), jnp.int32),
            pltpu.VMEM((chunks, rows, lanes), bf16),
            pltpu.VMEM((chunks, rows, lanes), f32),
            pltpu.VMEM((chunks, rows, lanes), f32),
            pltpu.VMEM((chunks, group, width), f32),
            pltpu.VMEM((16, width), bf16),
            pltpu.VMEM((chunks, 8, rows), f32),
            pltpu.VMEM((4, chunks, 4, 4, rows), f32),
            dma((4,)),
            dma((2, parts)),
            dma((9,)),
            dma,
            dma((2, parts)),
            dma,
            dma((2, parts)),
            dma,
            dma((parts,)),
            dma((3,)),
            dma((chunks, 2)),
            dma((parts,)),
            dma((2,)),
            dma((parts + chunks - 1,)),
            dma,
            dma((2,)),
            dma,
            dma,
            dma,
            dma((2, chunks)),
            dma,
            dma((2, 2, chunks)),
            dma((2, outer - 1)),
            dma((2, outer - 1)),
            dma,
            dma,
            dma,
            dma((2, outer - 1)),
            dma,
            dma,
            dma,
            dma,
            dma,
            dma,
            dma,
            dma((2,)),
        ],
        compiler_params=pltpu.CompilerParams(
            collective_id=0, has_side_effects=True, vmem_limit_bytes=52 * 1024 * 1024
        ),
    )(
        *(
            pltpu.with_memory_space_constraint(value, pltpu.HBM)
            for value in (
                token_ids,
                embedding,
                mix_weights,
                factors_in,
                factors_out,
                fitness_ranks,
                decay_rates,
                norm_gain,
                reward_dir.reshape(1, width),
            )
        )
    )
    final_features, scores, weight_step = pl.pallas_call(
        publish,
        out_shape=(
            jax.ShapeDtypeStruct((members, seqs, width), bf16),
            jax.ShapeDtypeStruct((seqs, members), f32),
            jax.ShapeDtypeStruct((layers, width, columns), f32),
        ),
        in_specs=[vmem, vmem, vmem],
        out_specs=(hbm, hbm, hbm),
        scratch_shapes=[dma((layers + 1, cuts))],
        compiler_params=pltpu.CompilerParams(vmem_limit_bytes=1024 * 1024),
    )(final_features, scores, step)
    return (final_features, scores.T, weight_step)


def solution(mesh):
    return jax.shard_map(
        shards,
        mesh=mesh,
        in_specs=(
            P("pop", None, None),
            P("pop"),
            P(None, "mp"),
            P(None, "mp", None),
            P(None, "pop", None, "mp"),
            P(None, "pop", None, None),
            P(None, "mp"),
            P(None, "mp"),
            P("mp"),
        ),
        out_specs=(P("pop", None, "mp"), P("pop", None), P(None, "mp", "pop")),
        check_vma=False,
    )
```
